8 devices in a mesh: dp: 1 (over z), tp: 2 (over y), pp: 4 (over x, core).
Axes of the slice: x: 2, y: 2, z: 1, core: 2. Of those that a mesh axis runs over, the one named last changes fastest.
Arguments:
- x_in: bfloat16 [2, 12, 256, 1536], P(None, 'dp')
- dy_out: bfloat16 [2, 12, 256, 1536], P(None, 'dp')
- w_qkv: bfloat16 [4, 3, 1536, 16, 96], P('pp', None, None, 'tp')
- b_qkv: bfloat16 [4, 3, 16, 96], P('pp', None, 'tp')
- w_out: bfloat16 [4, 16, 96, 1536], P('pp', 'tp')
- b_out: bfloat16 [4, 1536], P('pp')
- ln_par: bfloat16 [4, 4, 1536], P('pp')
- w_fc1: bfloat16 [4, 1536, 6144], P('pp', None, 'tp')
- b_fc1: bfloat16 [4, 6144], P('pp', 'tp')
- w_fc2: bfloat16 [4, 6144, 1536], P('pp', 'tp')
- b_fc2: bfloat16 [4, 1536], P('pp')
Outputs:
- output 1: bfloat16 [4, 2, 12, 256, 1536], P('pp', None, 'dp')
- output 2: bfloat16 [4, 2, 12, 256, 1536], P('pp', None, 'dp')
- output 3: float32 [4, 3, 1536, 16, 96], P(('dp', 'pp'), None, None, 'tp')
- output 4: float32 [4, 3, 16, 96], P(('dp', 'pp'), None, 'tp')
- output 5: float32 [4, 16, 96, 1536], P(('dp', 'pp'), 'tp')
- output 6: float32 [4, 1536], P(('dp', 'pp'))
- output 7: float32 [4, 4, 1536], P(('dp', 'pp'))
- output 8: float32 [4, 1536, 6144], P(('dp', 'pp'), None, 'tp')
- output 9: float32 [4, 6144], P(('dp', 'pp'), 'tp')
- output 10: float32 [4, 6144, 1536], P(('dp', 'pp'), 'tp')
- output 11: float32 [4, 1536], P(('dp', 'pp'))
All inputs are finite; a program needn't handle non-finite values.
Results may differ from the reference program's by a relative error of at most 0.02.
Values are sent between devices in bfloat16 or wider.
A program may use at most 1 GiB of HBM per device.

```python
import jax
import jax.numpy as jnp
from jax import lax

NUM_STAGES = 4
NUM_MICRO = 2
MICRO_ROWS = 12
SEQ_LEN = 256
D_MODEL = 1536
NUM_HEADS = 16
D_FF = 6144

HEAD_DIM = D_MODEL // NUM_HEADS
LN_EPS = 1e-5


def setup_inputs(seed: int = 0, part: int = 0) -> dict:
    base_key = jax.random.key(seed)
    data_keys = jax.random.split(jax.random.fold_in(base_key, part), 2)
    param_keys = jax.random.split(base_key, 9)
    act_shape = (NUM_MICRO, MICRO_ROWS, SEQ_LEN, D_MODEL)
    in_scale = D_MODEL ** -0.5
    ff_scale = D_FF ** -0.5
    ln_offset = jnp.array([1.0, 0.0, 1.0, 0.0], jnp.float32)[None, :, None]

    def normal_draw(key_item, shape_tuple, draw_scale):
        return jax.random.normal(key_item, shape_tuple, jnp.float32) * draw_scale

    return {
        "x_in": normal_draw(data_keys[0], act_shape, 1.0).astype(jnp.bfloat16),
        "dy_out": normal_draw(data_keys[1], act_shape, 1.0).astype(jnp.bfloat16),
        "w_qkv": normal_draw(param_keys[0], (NUM_STAGES, 3, D_MODEL, NUM_HEADS, HEAD_DIM), in_scale).astype(jnp.bfloat16),
        "b_qkv": normal_draw(param_keys[1], (NUM_STAGES, 3, NUM_HEADS, HEAD_DIM), 0.5).astype(jnp.bfloat16),
        "w_out": normal_draw(param_keys[2], (NUM_STAGES, NUM_HEADS, HEAD_DIM, D_MODEL), in_scale).astype(jnp.bfloat16),
        "b_out": normal_draw(param_keys[3], (NUM_STAGES, D_MODEL), 0.3).astype(jnp.bfloat16),
        "ln_par": (normal_draw(param_keys[4], (NUM_STAGES, 4, D_MODEL), 0.3) + ln_offset).astype(jnp.bfloat16),
        "w_fc1": normal_draw(param_keys[5], (NUM_STAGES, D_MODEL, D_FF), in_scale).astype(jnp.bfloat16),
        "b_fc1": normal_draw(param_keys[6], (NUM_STAGES, D_FF), 0.5).astype(jnp.bfloat16),
        "w_fc2": normal_draw(param_keys[7], (NUM_STAGES, D_FF, D_MODEL), ff_scale).astype(jnp.bfloat16),
        "b_fc2": normal_draw(param_keys[8], (NUM_STAGES, D_MODEL), 0.3).astype(jnp.bfloat16),
    }


def layer_norm(x_act, ln_gain, ln_shift):
    x_wide = x_act.astype(jnp.float32)
    row_mean = jnp.mean(x_wide, axis=-1, keepdims=True)
    centered = x_wide - row_mean
    row_var = jnp.mean(centered * centered, axis=-1, keepdims=True)
    normed = centered * lax.rsqrt(row_var + LN_EPS)
    return (normed * ln_gain.astype(jnp.float32) + ln_shift.astype(jnp.float32)).astype(jnp.bfloat16)


def causal_attention(q_heads, k_heads, v_heads):
    scores = jnp.einsum("bqhe,bkhe->bhqk", q_heads.astype(jnp.float32), k_heads.astype(jnp.float32)) * (HEAD_DIM ** -0.5)
    positions = jnp.arange(SEQ_LEN)
    causal = positions[:, None] >= positions[None, :]
    scores = jnp.where(causal, scores, -1e30)
    attn_probs = jax.nn.softmax(scores, axis=-1).astype(jnp.bfloat16)
    attn_mix = jnp.einsum("bhqk,bkhe->bqhe", attn_probs.astype(jnp.float32), v_heads.astype(jnp.float32))
    return attn_mix.astype(jnp.bfloat16)


def gpt_layer(x_act, w_qkv, b_qkv, w_out, b_out, ln_par, w_fc1, b_fc1, w_fc2, b_fc2):
    h_one = layer_norm(x_act, ln_par[0], ln_par[1])
    qkv_pre = jnp.einsum("bsd,cdhe->bsche", h_one.astype(jnp.float32), w_qkv.astype(jnp.float32)) + b_qkv.astype(jnp.float32)
    qkv_all = qkv_pre.astype(jnp.bfloat16)
    attn_mix = causal_attention(qkv_all[:, :, 0], qkv_all[:, :, 1], qkv_all[:, :, 2])
    attn_sum = jnp.einsum("bshe,hed->bsd", attn_mix.astype(jnp.float32), w_out.astype(jnp.float32))
    x_mid = (x_act.astype(jnp.float32) + attn_sum + b_out.astype(jnp.float32)).astype(jnp.bfloat16)
    h_two = layer_norm(x_mid, ln_par[2], ln_par[3])
    pre_act = jnp.einsum("bsd,df->bsf", h_two.astype(jnp.float32), w_fc1.astype(jnp.float32)) + b_fc1.astype(jnp.float32)
    gelu_out = jax.nn.gelu(pre_act, approximate=True).astype(jnp.bfloat16)
    mlp_sum = jnp.einsum("bsf,fd->bsd", gelu_out.astype(jnp.float32), w_fc2.astype(jnp.float32))
    return (x_mid.astype(jnp.float32) + mlp_sum + b_fc2.astype(jnp.float32)).astype(jnp.bfloat16)


def reference(x_in, dy_out, w_qkv, b_qkv, w_out, b_out, ln_par, w_fc1, b_fc1, w_fc2, b_fc2):
    weights = (w_qkv, b_qkv, w_out, b_out, ln_par, w_fc1, b_fc1, w_fc2, b_fc2)

    def forward_step(x_act, layer_w):
        y_act = gpt_layer(x_act, *layer_w)
        return y_act, (x_act, y_act)

    def backward_step(grad_act, layer_pack):
        layer_in, layer_w = layer_pack
        wide_w = tuple(w_item.astype(jnp.float32) for w_item in layer_w)
        _, pullback = jax.vjp(gpt_layer, layer_in, *wide_w)
        grad_list = pullback(grad_act)
        return grad_list[0], (grad_list[0], grad_list[1:])

    def one_micro(grad_acc, micro_pack):
        x_micro, dy_micro = micro_pack
        _, (stage_in, stage_out) = lax.scan(forward_step, x_micro, weights)
        _, (stage_grad, weight_grad) = lax.scan(backward_step, dy_micro, (stage_in, weights), reverse=True)
        grad_acc = tuple(acc_item + new_item for acc_item, new_item in zip(grad_acc, weight_grad))
        return grad_acc, (stage_out, stage_grad)

    grad_init = tuple(jnp.zeros(w_item.shape, jnp.float32) for w_item in weights)
    grad_sum, (all_out, all_grad) = lax.scan(one_micro, grad_init, (x_in, dy_out))
    h_out = jnp.swapaxes(all_out, 0, 1)
    g_in = jnp.swapaxes(all_grad, 0, 1)
    return (h_out, g_in, grad_sum[0], grad_sum[1], grad_sum[2], grad_sum[3], grad_sum[4], grad_sum[5], grad_sum[6], grad_sum[7], grad_sum[8])
```

```python
import functools

import jax
import jax.numpy as jnp
from jax import lax
from jax.experimental import pallas as pl
from jax.experimental.pallas import tpu as pltpu
from jax.sharding import PartitionSpec as P

LN_EPS = 1e-5
F32 = jnp.float32
BF16 = jnp.bfloat16
MESH = pl.DeviceIdType.MESH
NEG = -1e30
ROW_CHUNK = 32
GELU_C = 0.7978845608028654
GELU_K = 0.044715

WINDOWS = ((0, 128, 0), (0, 256, 96), (128, 256, 64), (256, 128, 32))


def dot_nn(lhs, rhs):
    return lax.dot_general(lhs, rhs, (((1,), (0,)), ((), ())), preferred_element_type=F32)


def dot_nt(lhs, rhs):
    return lax.dot_general(lhs, rhs, (((1,), (1,)), ((), ())), preferred_element_type=F32)


def dot_tn(lhs, rhs):
    return lax.dot_general(lhs, rhs, (((0,), (0,)), ((), ())), preferred_element_type=F32)


def head_only(window, offset, width):
    lane = lax.broadcasted_iota(jnp.int32, window.shape, 1)
    return jnp.where((lane >= offset) & (lane < offset + width), window, jnp.zeros_like(window))


def join_heads(parts, width):
    lane = lax.broadcasted_iota(jnp.int32, (parts[0].shape[0], 128), 1)
    first = jnp.where(lane < width, parts[0], parts[1][:, :128])
    second = jnp.where(lane < 2 * width - 128, parts[1][:, 128:], parts[2][:, :128])
    third = jnp.where(lane < 3 * width - 256, parts[2][:, 128:], parts[3])
    return first, second, third


def norm_stats(x_wide):
    centered = x_wide - jnp.mean(x_wide, axis=-1, keepdims=True)
    inv_std = lax.rsqrt(jnp.mean(centered * centered, axis=-1, keepdims=True) + LN_EPS)
    return centered * inv_std, inv_std


def fold_rows(block):
    rows, cols = block.shape
    return jnp.sum(block.reshape(rows // 8, 8, cols), axis=0)


def neighbour_barrier(stage, tp_peer, stages):
    barrier = pltpu.get_barrier_semaphore()
    pl.semaphore_signal(barrier, inc=1, device_id={"tp": tp_peer}, device_id_type=MESH)
    pl.semaphore_signal(barrier, inc=1, device_id={"pp": lax.rem(stage + 1, stages)}, device_id_type=MESH)
    pl.semaphore_signal(barrier, inc=1, device_id={"pp": lax.rem(stage + stages - 1, stages)}, device_id_type=MESH)
    pl.semaphore_wait(barrier, 3)


def fwd_kernel(subs, stages, width, tile,
               x_in, wq_h, wo_h, w1_h, w2_h, bq, bo, ln, b1, b2,
               x_all, qkv_all, o_all, mid_all, h1_all, h2_all, u_all, a_all, y_all, part_all,
               wq, wo, w1, w2, xb, h1b, qkvb, ob, midb, h2b, ub, ab, partb, rb, yb,
               w_sem, in_sem, out_sem, mid_sem, y_sem, part_send, part_recv, y_send, x_recv):
    stage = lax.axis_index("pp")
    tp_me = lax.axis_index("tp")
    tp_peer = 1 - tp_me
    last_stage = stages - 1
    rows, d_model = xb.shape
    half = d_model // 2
    ff = ub.shape[1]
    scale = width ** -0.5

    loads = [pltpu.make_async_copy(src, dst, w_sem.at[i]) for i, (src, dst) in enumerate(((wq_h, wq), (wo_h, wo), (w1_h, w1), (w2_h, w2)))]
    for load in loads:
        load.start()
    neighbour_barrier(stage, tp_peer, stages)

    def outs(m):
        return (pltpu.make_async_copy(h1b, h1_all.at[m], out_sem.at[0]),
                pltpu.make_async_copy(qkvb, qkv_all.at[m], out_sem.at[1]),
                pltpu.make_async_copy(ob.at[:, pl.ds(pl.multiple_of(tp_me * half, 128), half)], o_all.at[m], out_sem.at[2]),
                pltpu.make_async_copy(h2b, h2_all.at[m], out_sem.at[3]),
                pltpu.make_async_copy(ub, u_all.at[m], out_sem.at[4]),
                pltpu.make_async_copy(ab, a_all.at[m], out_sem.at[5]),
                pltpu.make_async_copy(xb, x_all.at[m], out_sem.at[6]))

    def mid_out(m):
        slot = lax.rem(m, 2)
        return pltpu.make_async_copy(midb.at[slot], mid_all.at[m], mid_sem.at[slot])

    def y_out(m):
        slot = lax.rem(m, 2)
        return pltpu.make_async_copy(yb.at[slot], y_all.at[m], y_sem.at[slot])

    def part_copy(m):
        slot = lax.rem(m, 2)
        return pltpu.make_async_remote_copy(src_ref=partb.at[slot], dst_ref=part_all.at[m], send_sem=part_send.at[slot], recv_sem=part_recv.at[m],
                                            device_id={"tp": tp_peer}, device_id_type=MESH)

    def next_copy(m):
        slot = lax.rem(m, 2)
        return pltpu.make_async_remote_copy(src_ref=yb.at[slot], dst_ref=x_all.at[m], send_sem=y_send.at[slot], recv_sem=x_recv.at[m],
                                            device_id={"pp": jnp.minimum(stage + 1, last_stage)}, device_id_type=MESH)

    def layer_norm(src, dst, gain, shift):
        for r in range(0, rows, ROW_CHUNK):
            normed, _ = norm_stats(src[r:r + ROW_CHUNK, :].astype(F32))
            dst[r:r + ROW_CHUNK, :] = (normed * gain + shift).astype(BF16)

    def attend(group, carry):
        base = pl.multiple_of((group // 2) * (3 * half) + lax.rem(group, 2) * (4 * width), 128)
        out_base = pl.multiple_of(group * (4 * width), 128)
        for blk in range(rows // 128):
            r0, keys = blk * 128, (blk + 1) * 128
            row = lax.broadcasted_iota(jnp.int32, (128, keys), 0) + r0
            col = lax.broadcasted_iota(jnp.int32, (128, keys), 1)
            parts = []
            for start, size, offset in WINDOWS:
                query = head_only(qkvb[r0:r0 + 128, pl.ds(base + start, size)], offset, width)
                key = qkvb[0:keys, pl.ds(base + half + start, size)]
                value = qkvb[0:keys, pl.ds(base + 2 * half + start, size)]
                score = jnp.where(row >= col, dot_nt(query, key) * scale, NEG)
                weight = jnp.exp(score - jnp.max(score, axis=1, keepdims=True))
                prob = (weight * (1.0 / jnp.sum(weight, axis=1, keepdims=True))).astype(BF16)
                parts.append(dot_nn(prob, value))
            for i, piece in enumerate(join_heads(parts, width)):
                ob[r0:r0 + 128, pl.ds(out_base + i * 128, 128)] = piece.astype(BF16)
        return carry

    def finish(m):
        slot = lax.rem(m, 2)
        part_copy(m).wait_recv()
        load = pltpu.make_async_copy(part_all.at[m], rb, in_sem)
        load.start()

        @pl.when(m >= 2)
        def _():
            y_out(m - 2).wait()

            @pl.when(stage < last_stage)
            def _():
                next_copy(m - 2).wait_send()

        load.wait()
        for r in range(0, rows, ROW_CHUNK):
            both = partb[slot, r:r + ROW_CHUNK, :].astype(F32) + rb[r:r + ROW_CHUNK, :].astype(F32)
            yb[slot, r:r + ROW_CHUNK, :] = (midb[slot, r:r + ROW_CHUNK, :].astype(F32) + both + b2[...]).astype(BF16)

        @pl.when(stage < last_stage)
        def _():
            next_copy(m).start()

        y_out(m).start()
        part_copy(m).wait_send()

    def one_sub(m, carry):
        slot = lax.rem(m, 2)
        prev = jnp.maximum(m - 1, 0)
        h1_o, qkv_o, o_o, h2_o, u_o, a_o, x_o = outs(m)
        h1_p, qkv_p, o_p, h2_p, u_p, a_p, x_p = outs(prev)

        @pl.when(stage == 0)
        def _():
            @pl.when(m > 0)
            def _():
                x_p.wait()

            load = pltpu.make_async_copy(x_in.at[m], xb, in_sem)
            load.start()
            load.wait()
            x_o.start()

        @pl.when(stage > 0)
        def _():
            next_copy(m).wait_recv()
            load = pltpu.make_async_copy(x_all.at[m], xb, in_sem)
            load.start()
            load.wait()

        @pl.when(m > 0)
        def _():
            h1_p.wait()
            qkv_p.wait()
            o_p.wait()
            h2_p.wait()

        layer_norm(xb, h1b, ln[0:1, :], ln[1:2, :])
        h1_o.start()

        @pl.when(m == 0)
        def _():
            loads[0].wait()

        for n in range(0, 3 * d_model, tile):
            qkvb[:, n:n + tile] = (dot_nn(h1b[...], wq[:, n:n + tile]) + bq[:, n:n + tile]).astype(BF16)
        qkv_o.start()
        lax.fori_loop(0, d_model // (4 * width), attend, 0)
        o_o.start()

        @pl.when(m == 0)
        def _():
            for load in loads[1:]:
                load.wait()

        @pl.when(m >= 2)
        def _():
            mid_out(m - 2).wait()

        for n in range(0, d_model, tile):
            midb[slot, :, n:n + tile] = (xb[:, n:n + tile].astype(F32) + dot_nn(ob[...], wo[:, n:n + tile]) + bo[:, n:n + tile]).astype(BF16)
        mid_out(m).start()
        layer_norm(midb.at[slot], h2b, ln[2:3, :], ln[3:4, :])
        h2_o.start()

        @pl.when(m > 0)
        def _():
            u_p.wait()
            a_p.wait()

        for n in range(0, ff, tile):
            pre = dot_nn(h2b[...], w1[:, n:n + tile]) + b1[:, n:n + tile]
            ub[:, n:n + tile] = pre
            cdf = 0.5 * (1.0 + jnp.tanh(GELU_C * (pre + GELU_K * (pre * pre * pre))))
            ab[:, n:n + tile] = (pre * cdf).astype(BF16)
        u_o.start()
        a_o.start()
        for n in range(0, d_model, tile):
            partb[slot, :, n:n + tile] = dot_nn(ab[...], w2[:, n:n + tile]).astype(BF16)
        part_copy(m).start()

        @pl.when(m > 0)
        def _():
            finish(m - 1)

        return carry

    lax.fori_loop(0, subs, one_sub, 0)
    finish(subs - 1)
    h1_o, qkv_o, o_o, h2_o, u_o, a_o, x_o = outs(subs - 1)
    for copy in (h1_o, qkv_o, o_o, h2_o, u_o, a_o):
        copy.wait()

    @pl.when(stage == 0)
    def _():
        x_o.wait()

    for m in (subs - 2, subs - 1):
        mid_out(m).wait()
        y_out(m).wait()

        @pl.when(stage < last_stage)
        def _():
            next_copy(m).wait_send()


def bwd_kernel(subs, stages, width, tile,
               dy_in, x_all, mid_all, u_all, qkv_all, w2t_h, w1t_h, wot_h, wqt_h, ln,
               dy_all, dpre_all, gmid_all, dqkv_all, gin_all, part_all, db1, db2, dbo, dbq, dln,
               w2t, w1t, wot, wqt, dyb, ub, dpb, partb, rb, midb, xb, gmb, qkvb, gib,
               w_sem, in_sem, pre_sem, out_sem, dy_sem, gi_sem, part_send, part_recv, gi_send, dy_recv):
    stage = lax.axis_index("pp")
    tp_me = lax.axis_index("tp")
    tp_peer = 1 - tp_me
    last_stage = stages - 1
    rows, d_model = xb.shape
    half = d_model // 2
    ff = ub.shape[1]
    scale = width ** -0.5

    loads = [pltpu.make_async_copy(src, dst, w_sem.at[i]) for i, (src, dst) in enumerate(((w2t_h, w2t), (w1t_h, w1t), (wot_h, wot), (wqt_h, wqt)))]
    for load in loads:
        load.start()

    def fetch(m):
        return (pltpu.make_async_copy(u_all.at[m], ub, pre_sem.at[0]),
                pltpu.make_async_copy(mid_all.at[m], midb, pre_sem.at[1]),
                pltpu.make_async_copy(qkv_all.at[m], qkvb, pre_sem.at[2]),
                pltpu.make_async_copy(x_all.at[m], xb, pre_sem.at[3]))

    for copy in fetch(0):
        copy.start()
    for acc in (db1, db2, dbo, dbq, dln):
        acc[...] = jnp.zeros_like(acc)
    neighbour_barrier(stage, tp_peer, stages)

    def outs(m):
        return (pltpu.make_async_copy(dpb, dpre_all.at[m], out_sem.at[0]),
                pltpu.make_async_copy(gmb, gmid_all.at[m], out_sem.at[1]),
                pltpu.make_async_copy(qkvb.at[:, pl.ds(pl.multiple_of(tp_me * (3 * half), 128), 3 * half)], dqkv_all.at[m], out_sem.at[2]))

    def dy_out(m):
        slot = lax.rem(m, 2)
        return pltpu.make_async_copy(dyb.at[slot], dy_all.at[m], dy_sem.at[slot])

    def gi_out(m):
        slot = lax.rem(m, 2)
        return pltpu.make_async_copy(gib.at[slot], gin_all.at[m], gi_sem.at[slot])

    def part_copy(m):
        slot = lax.rem(m, 2)
        return pltpu.make_async_remote_copy(src_ref=partb.at[slot], dst_ref=part_all.at[m], send_sem=part_send.at[slot], recv_sem=part_recv.at[m],
                                            device_id={"tp": tp_peer}, device_id_type=MESH)

    def prev_copy(m):
        slot = lax.rem(m, 2)
        return pltpu.make_async_remote_copy(src_ref=gib.at[slot], dst_ref=dy_all.at[m], send_sem=gi_send.at[slot], recv_sem=dy_recv.at[m],
                                            device_id={"pp": jnp.maximum(stage - 1, 0)}, device_id_type=MESH)

    def norm_grad(x_rows, grad, gain, which):
        normed, inv_std = norm_stats(x_rows)
        dln[which] += fold_rows(grad * normed)
        dln[which + 1] += fold_rows(grad)
        scaled = grad * gain
        mean_scaled = jnp.mean(scaled, axis=-1, keepdims=True)
        mean_proj = jnp.mean(scaled * normed, axis=-1, keepdims=True)
        return inv_std * (scaled - mean_scaled - normed * mean_proj)

    def mlp_part(m):
        slot = lax.rem(m, 2)
        u_f = fetch(m)[0]

        @pl.when(stage == last_stage)
        def _():
            @pl.when(m >= 2)
            def _():
                dy_out(m - 2).wait()

            load = pltpu.make_async_copy(dy_in.at[m], dyb.at[slot], in_sem)
            load.start()
            load.wait()
            dy_out(m).start()

        @pl.when(stage < last_stage)
        def _():
            prev_copy(m).wait_recv()
            load = pltpu.make_async_copy(dy_all.at[m], dyb.at[slot], in_sem)
            load.start()
            load.wait()

        @pl.when(m == 0)
        def _():
            loads[0].wait()
            loads[1].wait()

        @pl.when(m > 0)
        def _():
            outs(m - 1)[0].wait()

        u_f.wait()
        for r in range(0, rows, ROW_CHUNK):
            db2[...] += fold_rows(dyb[slot, r:r + ROW_CHUNK, :].astype(F32))
        for n in range(0, ff, tile):
            grad = dot_nn(dyb[slot], w2t[:, n:n + tile]).astype(BF16).astype(F32)
            pre = ub[:, n:n + tile]
            square = pre * pre
            bend = jnp.tanh(GELU_C * (pre + GELU_K * (square * pre)))
            slope = 0.5 * (1.0 + bend) + (0.5 * GELU_C) * pre * (1.0 - bend * bend) * (1.0 + (3.0 * GELU_K) * square)
            grad = grad * slope
            db1[:, n:n + tile] += fold_rows(grad)
            dpb[:, n:n + tile] = grad.astype(BF16)
        outs(m)[0].start()

        @pl.when(m + 1 < subs)
        def _():
            fetch(m + 1)[0].start()

        for n in range(0, d_model, tile):
            partb[slot, :, n:n + tile] = dot_nn(dpb[...], w1t[:, n:n + tile]).astype(BF16)
        part_copy(m).start()

    def attend_grad(group, carry):
        base = pl.multiple_of((group // 2) * (3 * half) + lax.rem(group, 2) * (4 * width), 128)
        do_base = pl.multiple_of(group * (4 * width), 128)
        key_rows = rows
        d_query = [[], []]
        d_key, d_value = [], []
        for start, size, offset in WINDOWS:
            dk_sum = dv_sum = None
            for blk in range(rows // 128):
                r0, keys = blk * 128, (blk + 1) * 128
                query = qkvb[r0:r0 + 128, pl.ds(base + start, size)]
                d_out = rb[r0:r0 + 128, pl.ds(do_base + start, size)]
                key = qkvb[0:keys, pl.ds(base + half + start, size)]
                value = qkvb[0:keys, pl.ds(base + 2 * half + start, size)]
                krow = lax.broadcasted_iota(jnp.int32, (keys, 128), 0)
                qcol = lax.broadcasted_iota(jnp.int32, (keys, 128), 1) + r0
                score = jnp.where(qcol >= krow, dot_nt(key, head_only(query, offset, width)) * scale, NEG)
                weight = jnp.exp(score - jnp.max(score, axis=0, keepdims=True))
                prob = weight * (1.0 / jnp.sum(weight, axis=0, keepdims=True))
                d_prob = dot_nt(value, head_only(d_out, offset, width))
                d_score = prob * (d_prob - jnp.sum(prob * d_prob, axis=0, keepdims=True))
                d_score = d_score.astype(BF16)
                d_query[blk].append(dot_tn(d_score, key) * scale)
                dk_new = dot_nn(d_score, query) * scale
                dv_new = dot_nn(prob.astype(BF16), d_out)
                if keys < key_rows:
                    rest = jnp.zeros((key_rows - keys, size), F32)
                    dk_new = jnp.concatenate([dk_new, rest], axis=0)
                    dv_new = jnp.concatenate([dv_new, rest], axis=0)
                dk_sum = dk_new if dk_sum is None else dk_sum + dk_new
                dv_sum = dv_new if dv_sum is None else dv_sum + dv_new
            d_key.append(dk_sum)
            d_value.append(dv_sum)
        for blk in range(rows // 128):
            for i, piece in enumerate(join_heads(d_query[blk], width)):
                piece = piece.astype(BF16)
                lanes = pl.ds(base + i * 128, 128)
                qkvb[blk * 128:(blk + 1) * 128, lanes] = piece
                dbq[:, lanes] += fold_rows(piece.astype(F32))
        for c, parts in ((1, d_key), (2, d_value)):
            for i, piece in enumerate(join_heads(parts, width)):
                piece = piece.astype(BF16)
                lanes = pl.ds(base + c * half + i * 128, 128)
                qkvb[:, lanes] = piece
                dbq[:, lanes] += fold_rows(piece.astype(F32))
        return carry

    def attn_part(m):
        slot = lax.rem(m, 2)
        _, mid_f, qkv_f, x_f = fetch(m)
        _, gm_o, dq_o = outs(m)
        part_copy(m).wait_recv()
        load = pltpu.make_async_copy(part_all.at[m], rb, in_sem)
        load.start()
        mid_f.wait()

        @pl.when(m > 0)
        def _():
            outs(m - 1)[1].wait()

        @pl.when(m == 0)
        def _():
            loads[2].wait()
            loads[3].wait()

        load.wait()
        for r in range(0, rows, ROW_CHUNK):
            rr = slice(r, r + ROW_CHUNK)
            grad = (partb[slot, rr, :].astype(F32) + rb[rr, :].astype(F32)).astype(BF16).astype(F32)
            total = dyb[slot, rr, :].astype(F32) + norm_grad(midb[rr, :].astype(F32), grad, ln[2:3, :], 2)
            gmb[rr, :] = total.astype(BF16)
            dbo[...] += fold_rows(total)
        gm_o.start()

        @pl.when(m + 1 < subs)
        def _():
            fetch(m + 1)[1].start()

        for n in range(0, d_model, tile):
            rb[:, n:n + tile] = dot_nn(gmb[...], wot[:, n:n + tile]).astype(BF16)
        qkv_f.wait()
        lax.fori_loop(0, d_model // (4 * width), attend_grad, 0)
        dq_o.start()
        part_copy(m).wait_send()
        for n in range(0, d_model, tile):
            rb[:, n:n + tile] = dot_nn(qkvb[...], wqt[:, n:n + tile]).astype(BF16)
        x_f.wait()

        @pl.when(m >= 2)
        def _():
            gi_out(m - 2).wait()

            @pl.when(stage > 0)
            def _():
                prev_copy(m - 2).wait_send()

        for r in range(0, rows, ROW_CHUNK):
            rr = slice(r, r + ROW_CHUNK)
            total = gmb[rr, :].astype(F32) + norm_grad(xb[rr, :].astype(F32), rb[rr, :].astype(F32), ln[0:1, :], 0)
            gib[slot, rr, :] = total.astype(BF16)

        @pl.when(stage > 0)
        def _():
            prev_copy(m).start()

        gi_out(m).start()
        dq_o.wait()

        @pl.when(m + 1 < subs)
        def _():
            fetch(m + 1)[2].start()
            fetch(m + 1)[3].start()

    def one_sub(m, carry):
        mlp_part(m)

        @pl.when(m > 0)
        def _():
            attn_part(m - 1)

        return carry

    lax.fori_loop(0, subs, one_sub, 0)
    attn_part(subs - 1)
    for copy in outs(subs - 1)[:2]:
        copy.wait()
    for m in (subs - 2, subs - 1):
        gi_out(m).wait()

        @pl.when(stage > 0)
        def _():
            prev_copy(m).wait_send()

        @pl.when(stage == last_stage)
        def _():
            dy_out(m).wait()


ANY = pl.BlockSpec(memory_space=pl.ANY)
VMEM = pl.BlockSpec(memory_space=pltpu.VMEM)
DMA = pltpu.SemaphoreType.DMA
VMEM_LIMIT = 67043328


def fwd_call(stages, width, tile, x_in, wq, wo, w1, w2, bq, bo, ln, b1, b2):
    subs, rows, d_model = x_in.shape
    ff = w1.shape[1]
    half = d_model // 2

    def hbm(cols, dtype=BF16):
        return jax.ShapeDtypeStruct((subs, rows, cols), dtype)

    def buf(cols, dtype=BF16):
        return pltpu.VMEM((rows, cols), dtype)

    def two(cols):
        return pltpu.VMEM((2, rows, cols), BF16)

    weights = 2 * (4 * d_model * d_model + 2 * d_model * ff)
    return pl.pallas_call(
        functools.partial(fwd_kernel, subs, stages, width, tile),
        name="fwd_stage",
        out_shape=(hbm(d_model), hbm(3 * d_model), hbm(half), hbm(d_model), hbm(d_model), hbm(d_model), hbm(ff, F32), hbm(ff), hbm(d_model), hbm(d_model)),
        in_specs=[ANY] * 5 + [VMEM] * 5,
        out_specs=[ANY] * 10,
        scratch_shapes=[
            pltpu.VMEM(wq.shape, BF16), pltpu.VMEM(wo.shape, BF16), pltpu.VMEM(w1.shape, BF16), pltpu.VMEM(w2.shape, BF16),
            buf(d_model), buf(d_model), buf(3 * d_model), buf(d_model), two(d_model), buf(d_model), buf(ff, F32), buf(ff), two(d_model), buf(d_model), two(d_model),
            DMA((4,)), DMA, DMA((7,)), DMA((2,)), DMA((2,)), DMA((2,)), DMA((subs,)), DMA((2,)), DMA((subs,)),
        ],
        cost_estimate=pl.CostEstimate(flops=subs * rows * weights, bytes_accessed=weights + subs * rows * d_model * 30, transcendentals=subs * rows * (ff + rows * 16)),
        compiler_params=pltpu.CompilerParams(collective_id=0, has_side_effects=True, vmem_limit_bytes=VMEM_LIMIT),
    )(x_in, wq, wo, w1, w2, bq, bo, ln, b1, b2)


def bwd_call(stages, width, tile, dy_in, x_all, mid_all, u_all, qkv_all, w2t, w1t, wot, wqt, ln):
    subs, rows, d_model = dy_in.shape
    ff = u_all.shape[2]
    half = d_model // 2

    def hbm(cols, dtype=BF16):
        return jax.ShapeDtypeStruct((subs, rows, cols), dtype)

    def buf(cols, dtype=BF16):
        return pltpu.VMEM((rows, cols), dtype)

    def two(cols):
        return pltpu.VMEM((2, rows, cols), BF16)

    def acc(*shape):
        return jax.ShapeDtypeStruct(shape, F32)

    weights = 2 * (4 * d_model * d_model + 2 * d_model * ff)
    return pl.pallas_call(
        functools.partial(bwd_kernel, subs, stages, width, tile),
        name="bwd_stage",
        out_shape=(hbm(d_model), hbm(ff), hbm(d_model), hbm(3 * half), hbm(d_model), hbm(d_model),
                   acc(8, ff), acc(8, d_model), acc(8, d_model), acc(8, 3 * d_model), acc(4, 8, d_model)),
        in_specs=[ANY] * 9 + [VMEM],
        out_specs=[ANY] * 6 + [VMEM] * 5,
        scratch_shapes=[
            pltpu.VMEM(w2t.shape, BF16), pltpu.VMEM(w1t.shape, BF16), pltpu.VMEM(wot.shape, BF16), pltpu.VMEM(wqt.shape, BF16),
            two(d_model), buf(ff, F32), buf(ff), two(d_model), buf(d_model), buf(d_model), buf(d_model), buf(d_model), buf(3 * d_model), two(d_model),
            DMA((4,)), DMA, DMA((4,)), DMA((3,)), DMA((2,)), DMA((2,)), DMA((2,)), DMA((subs,)), DMA((2,)), DMA((subs,)),
        ],
        cost_estimate=pl.CostEstimate(flops=subs * rows * weights, bytes_accessed=weights + subs * rows * d_model * 30, transcendentals=subs * rows * (ff + rows * 16)),
        compiler_params=pltpu.CompilerParams(collective_id=1, has_side_effects=True, vmem_limit_bytes=VMEM_LIMIT),
    )(dy_in, x_all, mid_all, u_all, qkv_all, w2t, w1t, wot, wqt, ln)


def solution(mesh):
    stages = mesh.shape["pp"]
    swap = [(0, 1), (1, 0)]

    def stage_program(x_in, dy_out, w_qkv, b_qkv, w_out, b_out, ln_par, w_fc1, b_fc1, w_fc2, b_fc2):
        micro, batch, rows, d_model = x_in.shape
        heads, width = w_qkv.shape[3:]
        half = heads * width
        subs = micro * batch
        tile = half
        tp_me = lax.axis_index("tp")

        def both_halves(own, axis):
            other = lax.ppermute(own, "tp", swap)
            first = jnp.where(tp_me == 0, own, other)
            second = jnp.where(tp_me == 0, other, own)
            return jnp.concatenate([first, second], axis=axis)

        wq_own = jnp.transpose(w_qkv[0].reshape(3, d_model, half), (1, 0, 2)).reshape(d_model, 3 * half)
        wq = both_halves(wq_own, 1)
        wo = both_halves(w_out[0].reshape(half, d_model), 0)
        bq = both_halves(b_qkv[0].reshape(1, 3 * half), 1).astype(F32)
        w1, w2 = w_fc1[0], w_fc2[0]
        ln = ln_par[0].astype(F32)
        x_all, qkv_all, o_all, mid_all, h1_all, h2_all, u_all, a_all, y_all, _ = fwd_call(
            stages, width, tile, x_in.reshape(subs, rows, d_model), wq, wo, w1, w2, bq, b_out.astype(F32), ln, b_fc1.astype(F32), b_fc2.astype(F32))
        dy_all, dpre_all, gmid_all, dqkv_all, gin_all, _, db1, db2, dbo, dbq, dln = bwd_call(
            stages, width, tile, dy_out.reshape(subs, rows, d_model), x_all, mid_all, u_all, qkv_all, w2.T, w1.T, wo.T, wq.T, ln)

        def weight_grad(left, right):
            return lax.dot_general(left.reshape(subs * rows, -1), right.reshape(subs * rows, -1), (((0,), (0,)), ((), ())), preferred_element_type=F32)

        g_w_fc2 = weight_grad(a_all, dy_all)
        g_w_fc1 = weight_grad(h2_all, dpre_all)
        g_w_out = weight_grad(o_all, gmid_all).reshape(heads, width, d_model)
        g_w_qkv = jnp.transpose(weight_grad(h1_all, dqkv_all).reshape(d_model, 3, heads, width), (1, 0, 2, 3))
        g_b_qkv = lax.dynamic_slice_in_dim(jnp.sum(dbq, axis=0), tp_me * (3 * half), 3 * half).reshape(3, heads, width)
        act = (1, micro, batch, rows, d_model)
        return (y_all.reshape(act), gin_all.reshape(act), g_w_qkv[None], g_b_qkv[None], g_w_out[None], jnp.sum(dbo, axis=0)[None],
                jnp.sum(dln, axis=1)[None], g_w_fc1[None], jnp.sum(db1, axis=0)[None], g_w_fc2[None], jnp.sum(db2, axis=0)[None])

    act_spec = P(None, "dp", None, None)
    arg_specs = (act_spec, act_spec,
                 P("pp", None, None, "tp", None), P("pp", None, "tp", None), P("pp", "tp", None, None),
                 P("pp", None), P("pp", None, None), P("pp", None, "tp"), P("pp", "tp"),
                 P("pp", "tp", None), P("pp", None))
    stage_spec = P("pp", None, "dp", None, None)
    grad_axes = ("dp", "pp")
    result_specs = (stage_spec, stage_spec,
                    P(grad_axes, None, None, "tp", None), P(grad_axes, None, "tp", None), P(grad_axes, "tp", None, None),
                    P(grad_axes, None), P(grad_axes, None, None), P(grad_axes, None, "tp"), P(grad_axes, "tp"),
                    P(grad_axes, "tp", None), P(grad_axes, None))
    return jax.shard_map(stage_program, mesh=mesh, in_specs=arg_specs, out_specs=result_specs, check_vma=False)
```

```python
import functools

import jax
import jax.numpy as jnp
from jax import lax
from jax.experimental import pallas as pl
from jax.experimental.pallas import tpu as pltpu
from jax.sharding import PartitionSpec as P

LN_EPS = 1e-5
F32 = jnp.float32
BF16 = jnp.bfloat16
MESH = pl.DeviceIdType.MESH
NEG = -1e30
ROW_CHUNK = 32
GELU_C = 0.7978845608028654
GELU_K = 0.044715
LOG2_E = 1.4426950408889634
SOFT_ROWS = 64

WINDOWS = ((0, 128, 0), (0, 256, 96), (128, 256, 64), (256, 128, 32))


def dot_nn(lhs, rhs):
    return lax.dot_general(lhs, rhs, (((1,), (0,)), ((), ())), preferred_element_type=F32)


def dot_nt(lhs, rhs):
    return lax.dot_general(lhs, rhs, (((1,), (1,)), ((), ())), preferred_element_type=F32)


def dot_tn(lhs, rhs):
    return lax.dot_general(lhs, rhs, (((0,), (0,)), ((), ())), preferred_element_type=F32)


def head_only(window, offset, width):
    lane = lax.broadcasted_iota(jnp.int32, window.shape, 1)
    return jnp.where((lane >= offset) & (lane < offset + width), window, jnp.zeros_like(window))


def join_heads(parts, width):
    lane = lax.broadcasted_iota(jnp.int32, (parts[0].shape[0], 128), 1)
    first = jnp.where(lane < width, parts[0], parts[1][:, :128])
    second = jnp.where(lane < 2 * width - 128, parts[1][:, 128:], parts[2][:, :128])
    third = jnp.where(lane < 3 * width - 256, parts[2][:, 128:], parts[3])
    return first, second, third


def norm_stats(x_wide):
    centered = x_wide - jnp.mean(x_wide, axis=-1, keepdims=True)
    inv_std = lax.rsqrt(jnp.mean(centered * centered, axis=-1, keepdims=True) + LN_EPS)
    return centered * inv_std, inv_std


def fold_rows(block):
    rows, cols = block.shape
    return jnp.sum(block.reshape(rows // 8, 8, cols), axis=0)


def neighbour_barrier(stage, tp_peer, stages):
    barrier = pltpu.get_barrier_semaphore()
    pl.semaphore_signal(barrier, inc=1, device_id={"tp": tp_peer}, device_id_type=MESH)
    pl.semaphore_signal(barrier, inc=1, device_id={"pp": lax.rem(stage + 1, stages)}, device_id_type=MESH)
    pl.semaphore_signal(barrier, inc=1, device_id={"pp": lax.rem(stage + stages - 1, stages)}, device_id_type=MESH)
    pl.semaphore_wait(barrier, 3)


def fwd_kernel(subs, stages, width, tile,
               x_in, wq_h, wq_p, wo_h, wo_p, w1_h, w2_h, bq, bo, ln, b1, b2,
               x_all, qkv_all, o_all, mid_all, h1_all, h2_all, u_all, a_all, y_all, part_all,
               wq, wo, w1, w2, xb, h1b, qkvb, ob, midb, h2b, ub, ab, partb, rb, yb, sb, pb,
               w_sem, in_sem, out_sem, mid_sem, y_sem, part_send, part_recv, y_send, x_recv):
    stage = lax.axis_index("pp")
    tp_me = lax.axis_index("tp")
    tp_peer = 1 - tp_me
    last_stage = stages - 1
    rows, d_model = xb.shape
    half = d_model // 2
    ff = ub.shape[1]
    scale = width ** -0.5
    log2_scale = scale * LOG2_E

    mine = pl.ds(pl.multiple_of(tp_me * half, 128), half)
    theirs = pl.ds(pl.multiple_of(tp_peer * half, 128), half)
    mine_q = pl.ds(pl.multiple_of(tp_me * (3 * half), 128), 3 * half)
    theirs_q = pl.ds(pl.multiple_of(tp_peer * (3 * half), 128), 3 * half)
    loads = [pltpu.make_async_copy(src, dst, w_sem.at[i]) for i, (src, dst) in enumerate((
        (wq_h, wq.at[:, mine_q]), (wq_p, wq.at[:, theirs_q]), (wo_h, wo.at[mine, :]), (wo_p, wo.at[theirs, :]), (w1_h, w1), (w2_h, w2)))]
    for load in loads:
        load.start()
    pb[:, :, 0:128, 128:rows] = jnp.zeros((2, 4, 128, rows - 128), BF16)
    neighbour_barrier(stage, tp_peer, stages)

    def outs(m):
        return (pltpu.make_async_copy(h1b, h1_all.at[m], out_sem.at[0]),
                pltpu.make_async_copy(qkvb, qkv_all.at[m], out_sem.at[1]),
                pltpu.make_async_copy(ob.at[:, pl.ds(pl.multiple_of(tp_me * half, 128), half)], o_all.at[m], out_sem.at[2]),
                pltpu.make_async_copy(h2b, h2_all.at[m], out_sem.at[3]),
                pltpu.make_async_copy(ub, u_all.at[m], out_sem.at[4]),
                pltpu.make_async_copy(ab, a_all.at[m], out_sem.at[5]),
                pltpu.make_async_copy(xb, x_all.at[m], out_sem.at[6]))

    def mid_out(m):
        slot = lax.rem(m, 2)
        return pltpu.make_async_copy(midb.at[slot], mid_all.at[m], mid_sem.at[slot])

    def y_out(m):
        slot = lax.rem(m, 2)
        return pltpu.make_async_copy(yb.at[slot], y_all.at[m], y_sem.at[slot])

    def part_copy(m):
        slot = lax.rem(m, 2)
        return pltpu.make_async_remote_copy(src_ref=partb.at[slot], dst_ref=part_all.at[m], send_sem=part_send.at[slot], recv_sem=part_recv.at[m],
                                            device_id={"tp": tp_peer}, device_id_type=MESH)

    def next_copy(m):
        slot = lax.rem(m, 2)
        return pltpu.make_async_remote_copy(src_ref=yb.at[slot], dst_ref=x_all.at[m], send_sem=y_send.at[slot], recv_sem=x_recv.at[m],
                                            device_id={"pp": jnp.minimum(stage + 1, last_stage)}, device_id_type=MESH)

    def layer_norm(src, dst, gain, shift):
        for r in range(0, rows, ROW_CHUNK):
            normed, _ = norm_stats(src[r:r + ROW_CHUNK, :].astype(F32))
            dst[r:r + ROW_CHUNK, :] = (normed * gain + shift).astype(BF16)

    def group_base(group):
        return (group // 2) * (3 * half) + (group % 2) * (4 * width)

    def attend():
        def scores(group):
            base = group_base(group)
            for j, (start, size, offset) in enumerate(WINDOWS):
                query = head_only(qkvb[:, base + start:base + start + size], offset, width)
                key = qkvb[:, base + half + start:base + half + start + size]
                sb[group % 2, j] = dot_nt(query, key)

        def softmax(group):
            for j in range(4):
                for r0 in range(0, rows, SOFT_ROWS):
                    keys = 128 * (r0 // 128 + 1)
                    row = lax.broadcasted_iota(jnp.int32, (SOFT_ROWS, keys), 0) + r0
                    col = lax.broadcasted_iota(jnp.int32, (SOFT_ROWS, keys), 1)
                    score = jnp.where(row >= col, sb[group % 2, j, r0:r0 + SOFT_ROWS, 0:keys], NEG)
                    weight = jnp.exp2((score - jnp.max(score, axis=1, keepdims=True)) * log2_scale)
                    inv = 1.0 / jnp.sum(weight, axis=1, keepdims=True)
                    pb[group % 2, j, r0:r0 + SOFT_ROWS, 0:keys] = (weight * inv).astype(BF16)

        def values(group):
            base = group_base(group) + 2 * half
            parts = [dot_nn(pb[group % 2, j], qkvb[:, base + start:base + start + size]) for j, (start, size, _) in enumerate(WINDOWS)]
            for i, piece in enumerate(join_heads(parts, width)):
                first = group * (4 * width) + i * 128
                ob[:, first:first + 128] = piece.astype(BF16)

        groups = d_model // (4 * width)
        scores(0)
        for group in range(groups):
            if group + 1 < groups:
                scores(group + 1)
            softmax(group)
            values(group)

    def finish(m):
        slot = lax.rem(m, 2)
        part_copy(m).wait_recv()
        load = pltpu.make_async_copy(part_all.at[m], rb, in_sem)
        load.start()

        @pl.when(m >= 2)
        def _():
            y_out(m - 2).wait()

            @pl.when(stage < last_stage)
            def _():
                next_copy(m - 2).wait_send()

        load.wait()
        for r in range(0, rows, ROW_CHUNK):
            both = partb[slot, r:r + ROW_CHUNK, :].astype(F32) + rb[r:r + ROW_CHUNK, :].astype(F32)
            yb[slot, r:r + ROW_CHUNK, :] = (midb[slot, r:r + ROW_CHUNK, :].astype(F32) + both + b2[...]).astype(BF16)

        @pl.when(stage < last_stage)
        def _():
            next_copy(m).start()

        y_out(m).start()
        part_copy(m).wait_send()

    def one_sub(m):
        slot = lax.rem(m, 2)
        prev = jnp.maximum(m - 1, 0)
        h1_o, qkv_o, o_o, h2_o, u_o, a_o, x_o = outs(m)
        h1_p, qkv_p, o_p, h2_p, u_p, a_p, x_p = outs(prev)

        @pl.when(stage == 0)
        def _():
            @pl.when(m > 0)
            def _():
                x_p.wait()

            load = pltpu.make_async_copy(x_in.at[m], xb, in_sem)
            load.start()
            load.wait()
            x_o.start()

        @pl.when(stage > 0)
        def _():
            next_copy(m).wait_recv()
            load = pltpu.make_async_copy(x_all.at[m], xb, in_sem)
            load.start()
            load.wait()

        @pl.when(m > 0)
        def _():
            h1_p.wait()
            qkv_p.wait()
            o_p.wait()
            h2_p.wait()

        layer_norm(xb, h1b, ln[0:1, :], ln[1:2, :])
        h1_o.start()

        @pl.when(m == 0)
        def _():
            loads[0].wait()
            loads[1].wait()

        for n in range(0, 3 * d_model, tile):
            qkvb[:, n:n + tile] = (dot_nn(h1b[...], wq[:, n:n + tile]) + bq[:, n:n + tile]).astype(BF16)
        qkv_o.start()
        attend()
        o_o.start()

        @pl.when(m == 0)
        def _():
            for load in loads[2:]:
                load.wait()

        @pl.when(m >= 2)
        def _():
            mid_out(m - 2).wait()

        for n in range(0, d_model, tile):
            midb[slot, :, n:n + tile] = (xb[:, n:n + tile].astype(F32) + dot_nn(ob[...], wo[:, n:n + tile]) + bo[:, n:n + tile]).astype(BF16)
        mid_out(m).start()
        layer_norm(midb.at[slot], h2b, ln[2:3, :], ln[3:4, :])
        h2_o.start()

        @pl.when(m > 0)
        def _():
            u_p.wait()
            a_p.wait()

        for n in range(0, ff, tile):
            pre = dot_nn(h2b[...], w1[:, n:n + tile]) + b1[:, n:n + tile]
            ub[:, n:n + tile] = pre
            cdf = 0.5 * (1.0 + jnp.tanh(GELU_C * (pre + GELU_K * (pre * pre * pre))))
            ab[:, n:n + tile] = (pre * cdf).astype(BF16)
        u_o.start()
        a_o.start()
        for n in range(0, d_model, tile):
            partb[slot, :, n:n + tile] = dot_nn(ab[...], w2[:, n:n + tile]).astype(BF16)
        part_copy(m).start()

    def step(m, carry):
        @pl.when(m < subs)
        def _():
            one_sub(m)

        @pl.when(m > 0)
        def _():
            finish(m - 1)

        return carry

    lax.fori_loop(0, subs + 1, step, 0)
    h1_o, qkv_o, o_o, h2_o, u_o, a_o, x_o = outs(subs - 1)
    for copy in (h1_o, qkv_o, o_o, h2_o, u_o, a_o):
        copy.wait()

    @pl.when(stage == 0)
    def _():
        x_o.wait()

    for m in (subs - 2, subs - 1):
        mid_out(m).wait()
        y_out(m).wait()

        @pl.when(stage < last_stage)
        def _():
            next_copy(m).wait_send()


def bwd_kernel(subs, stages, width, tile,
               dy_in, x_all, mid_all, u_all, qkv_all, w2t_h, w1t_h, wot_h, wot_p, wqt_h, wqt_p, ln,
               dy_all, dpre_all, gmid_all, dqkv_all, gin_all, part_all, db1, db2, dbo, dbq, dln,
               w2t, w1t, wot, wqt, dyb, ub, dpb, partb, rb, midb, xb, gmb, qkvb, gib, sb, db, pb, dsb,
               w_sem, in_sem, pre_sem, out_sem, dy_sem, gi_sem, part_send, part_recv, gi_send, dy_recv):
    stage = lax.axis_index("pp")
    tp_me = lax.axis_index("tp")
    tp_peer = 1 - tp_me
    last_stage = stages - 1
    rows, d_model = xb.shape
    half = d_model // 2
    ff = ub.shape[1]
    scale = width ** -0.5
    log2_scale = scale * LOG2_E

    mine = pl.ds(pl.multiple_of(tp_me * half, 128), half)
    theirs = pl.ds(pl.multiple_of(tp_peer * half, 128), half)
    mine_q = pl.ds(pl.multiple_of(tp_me * (3 * half), 128), 3 * half)
    theirs_q = pl.ds(pl.multiple_of(tp_peer * (3 * half), 128), 3 * half)
    loads = [pltpu.make_async_copy(src, dst, w_sem.at[i]) for i, (src, dst) in enumerate((
        (w2t_h, w2t), (w1t_h, w1t), (wot_h, wot.at[:, mine]), (wot_p, wot.at[:, theirs]), (wqt_h, wqt.at[mine_q, :]), (wqt_p, wqt.at[theirs_q, :])))]
    for load in loads:
        load.start()

    def fetch(m):
        return (pltpu.make_async_copy(u_all.at[m], ub, pre_sem.at[0]),
                pltpu.make_async_copy(mid_all.at[m], midb, pre_sem.at[1]),
                pltpu.make_async_copy(qkv_all.at[m], qkvb, pre_sem.at[2]),
                pltpu.make_async_copy(x_all.at[m], xb, pre_sem.at[3]))

    for copy in fetch(0):
        copy.start()
    for acc in (db1, db2, dbo, dbq, dln):
        acc[...] = jnp.zeros_like(acc)
    for acc in (pb, dsb):
        acc[:, 128:rows, 0:128] = jnp.zeros((4, rows - 128, 128), BF16)
    neighbour_barrier(stage, tp_peer, stages)

    def outs(m):
        return (pltpu.make_async_copy(dpb, dpre_all.at[m], out_sem.at[0]),
                pltpu.make_async_copy(gmb, gmid_all.at[m], out_sem.at[1]),
                pltpu.make_async_copy(qkvb.at[:, pl.ds(pl.multiple_of(tp_me * (3 * half), 128), 3 * half)], dqkv_all.at[m], out_sem.at[2]))

    def dy_out(m):
        slot = lax.rem(m, 2)
        return pltpu.make_async_copy(dyb.at[slot], dy_all.at[m], dy_sem.at[slot])

    def gi_out(m):
        slot = lax.rem(m, 2)
        return pltpu.make_async_copy(gib.at[slot], gin_all.at[m], gi_sem.at[slot])

    def part_copy(m):
        slot = lax.rem(m, 2)
        return pltpu.make_async_remote_copy(src_ref=partb.at[slot], dst_ref=part_all.at[m], send_sem=part_send.at[slot], recv_sem=part_recv.at[m],
                                            device_id={"tp": tp_peer}, device_id_type=MESH)

    def prev_copy(m):
        slot = lax.rem(m, 2)
        return pltpu.make_async_remote_copy(src_ref=gib.at[slot], dst_ref=dy_all.at[m], send_sem=gi_send.at[slot], recv_sem=dy_recv.at[m],
                                            device_id={"pp": jnp.maximum(stage - 1, 0)}, device_id_type=MESH)

    def norm_grad(x_rows, grad, gain, which):
        normed, inv_std = norm_stats(x_rows)
        dln[which] += fold_rows(grad * normed)
        dln[which + 1] += fold_rows(grad)
        scaled = grad * gain
        mean_scaled = jnp.mean(scaled, axis=-1, keepdims=True)
        mean_proj = jnp.mean(scaled * normed, axis=-1, keepdims=True)
        return inv_std * (scaled - mean_scaled - normed * mean_proj)

    def mlp_part(m):
        slot = lax.rem(m, 2)
        u_f = fetch(m)[0]

        @pl.when(stage == last_stage)
        def _():
            @pl.when(m >= 2)
            def _():
                dy_out(m - 2).wait()

            load = pltpu.make_async_copy(dy_in.at[m], dyb.at[slot], in_sem)
            load.start()
            load.wait()
            dy_out(m).start()

        @pl.when(stage < last_stage)
        def _():
            prev_copy(m).wait_recv()
            load = pltpu.make_async_copy(dy_all.at[m], dyb.at[slot], in_sem)
            load.start()
            load.wait()

        @pl.when(m == 0)
        def _():
            loads[0].wait()
            loads[1].wait()

        @pl.when(m > 0)
        def _():
            outs(m - 1)[0].wait()

        u_f.wait()
        for r in range(0, rows, ROW_CHUNK):
            db2[...] += fold_rows(dyb[slot, r:r + ROW_CHUNK, :].astype(F32))
        for n in range(0, ff, tile):
            grad = dot_nn(dyb[slot], w2t[:, n:n + tile]).astype(BF16).astype(F32)
            pre = ub[:, n:n + tile]
            square = pre * pre
            bend = jnp.tanh(GELU_C * (pre + GELU_K * (square * pre)))
            slope = 0.5 * (1.0 + bend) + (0.5 * GELU_C) * pre * (1.0 - bend * bend) * (1.0 + (3.0 * GELU_K) * square)
            grad = grad * slope
            db1[:, n:n + tile] += fold_rows(grad)
            dpb[:, n:n + tile] = grad.astype(BF16)
        outs(m)[0].start()

        @pl.when(m + 1 < subs)
        def _():
            fetch(m + 1)[0].start()

        for n in range(0, d_model, tile):
            partb[slot, :, n:n + tile] = dot_nn(dpb[...], w1t[:, n:n + tile]).astype(BF16)
        part_copy(m).start()

    def attend_grad():
        def window(base, spec):
            start, size, offset = spec
            return slice(base + start, base + start + size), offset

        def scores(group, base):
            for j, spec in enumerate(WINDOWS):
                q_lanes, offset = window(base, spec)
                k_lanes, _ = window(base + half, spec)
                v_lanes, _ = window(base + 2 * half, spec)
                d_lanes, _ = window(group * (4 * width), spec)
                sb[j] = dot_nt(qkvb[:, k_lanes], head_only(qkvb[:, q_lanes], offset, width))
                db[j] = dot_nt(qkvb[:, v_lanes], head_only(rb[:, d_lanes], offset, width))

        def softmax():
            for j in range(4):
                for q0 in range(0, rows, 128):
                    keys, lanes = q0 + 128, slice(q0, q0 + 128)
                    krow = lax.broadcasted_iota(jnp.int32, (keys, 128), 0)
                    qcol = lax.broadcasted_iota(jnp.int32, (keys, 128), 1) + q0
                    score = jnp.where(qcol >= krow, sb[j, 0:keys, lanes], NEG)
                    weight = jnp.exp2((score - jnp.max(score, axis=0, keepdims=True)) * log2_scale)
                    prob = weight * (1.0 / jnp.sum(weight, axis=0, keepdims=True))
                    pb[j, 0:keys, lanes] = prob.astype(BF16)
                    d_prob = db[j, 0:keys, lanes]
                    d_score = prob * (d_prob - jnp.sum(prob * d_prob, axis=0, keepdims=True))
                    dsb[j, 0:keys, lanes] = d_score.astype(BF16)

        def products(group, base):
            d_query, d_key, d_value = [], [], []
            for j, spec in enumerate(WINDOWS):
                q_lanes, _ = window(base, spec)
                k_lanes, _ = window(base + half, spec)
                d_lanes, _ = window(group * (4 * width), spec)
                d_value.append(dot_nn(pb[j], rb[:, d_lanes]))
                d_key.append(dot_nn(dsb[j], qkvb[:, q_lanes]) * scale)
                d_query.append(dot_tn(dsb[j], qkvb[:, k_lanes]) * scale)
            for c, parts in enumerate((d_query, d_key, d_value)):
                for i, piece in enumerate(join_heads(parts, width)):
                    piece = piece.astype(BF16)
                    first = base + c * half + i * 128
                    qkvb[:, first:first + 128] = piece
                    dbq[:, first:first + 128] += fold_rows(piece.astype(F32))

        for group in range(d_model // (4 * width)):
            base = (group // 2) * (3 * half) + (group % 2) * (4 * width)
            scores(group, base)
            softmax()
            products(group, base)

    def attn_part(m):
        slot = lax.rem(m, 2)
        _, mid_f, qkv_f, x_f = fetch(m)
        _, gm_o, dq_o = outs(m)
        part_copy(m).wait_recv()
        load = pltpu.make_async_copy(part_all.at[m], rb, in_sem)
        load.start()
        mid_f.wait()

        @pl.when(m > 0)
        def _():
            outs(m - 1)[1].wait()

        @pl.when(m == 0)
        def _():
            for load in loads[2:]:
                load.wait()

        load.wait()
        for r in range(0, rows, ROW_CHUNK):
            rr = slice(r, r + ROW_CHUNK)
            grad = (partb[slot, rr, :].astype(F32) + rb[rr, :].astype(F32)).astype(BF16).astype(F32)
            total = dyb[slot, rr, :].astype(F32) + norm_grad(midb[rr, :].astype(F32), grad, ln[2:3, :], 2)
            gmb[rr, :] = total.astype(BF16)
            dbo[...] += fold_rows(total)
        gm_o.start()

        @pl.when(m + 1 < subs)
        def _():
            fetch(m + 1)[1].start()

        for n in range(0, d_model, tile):
            rb[:, n:n + tile] = dot_nn(gmb[...], wot[:, n:n + tile]).astype(BF16)
        qkv_f.wait()
        attend_grad()
        dq_o.start()
        part_copy(m).wait_send()
        for n in range(0, d_model, tile):
            rb[:, n:n + tile] = dot_nn(qkvb[...], wqt[:, n:n + tile]).astype(BF16)
        x_f.wait()

        @pl.when(m >= 2)
        def _():
            gi_out(m - 2).wait()

            @pl.when(stage > 0)
            def _():
                prev_copy(m - 2).wait_send()

        for r in range(0, rows, ROW_CHUNK):
            rr = slice(r, r + ROW_CHUNK)
            total = gmb[rr, :].astype(F32) + norm_grad(xb[rr, :].astype(F32), rb[rr, :].astype(F32), ln[0:1, :], 0)
            gib[slot, rr, :] = total.astype(BF16)

        @pl.when(stage > 0)
        def _():
            prev_copy(m).start()

        gi_out(m).start()
        dq_o.wait()

        @pl.when(m + 1 < subs)
        def _():
            fetch(m + 1)[2].start()
            fetch(m + 1)[3].start()

    def step(m, carry):
        @pl.when(m < subs)
        def _():
            mlp_part(m)

        @pl.when(m > 0)
        def _():
            attn_part(m - 1)

        return carry

    lax.fori_loop(0, subs + 1, step, 0)
    for copy in outs(subs - 1)[:2]:
        copy.wait()
    for m in (subs - 2, subs - 1):
        gi_out(m).wait()

        @pl.when(stage > 0)
        def _():
            prev_copy(m).wait_send()

        @pl.when(stage == last_stage)
        def _():
            dy_out(m).wait()


ANY = pl.BlockSpec(memory_space=pl.ANY)
VMEM = pl.BlockSpec(memory_space=pltpu.VMEM)
DMA = pltpu.SemaphoreType.DMA
VMEM_LIMIT = 67043328


def fwd_call(stages, width, tile, x_in, wq_own, wq_peer, wo_own, wo_peer, w1, w2, bq, bo, ln, b1, b2):
    subs, rows, d_model = x_in.shape
    ff = w1.shape[1]
    half = d_model // 2

    def hbm(cols, dtype=BF16):
        return jax.ShapeDtypeStruct((subs, rows, cols), dtype)

    def buf(cols, dtype=BF16):
        return pltpu.VMEM((rows, cols), dtype)

    def two(cols):
        return pltpu.VMEM((2, rows, cols), BF16)

    weights = 2 * (4 * d_model * d_model + 2 * d_model * ff)
    return pl.pallas_call(
        functools.partial(fwd_kernel, subs, stages, width, tile),
        name="fwd_stage",
        out_shape=(hbm(d_model), hbm(3 * d_model), hbm(half), hbm(d_model), hbm(d_model), hbm(d_model), hbm(ff, F32), hbm(ff), hbm(d_model), hbm(d_model)),
        in_specs=[ANY] * 7 + [VMEM] * 5,
        out_specs=[ANY] * 10,
        scratch_shapes=[
            pltpu.VMEM((d_model, 3 * d_model), BF16), pltpu.VMEM((d_model, d_model), BF16), pltpu.VMEM(w1.shape, BF16), pltpu.VMEM(w2.shape, BF16),
            buf(d_model), buf(d_model), buf(3 * d_model), buf(d_model), two(d_model), buf(d_model), buf(ff, F32), buf(ff), two(d_model), buf(d_model), two(d_model),
            pltpu.VMEM((2, 4, rows, rows), F32), pltpu.VMEM((2, 4, rows, rows), BF16),
            DMA((6,)), DMA, DMA((7,)), DMA((2,)), DMA((2,)), DMA((2,)), DMA((subs,)), DMA((2,)), DMA((subs,)),
        ],
        cost_estimate=pl.CostEstimate(flops=subs * rows * weights, bytes_accessed=weights + subs * rows * d_model * 30, transcendentals=subs * rows * (ff + rows * 16)),
        compiler_params=pltpu.CompilerParams(collective_id=0, has_side_effects=True, vmem_limit_bytes=VMEM_LIMIT),
    )(x_in, wq_own, wq_peer, wo_own, wo_peer, w1, w2, bq, bo, ln, b1, b2)


def bwd_call(stages, width, tile, dy_in, x_all, mid_all, u_all, qkv_all, w2t, w1t, wot_own, wot_peer, wqt_own, wqt_peer, ln):
    subs, rows, d_model = dy_in.shape
    ff = u_all.shape[2]
    half = d_model // 2

    def hbm(cols, dtype=BF16):
        return jax.ShapeDtypeStruct((subs, rows, cols), dtype)

    def buf(cols, dtype=BF16):
        return pltpu.VMEM((rows, cols), dtype)

    def two(cols):
        return pltpu.VMEM((2, rows, cols), BF16)

    def acc(*shape):
        return jax.ShapeDtypeStruct(shape, F32)

    weights = 2 * (4 * d_model * d_model + 2 * d_model * ff)
    return pl.pallas_call(
        functools.partial(bwd_kernel, subs, stages, width, tile),
        name="bwd_stage",
        out_shape=(hbm(d_model), hbm(ff), hbm(d_model), hbm(3 * half), hbm(d_model), hbm(d_model),
                   acc(8, ff), acc(8, d_model), acc(8, d_model), acc(8, 3 * d_model), acc(4, 8, d_model)),
        in_specs=[ANY] * 11 + [VMEM],
        out_specs=[ANY] * 6 + [VMEM] * 5,
        scratch_shapes=[
            pltpu.VMEM(w2t.shape, BF16), pltpu.VMEM(w1t.shape, BF16), pltpu.VMEM((d_model, d_model), BF16), pltpu.VMEM((3 * d_model, d_model), BF16),
            two(d_model), buf(ff, F32), buf(ff), two(d_model), buf(d_model), buf(d_model), buf(d_model), buf(d_model), buf(3 * d_model), two(d_model),
            pltpu.VMEM((4, rows, rows), F32), pltpu.VMEM((4, rows, rows), F32), pltpu.VMEM((4, rows, rows), BF16), pltpu.VMEM((4, rows, rows), BF16),
            DMA((6,)), DMA, DMA((4,)), DMA((3,)), DMA((2,)), DMA((2,)), DMA((2,)), DMA((subs,)), DMA((2,)), DMA((subs,)),
        ],
        cost_estimate=pl.CostEstimate(flops=subs * rows * weights, bytes_accessed=weights + subs * rows * d_model * 30, transcendentals=subs * rows * (ff + rows * 16)),
        compiler_params=pltpu.CompilerParams(collective_id=1, has_side_effects=True, vmem_limit_bytes=VMEM_LIMIT),
    )(dy_in, x_all, mid_all, u_all, qkv_all, w2t, w1t, wot_own, wot_peer, wqt_own, wqt_peer, ln)


def solution(mesh):
    stages = mesh.shape["pp"]
    swap = [(0, 1), (1, 0)]

    def stage_program(x_in, dy_out, w_qkv, b_qkv, w_out, b_out, ln_par, w_fc1, b_fc1, w_fc2, b_fc2):
        micro, batch, rows, d_model = x_in.shape
        heads, width = w_qkv.shape[3:]
        half = heads * width
        subs = micro * batch
        tile = half
        tp_me = lax.axis_index("tp")

        wqt_own = jnp.transpose(w_qkv[0], (0, 2, 3, 1)).reshape(3 * half, d_model)
        wqt_peer = lax.ppermute(wqt_own, "tp", swap)
        wo_own = w_out[0].reshape(half, d_model)
        wo_peer = lax.ppermute(wo_own, "tp", swap)
        bq_own = b_qkv[0].reshape(1, 3 * half)
        bq_peer = lax.ppermute(bq_own, "tp", swap)
        bq = jnp.concatenate([jnp.where(tp_me == 0, bq_own, bq_peer), jnp.where(tp_me == 0, bq_peer, bq_own)], axis=1).astype(F32)
        w1, w2 = w_fc1[0], w_fc2[0]
        ln = ln_par[0].astype(F32)
        x_all, qkv_all, o_all, mid_all, h1_all, h2_all, u_all, a_all, y_all, _ = fwd_call(
            stages, width, tile, x_in.reshape(subs, rows, d_model), wqt_own.T, wqt_peer.T, wo_own, wo_peer, w1, w2, bq, b_out.astype(F32), ln, b_fc1.astype(F32), b_fc2.astype(F32))
        dy_all, dpre_all, gmid_all, dqkv_all, gin_all, _, db1, db2, dbo, dbq, dln = bwd_call(
            stages, width, tile, dy_out.reshape(subs, rows, d_model), x_all, mid_all, u_all, qkv_all, w2.T, w1.T, wo_own.T, wo_peer.T, wqt_own, wqt_peer, ln)

        def weight_grad(left, right):
            product = dot_tn(left.reshape(subs * rows, -1), right.reshape(subs * rows, -1))
            return lax.optimization_barrier(product)

        g_w_fc2 = weight_grad(a_all, dy_all)
        g_w_fc1 = weight_grad(h2_all, dpre_all)
        g_w_out = weight_grad(o_all, gmid_all).reshape(heads, width, d_model)
        g_w_qkv = jnp.transpose(weight_grad(dqkv_all, h1_all).reshape(3, heads, width, d_model), (0, 3, 1, 2))
        g_b_qkv = lax.dynamic_slice_in_dim(jnp.sum(dbq, axis=0), tp_me * (3 * half), 3 * half).reshape(3, heads, width)
        act = (1, micro, batch, rows, d_model)
        return (y_all.reshape(act), gin_all.reshape(act), g_w_qkv[None], g_b_qkv[None], g_w_out[None], jnp.sum(dbo, axis=0)[None],
                jnp.sum(dln, axis=1)[None], g_w_fc1[None], jnp.sum(db1, axis=0)[None], g_w_fc2[None], jnp.sum(db2, axis=0)[None])

    act_spec = P(None, "dp", None, None)
    arg_specs = (act_spec, act_spec,
                 P("pp", None, None, "tp", None), P("pp", None, "tp", None), P("pp", "tp", None, None),
                 P("pp", None), P("pp", None, None), P("pp", None, "tp"), P("pp", "tp"),
                 P("pp", "tp", None), P("pp", None))
    stage_spec = P("pp", None, "dp", None, None)
    grad_axes = ("dp", "pp")
    result_specs = (stage_spec, stage_spec,
                    P(grad_axes, None, None, "tp", None), P(grad_axes, None, "tp", None), P(grad_axes, "tp", None, None),
                    P(grad_axes, None), P(grad_axes, None, None), P(grad_axes, None, "tp"), P(grad_axes, "tp"),
                    P(grad_axes, "tp", None), P(grad_axes, None))
    return jax.shard_map(stage_program, mesh=mesh, in_specs=arg_specs, out_specs=result_specs, check_vma=False)
```

```python
import functools

import jax
import jax.numpy as jnp
from jax import lax
from jax.experimental import pallas as pl
from jax.experimental.pallas import tpu as pltpu
from jax.sharding import PartitionSpec as P

LN_EPS = 1e-5
F32 = jnp.float32
BF16 = jnp.bfloat16
MESH = pl.DeviceIdType.MESH
NEG = -1e30
ROW_CHUNK = 32
GELU_C = 0.7978845608028654
GELU_K = 0.044715
LOG2_E = 1.4426950408889634
SOFT_ROWS = 64
RING = 4

WINDOWS = ((0, 128, 0), (0, 256, 96), (128, 256, 64), (256, 128, 32))


def dot_nn(lhs, rhs):
    return lax.dot_general(lhs, rhs, (((1,), (0,)), ((), ())), preferred_element_type=F32)


def dot_nt(lhs, rhs):
    return lax.dot_general(lhs, rhs, (((1,), (1,)), ((), ())), preferred_element_type=F32)


def dot_tn(lhs, rhs):
    return lax.dot_general(lhs, rhs, (((0,), (0,)), ((), ())), preferred_element_type=F32)


def head_only(window, offset, width):
    lane = lax.broadcasted_iota(jnp.int32, window.shape, 1)
    return jnp.where((lane >= offset) & (lane < offset + width), window, jnp.zeros_like(window))


def join_heads(parts, width):
    lane = lax.broadcasted_iota(jnp.int32, (parts[0].shape[0], 128), 1)
    first = jnp.where(lane < width, parts[0], parts[1][:, :128])
    second = jnp.where(lane < 2 * width - 128, parts[1][:, 128:], parts[2][:, :128])
    third = jnp.where(lane < 3 * width - 256, parts[2][:, 128:], parts[3])
    return first, second, third


def norm_stats(x_wide):
    centered = x_wide - jnp.mean(x_wide, axis=-1, keepdims=True)
    inv_std = lax.rsqrt(jnp.mean(centered * centered, axis=-1, keepdims=True) + LN_EPS)
    return centered * inv_std, inv_std


def fold_rows(block):
    rows, cols = block.shape
    return jnp.sum(block.reshape(rows // 8, 8, cols), axis=0)


def neighbour_barrier(stage, tp_peer, stages):
    barrier = pltpu.get_barrier_semaphore()
    pl.semaphore_signal(barrier, inc=1, device_id={"tp": tp_peer}, device_id_type=MESH)
    pl.semaphore_signal(barrier, inc=1, device_id={"pp": lax.rem(stage + 1, stages)}, device_id_type=MESH)
    pl.semaphore_signal(barrier, inc=1, device_id={"pp": lax.rem(stage + stages - 1, stages)}, device_id_type=MESH)
    pl.semaphore_wait(barrier, 3)


def fwd_kernel(subs, stages, width, tile,
               x_in, wq_h, wq_p, wo_h, wo_p, w1_h, w2_h, bq, bo, ln, b1, b2,
               x_all, qkv_all, o_all, mid_all, h1_all, h2_all, s_all, a_all, y_all,
               wq, wo, w1, w2, xb, h1b, qkvb, ob, midb, h2b, slb, ab, partb, peerb, yb, sb, pb,
               w_sem, in_sem, out_sem, mid_sem, y_sem, part_send, part_recv, y_send, x_recv):
    stage = lax.axis_index("pp")
    tp_me = lax.axis_index("tp")
    tp_peer = 1 - tp_me
    last_stage = stages - 1
    rows, d_model = xb.shape
    half = d_model // 2
    ff = slb.shape[1]
    scale = width ** -0.5
    log2_scale = scale * LOG2_E

    mine = pl.ds(pl.multiple_of(tp_me * half, 128), half)
    theirs = pl.ds(pl.multiple_of(tp_peer * half, 128), half)
    mine_q = pl.ds(pl.multiple_of(tp_me * (3 * half), 128), 3 * half)
    theirs_q = pl.ds(pl.multiple_of(tp_peer * (3 * half), 128), 3 * half)
    loads = [pltpu.make_async_copy(src, dst, w_sem.at[i]) for i, (src, dst) in enumerate((
        (wq_h, wq.at[:, mine_q]), (wq_p, wq.at[:, theirs_q]), (wo_h, wo.at[mine, :]), (wo_p, wo.at[theirs, :]), (w1_h, w1), (w2_h, w2)))]
    for load in loads:
        load.start()
    pb[:, :, 0:128, 128:rows] = jnp.zeros((2, 4, 128, rows - 128), BF16)
    neighbour_barrier(stage, tp_peer, stages)

    def outs(m):
        return (pltpu.make_async_copy(h1b, h1_all.at[m], out_sem.at[0]),
                pltpu.make_async_copy(qkvb, qkv_all.at[m], out_sem.at[1]),
                pltpu.make_async_copy(ob.at[:, pl.ds(pl.multiple_of(tp_me * half, 128), half)], o_all.at[m], out_sem.at[2]),
                pltpu.make_async_copy(h2b, h2_all.at[m], out_sem.at[3]),
                pltpu.make_async_copy(slb, s_all.at[m], out_sem.at[4]),
                pltpu.make_async_copy(ab, a_all.at[m], out_sem.at[5]),
                pltpu.make_async_copy(xb, x_all.at[m], out_sem.at[6]))

    def mid_out(m):
        slot = lax.rem(m, 2)
        return pltpu.make_async_copy(midb.at[slot], mid_all.at[m], mid_sem.at[slot])

    def y_out(m):
        slot = lax.rem(m, 2)
        return pltpu.make_async_copy(yb.at[slot], y_all.at[m], y_sem.at[slot])

    def part_copy(m):
        slot = lax.rem(m, 2)
        return pltpu.make_async_remote_copy(src_ref=partb.at[slot], dst_ref=peerb.at[lax.rem(m, RING)], send_sem=part_send.at[slot], recv_sem=part_recv.at[m],
                                            device_id={"tp": tp_peer}, device_id_type=MESH)

    def next_copy(m):
        slot = lax.rem(m, 2)
        return pltpu.make_async_remote_copy(src_ref=yb.at[slot], dst_ref=x_all.at[m], send_sem=y_send.at[slot], recv_sem=x_recv.at[m],
                                            device_id={"pp": jnp.minimum(stage + 1, last_stage)}, device_id_type=MESH)

    def layer_norm(src, dst, gain, shift):
        for r in range(0, rows, ROW_CHUNK):
            normed, _ = norm_stats(src[r:r + ROW_CHUNK, :].astype(F32))
            dst[r:r + ROW_CHUNK, :] = (normed * gain + shift).astype(BF16)

    def group_base(group):
        return (group // 2) * (3 * half) + (group % 2) * (4 * width)

    def attend():
        def scores(group):
            base = group_base(group)
            for j, (start, size, offset) in enumerate(WINDOWS):
                query = head_only(qkvb[:, base + start:base + start + size], offset, width)
                key = qkvb[:, base + half + start:base + half + start + size]
                sb[group % 2, j] = dot_nt(query, key)

        def softmax(group):
            for j in range(4):
                for r0 in range(0, rows, SOFT_ROWS):
                    keys = 128 * (r0 // 128 + 1)
                    row = lax.broadcasted_iota(jnp.int32, (SOFT_ROWS, keys), 0) + r0
                    col = lax.broadcasted_iota(jnp.int32, (SOFT_ROWS, keys), 1)
                    score = jnp.where(row >= col, sb[group % 2, j, r0:r0 + SOFT_ROWS, 0:keys], NEG)
                    weight = jnp.exp2((score - jnp.max(score, axis=1, keepdims=True)) * log2_scale)
                    inv = 1.0 / jnp.sum(weight, axis=1, keepdims=True)
                    pb[group % 2, j, r0:r0 + SOFT_ROWS, 0:keys] = (weight * inv).astype(BF16)

        def values(group):
            base = group_base(group) + 2 * half
            parts = [dot_nn(pb[group % 2, j], qkvb[:, base + start:base + start + size]) for j, (start, size, _) in enumerate(WINDOWS)]
            for i, piece in enumerate(join_heads(parts, width)):
                first = group * (4 * width) + i * 128
                ob[:, first:first + 128] = piece.astype(BF16)

        groups = d_model // (4 * width)
        scores(0)
        for group in range(groups):
            if group + 1 < groups:
                scores(group + 1)
            softmax(group)
            values(group)

    def finish(m):
        slot = lax.rem(m, 2)
        peer_slot = lax.rem(m, RING)
        part_copy(m).wait_recv()

        @pl.when(m >= 2)
        def _():
            y_out(m - 2).wait()

            @pl.when(stage < last_stage)
            def _():
                next_copy(m - 2).wait_send()

        for r in range(0, rows, ROW_CHUNK):
            both = partb[slot, r:r + ROW_CHUNK, :].astype(F32) + peerb[peer_slot, r:r + ROW_CHUNK, :].astype(F32)
            yb[slot, r:r + ROW_CHUNK, :] = (midb[slot, r:r + ROW_CHUNK, :].astype(F32) + both + b2[...]).astype(BF16)

        @pl.when(stage < last_stage)
        def _():
            next_copy(m).start()

        y_out(m).start()
        part_copy(m).wait_send()

    def one_sub(m):
        slot = lax.rem(m, 2)
        prev = jnp.maximum(m - 1, 0)
        h1_o, qkv_o, o_o, h2_o, s_o, a_o, x_o = outs(m)
        h1_p, qkv_p, o_p, h2_p, s_p, a_p, x_p = outs(prev)

        @pl.when(stage == 0)
        def _():
            @pl.when(m > 0)
            def _():
                x_p.wait()

            load = pltpu.make_async_copy(x_in.at[m], xb, in_sem)
            load.start()
            load.wait()
            x_o.start()

        @pl.when(stage > 0)
        def _():
            next_copy(m).wait_recv()
            load = pltpu.make_async_copy(x_all.at[m], xb, in_sem)
            load.start()
            load.wait()

        @pl.when(m > 0)
        def _():
            h1_p.wait()
            qkv_p.wait()
            o_p.wait()
            h2_p.wait()

        layer_norm(xb, h1b, ln[0:1, :], ln[1:2, :])
        h1_o.start()

        @pl.when(m == 0)
        def _():
            loads[0].wait()
            loads[1].wait()

        for n in range(0, 3 * d_model, tile):
            qkvb[:, n:n + tile] = (dot_nn(h1b[...], wq[:, n:n + tile]) + bq[:, n:n + tile]).astype(BF16)
        qkv_o.start()
        attend()
        o_o.start()

        @pl.when(m == 0)
        def _():
            for load in loads[2:]:
                load.wait()

        @pl.when(m >= 2)
        def _():
            mid_out(m - 2).wait()

        for n in range(0, d_model, tile):
            midb[slot, :, n:n + tile] = (xb[:, n:n + tile].astype(F32) + dot_nn(ob[...], wo[:, n:n + tile]) + bo[:, n:n + tile]).astype(BF16)
        mid_out(m).start()
        layer_norm(midb.at[slot], h2b, ln[2:3, :], ln[3:4, :])
        h2_o.start()

        @pl.when(m > 0)
        def _():
            s_p.wait()
            a_p.wait()

        for n in range(0, ff, tile):
            pre = dot_nn(h2b[...], w1[:, n:n + tile]) + b1[:, n:n + tile]
            square = pre * pre
            bend = jnp.tanh(pre * (GELU_C + (GELU_C * GELU_K) * square))
            cdf = 0.5 + 0.5 * bend
            ab[:, n:n + tile] = (pre * cdf).astype(BF16)
            slb[:, n:n + tile] = cdf + (0.5 * pre) * (1.0 - bend * bend) * (GELU_C + (3.0 * GELU_C * GELU_K) * square)
        s_o.start()
        a_o.start()
        for n in range(0, d_model, tile):
            partb[slot, :, n:n + tile] = dot_nn(ab[...], w2[:, n:n + tile]).astype(BF16)
        part_copy(m).start()

    def step(m, carry):
        @pl.when(m < subs)
        def _():
            one_sub(m)

        @pl.when(m > 0)
        def _():
            finish(m - 1)

        return carry

    lax.fori_loop(0, subs + 1, step, 0)
    h1_o, qkv_o, o_o, h2_o, s_o, a_o, x_o = outs(subs - 1)
    for copy in (h1_o, qkv_o, o_o, h2_o, s_o, a_o):
        copy.wait()

    @pl.when(stage == 0)
    def _():
        x_o.wait()

    for m in (subs - 2, subs - 1):
        mid_out(m).wait()
        y_out(m).wait()

        @pl.when(stage < last_stage)
        def _():
            next_copy(m).wait_send()


def bwd_kernel(subs, stages, width, tile,
               dy_in, x_all, mid_all, s_all, qkv_all, w2t_h, w1t_h, wot_h, wot_p, wqt_h, wqt_p, ln,
               dy_all, dpre_all, gmid_all, dqkv_all, gin_all, db1, db2, dbo, dbq, dln,
               w2t, w1t, wot, wqt, dyb, slb, dpb, partb, peerb, rb, midb, xb, gmb, qkvb, gib, sb, db, pb, dsb,
               w_sem, in_sem, pre_sem, out_sem, dy_sem, gi_sem, part_send, part_recv, gi_send, dy_recv, dy_free):
    stage = lax.axis_index("pp")
    tp_me = lax.axis_index("tp")
    tp_peer = 1 - tp_me
    last_stage = stages - 1
    rows, d_model = xb.shape
    half = d_model // 2
    ff = slb.shape[1]
    scale = width ** -0.5
    log2_scale = scale * LOG2_E

    mine = pl.ds(pl.multiple_of(tp_me * half, 128), half)
    theirs = pl.ds(pl.multiple_of(tp_peer * half, 128), half)
    mine_q = pl.ds(pl.multiple_of(tp_me * (3 * half), 128), 3 * half)
    theirs_q = pl.ds(pl.multiple_of(tp_peer * (3 * half), 128), 3 * half)
    loads = [pltpu.make_async_copy(src, dst, w_sem.at[i]) for i, (src, dst) in enumerate((
        (w2t_h, w2t), (w1t_h, w1t), (wot_h, wot.at[:, mine]), (wot_p, wot.at[:, theirs]), (wqt_h, wqt.at[mine_q, :]), (wqt_p, wqt.at[theirs_q, :])))]
    for load in loads:
        load.start()

    def fetch(m):
        return (pltpu.make_async_copy(s_all.at[m], slb, pre_sem.at[0]),
                pltpu.make_async_copy(mid_all.at[m], midb, pre_sem.at[1]),
                pltpu.make_async_copy(qkv_all.at[m], qkvb, pre_sem.at[2]),
                pltpu.make_async_copy(x_all.at[m], xb, pre_sem.at[3]))

    for copy in fetch(0):
        copy.start()
    for acc in (db1, db2, dbo, dbq, dln):
        acc[...] = jnp.zeros_like(acc)
    for acc in (pb, dsb):
        acc[:, 128:rows, 0:128] = jnp.zeros((4, rows - 128, 128), BF16)
    neighbour_barrier(stage, tp_peer, stages)

    def outs(m):
        return (pltpu.make_async_copy(dpb, dpre_all.at[m], out_sem.at[0]),
                pltpu.make_async_copy(gmb, gmid_all.at[m], out_sem.at[1]),
                pltpu.make_async_copy(qkvb.at[:, pl.ds(pl.multiple_of(tp_me * (3 * half), 128), 3 * half)], dqkv_all.at[m], out_sem.at[2]))

    def dy_load(m):
        return pltpu.make_async_copy(dy_in.at[m], dyb.at[lax.rem(m, RING)], in_sem.at[lax.rem(m, 2)])

    def dy_out(m):
        return pltpu.make_async_copy(dyb.at[lax.rem(m, RING)], dy_all.at[m], dy_sem.at[lax.rem(m, 2)])

    def gi_out(m):
        slot = lax.rem(m, 2)
        return pltpu.make_async_copy(gib.at[slot], gin_all.at[m], gi_sem.at[slot])

    def part_copy(m):
        slot = lax.rem(m, 2)
        return pltpu.make_async_remote_copy(src_ref=partb.at[slot], dst_ref=peerb.at[lax.rem(m, RING)], send_sem=part_send.at[slot], recv_sem=part_recv.at[m],
                                            device_id={"tp": tp_peer}, device_id_type=MESH)

    def prev_copy(m):
        slot = lax.rem(m, 2)
        return pltpu.make_async_remote_copy(src_ref=gib.at[slot], dst_ref=dyb.at[lax.rem(m, RING)], send_sem=gi_send.at[slot], recv_sem=dy_recv.at[m],
                                            device_id={"pp": jnp.maximum(stage - 1, 0)}, device_id_type=MESH)

    @pl.when(stage == last_stage)
    def _():
        dy_load(0).start()

    def norm_grad(x_rows, grad, gain, which):
        normed, inv_std = norm_stats(x_rows)
        dln[which] += fold_rows(grad * normed)
        dln[which + 1] += fold_rows(grad)
        scaled = grad * gain
        mean_scaled = jnp.mean(scaled, axis=-1, keepdims=True)
        mean_proj = jnp.mean(scaled * normed, axis=-1, keepdims=True)
        return inv_std * (scaled - mean_scaled - normed * mean_proj)

    def mlp_part(m):
        slot = lax.rem(m, 2)
        slope_f = fetch(m)[0]

        dy_slot = lax.rem(m, RING)

        @pl.when(stage == last_stage)
        def _():
            dy_load(m).wait()

            @pl.when(m + 1 < subs)
            def _():
                dy_load(m + 1).start()

        @pl.when(stage < last_stage)
        def _():
            prev_copy(m).wait_recv()

        dy_out(m).start()

        @pl.when(m == 0)
        def _():
            loads[0].wait()
            loads[1].wait()

        @pl.when(m > 0)
        def _():
            outs(m - 1)[0].wait()

        slope_f.wait()
        for n in range(0, ff, tile):
            grad = dot_nn(dyb[dy_slot], w2t[:, n:n + tile]).astype(BF16).astype(F32) * slb[:, n:n + tile]
            db1[:, n:n + tile] += fold_rows(grad)
            dpb[:, n:n + tile] = grad.astype(BF16)
        outs(m)[0].start()

        @pl.when(m + 1 < subs)
        def _():
            fetch(m + 1)[0].start()

        for n in range(0, d_model, tile):
            partb[slot, :, n:n + tile] = dot_nn(dpb[...], w1t[:, n:n + tile]).astype(BF16)
        part_copy(m).start()

    def attend_grad():
        def window(base, spec):
            start, size, offset = spec
            return slice(base + start, base + start + size), offset

        def scores(group, base):
            for j, spec in enumerate(WINDOWS):
                q_lanes, offset = window(base, spec)
                k_lanes, _ = window(base + half, spec)
                v_lanes, _ = window(base + 2 * half, spec)
                d_lanes, _ = window(group * (4 * width), spec)
                sb[j] = dot_nt(qkvb[:, k_lanes], head_only(qkvb[:, q_lanes], offset, width))
                db[j] = dot_nt(qkvb[:, v_lanes], head_only(rb[:, d_lanes], offset, width))

        def softmax():
            for j in range(4):
                for q0 in range(0, rows, 128):
                    keys, lanes = q0 + 128, slice(q0, q0 + 128)
                    krow = lax.broadcasted_iota(jnp.int32, (keys, 128), 0)
                    qcol = lax.broadcasted_iota(jnp.int32, (keys, 128), 1) + q0
                    score = jnp.where(qcol >= krow, sb[j, 0:keys, lanes], NEG)
                    weight = jnp.exp2((score - jnp.max(score, axis=0, keepdims=True)) * log2_scale)
                    prob = weight * (1.0 / jnp.sum(weight, axis=0, keepdims=True))
                    pb[j, 0:keys, lanes] = prob.astype(BF16)
                    d_prob = db[j, 0:keys, lanes]
                    d_score = prob * (d_prob - jnp.sum(prob * d_prob, axis=0, keepdims=True))
                    dsb[j, 0:keys, lanes] = d_score.astype(BF16)

        def products(group, base):
            d_query, d_key, d_value = [], [], []
            for j, spec in enumerate(WINDOWS):
                q_lanes, _ = window(base, spec)
                k_lanes, _ = window(base + half, spec)
                d_lanes, _ = window(group * (4 * width), spec)
                d_value.append(dot_nn(pb[j], rb[:, d_lanes]))
                d_key.append(dot_nn(dsb[j], qkvb[:, q_lanes]) * scale)
                d_query.append(dot_tn(dsb[j], qkvb[:, k_lanes]) * scale)
            for c, parts in enumerate((d_query, d_key, d_value)):
                for i, piece in enumerate(join_heads(parts, width)):
                    piece = piece.astype(BF16)
                    first = base + c * half + i * 128
                    qkvb[:, first:first + 128] = piece
                    dbq[:, first:first + 128] += fold_rows(piece.astype(F32))

        for group in range(d_model // (4 * width)):
            base = (group // 2) * (3 * half) + (group % 2) * (4 * width)
            scores(group, base)
            softmax()
            products(group, base)

    def attn_part(m):
        slot = lax.rem(m, 2)
        _, mid_f, qkv_f, x_f = fetch(m)
        _, gm_o, dq_o = outs(m)
        peer_slot = lax.rem(m, RING)
        dy_slot = lax.rem(m, RING)
        mid_f.wait()

        @pl.when(m > 0)
        def _():
            outs(m - 1)[1].wait()

        @pl.when(m == 0)
        def _():
            for load in loads[2:]:
                load.wait()

        part_copy(m).wait_recv()
        for r in range(0, rows, ROW_CHUNK):
            rr = slice(r, r + ROW_CHUNK)
            grad = (partb[slot, rr, :].astype(F32) + peerb[peer_slot, rr, :].astype(F32)).astype(BF16).astype(F32)
            d_y = dyb[dy_slot, rr, :].astype(F32)
            db2[...] += fold_rows(d_y)
            total = d_y + norm_grad(midb[rr, :].astype(F32), grad, ln[2:3, :], 2)
            gmb[rr, :] = total.astype(BF16)
            dbo[...] += fold_rows(total)
        gm_o.start()
        dy_out(m).wait()

        @pl.when((stage < last_stage) & (m < subs - RING))
        def _():
            pl.semaphore_signal(dy_free, inc=1, device_id={"pp": jnp.minimum(stage + 1, last_stage)}, device_id_type=MESH)

        @pl.when(m + 1 < subs)
        def _():
            fetch(m + 1)[1].start()

        for n in range(0, d_model, tile):
            rb[:, n:n + tile] = dot_nn(gmb[...], wot[:, n:n + tile]).astype(BF16)
        qkv_f.wait()
        attend_grad()
        dq_o.start()
        part_copy(m).wait_send()
        for n in range(0, d_model, tile):
            rb[:, n:n + tile] = dot_nn(qkvb[...], wqt[:, n:n + tile]).astype(BF16)
        x_f.wait()

        @pl.when(m >= 2)
        def _():
            gi_out(m - 2).wait()

            @pl.when(stage > 0)
            def _():
                prev_copy(m - 2).wait_send()

        for r in range(0, rows, ROW_CHUNK):
            rr = slice(r, r + ROW_CHUNK)
            total = gmb[rr, :].astype(F32) + norm_grad(xb[rr, :].astype(F32), rb[rr, :].astype(F32), ln[0:1, :], 0)
            gib[slot, rr, :] = total.astype(BF16)

        @pl.when(stage > 0)
        def _():
            @pl.when(m >= RING)
            def _():
                pl.semaphore_wait(dy_free, 1)

            prev_copy(m).start()

        gi_out(m).start()
        dq_o.wait()

        @pl.when(m + 1 < subs)
        def _():
            fetch(m + 1)[2].start()
            fetch(m + 1)[3].start()

    def step(m, carry):
        @pl.when(m < subs)
        def _():
            mlp_part(m)

        @pl.when(m > 0)
        def _():
            attn_part(m - 1)

        return carry

    lax.fori_loop(0, subs + 1, step, 0)
    for copy in outs(subs - 1)[:2]:
        copy.wait()
    for m in (subs - 2, subs - 1):
        gi_out(m).wait()

        @pl.when(stage > 0)
        def _():
            prev_copy(m).wait_send()


ANY = pl.BlockSpec(memory_space=pl.ANY)
VMEM = pl.BlockSpec(memory_space=pltpu.VMEM)
DMA = pltpu.SemaphoreType.DMA
VMEM_LIMIT = 67043328


def fwd_call(stages, width, tile, x_in, wq_own, wq_peer, wo_own, wo_peer, w1, w2, bq, bo, ln, b1, b2):
    subs, rows, d_model = x_in.shape
    ff = w1.shape[1]
    half = d_model // 2

    def hbm(cols, dtype=BF16):
        return jax.ShapeDtypeStruct((subs, rows, cols), dtype)

    def buf(cols, dtype=BF16):
        return pltpu.VMEM((rows, cols), dtype)

    def two(cols):
        return pltpu.VMEM((2, rows, cols), BF16)

    weights = 2 * (4 * d_model * d_model + 2 * d_model * ff)
    return pl.pallas_call(
        functools.partial(fwd_kernel, subs, stages, width, tile),
        name="fwd_stage",
        out_shape=(hbm(d_model), hbm(3 * d_model), hbm(half), hbm(d_model), hbm(d_model), hbm(d_model), hbm(ff, F32), hbm(ff), hbm(d_model)),
        in_specs=[ANY] * 7 + [VMEM] * 5,
        out_specs=[ANY] * 9,
        scratch_shapes=[
            pltpu.VMEM((d_model, 3 * d_model), BF16), pltpu.VMEM((d_model, d_model), BF16), pltpu.VMEM(w1.shape, BF16), pltpu.VMEM(w2.shape, BF16),
            buf(d_model), buf(d_model), buf(3 * d_model), buf(d_model), two(d_model), buf(d_model), buf(ff, F32), buf(ff), two(d_model), pltpu.VMEM((RING, rows, d_model), BF16), two(d_model),
            pltpu.VMEM((2, 4, rows, rows), F32), pltpu.VMEM((2, 4, rows, rows), BF16),
            DMA((6,)), DMA, DMA((7,)), DMA((2,)), DMA((2,)), DMA((2,)), DMA((subs,)), DMA((2,)), DMA((subs,)),
        ],
        cost_estimate=pl.CostEstimate(flops=subs * rows * weights, bytes_accessed=weights + subs * rows * d_model * 30, transcendentals=subs * rows * (ff + rows * 16)),
        compiler_params=pltpu.CompilerParams(collective_id=0, has_side_effects=True, vmem_limit_bytes=VMEM_LIMIT),
    )(x_in, wq_own, wq_peer, wo_own, wo_peer, w1, w2, bq, bo, ln, b1, b2)


def bwd_call(stages, width, tile, dy_in, x_all, mid_all, s_all, qkv_all, w2t, w1t, wot_own, wot_peer, wqt_own, wqt_peer, ln):
    subs, rows, d_model = dy_in.shape
    ff = s_all.shape[2]
    half = d_model // 2

    def hbm(cols, dtype=BF16):
        return jax.ShapeDtypeStruct((subs, rows, cols), dtype)

    def buf(cols, dtype=BF16):
        return pltpu.VMEM((rows, cols), dtype)

    def two(cols):
        return pltpu.VMEM((2, rows, cols), BF16)

    ring = pltpu.VMEM((RING, rows, d_model), BF16)

    def acc(*shape):
        return jax.ShapeDtypeStruct(shape, F32)

    weights = 2 * (4 * d_model * d_model + 2 * d_model * ff)
    return pl.pallas_call(
        functools.partial(bwd_kernel, subs, stages, width, tile),
        name="bwd_stage",
        out_shape=(hbm(d_model), hbm(ff), hbm(d_model), hbm(3 * half), hbm(d_model),
                   acc(8, ff), acc(8, d_model), acc(8, d_model), acc(8, 3 * d_model), acc(4, 8, d_model)),
        in_specs=[ANY] * 11 + [VMEM],
        out_specs=[ANY] * 5 + [VMEM] * 5,
        scratch_shapes=[
            pltpu.VMEM(w2t.shape, BF16), pltpu.VMEM(w1t.shape, BF16), pltpu.VMEM((d_model, d_model), BF16), pltpu.VMEM((3 * d_model, d_model), BF16),
            ring, buf(ff, F32), buf(ff), two(d_model), ring, buf(d_model), buf(d_model), buf(d_model), buf(d_model), buf(3 * d_model), two(d_model),
            pltpu.VMEM((4, rows, rows), F32), pltpu.VMEM((4, rows, rows), F32), pltpu.VMEM((4, rows, rows), BF16), pltpu.VMEM((4, rows, rows), BF16),
            DMA((6,)), DMA((2,)), DMA((4,)), DMA((3,)), DMA((2,)), DMA((2,)), DMA((2,)), DMA((subs,)), DMA((2,)), DMA((subs,)), pltpu.SemaphoreType.REGULAR,
        ],
        cost_estimate=pl.CostEstimate(flops=subs * rows * weights, bytes_accessed=weights + subs * rows * d_model * 30, transcendentals=subs * rows * (ff + rows * 16)),
        compiler_params=pltpu.CompilerParams(collective_id=1, has_side_effects=True, vmem_limit_bytes=VMEM_LIMIT),
    )(dy_in, x_all, mid_all, s_all, qkv_all, w2t, w1t, wot_own, wot_peer, wqt_own, wqt_peer, ln)


def solution(mesh):
    stages = mesh.shape["pp"]
    swap = [(0, 1), (1, 0)]

    def stage_program(x_in, dy_out, w_qkv, b_qkv, w_out, b_out, ln_par, w_fc1, b_fc1, w_fc2, b_fc2):
        micro, batch, rows, d_model = x_in.shape
        heads, width = w_qkv.shape[3:]
        half = heads * width
        subs = micro * batch
        tile = half
        tp_me = lax.axis_index("tp")

        wqt_own = jnp.transpose(w_qkv[0], (0, 2, 3, 1)).reshape(3 * half, d_model)
        wo_own = w_out[0].reshape(half, d_model)
        wo_peer = lax.ppermute(wo_own, "tp", swap)
        wqt_peer = lax.ppermute(wqt_own, "tp", swap)
        bq_own = b_qkv[0].reshape(1, 3 * half)
        bq_peer = lax.ppermute(bq_own, "tp", swap)
        bq = jnp.concatenate([jnp.where(tp_me == 0, bq_own, bq_peer), jnp.where(tp_me == 0, bq_peer, bq_own)], axis=1).astype(F32)
        w1, w2 = w_fc1[0], w_fc2[0]
        ln = ln_par[0].astype(F32)
        x_all, qkv_all, o_all, mid_all, h1_all, h2_all, s_all, a_all, y_all = fwd_call(
            stages, width, tile, x_in.reshape(subs, rows, d_model), wqt_own.T, wqt_peer.T, wo_own, wo_peer, w1, w2, bq, b_out.astype(F32), ln, b_fc1.astype(F32), b_fc2.astype(F32))
        dy_all, dpre_all, gmid_all, dqkv_all, gin_all, db1, db2, dbo, dbq, dln = bwd_call(
            stages, width, tile, dy_out.reshape(subs, rows, d_model), x_all, mid_all, s_all, qkv_all, w2.T, w1.T, wo_own.T, wo_peer.T, wqt_own, wqt_peer, ln)

        def weight_grad(left, right):
            product = dot_tn(left.reshape(subs * rows, -1), right.reshape(subs * rows, -1))
            return lax.optimization_barrier(product)

        g_w_fc2 = weight_grad(a_all, dy_all)
        g_w_fc1 = weight_grad(h2_all, dpre_all)
        g_w_out = weight_grad(o_all, gmid_all).reshape(heads, width, d_model)
        g_w_qkv = jnp.transpose(weight_grad(dqkv_all, h1_all).reshape(3, heads, width, d_model), (0, 3, 1, 2))
        g_b_qkv = lax.dynamic_slice_in_dim(jnp.sum(dbq, axis=0), tp_me * (3 * half), 3 * half).reshape(3, heads, width)
        act = (1, micro, batch, rows, d_model)
        return (y_all.reshape(act), gin_all.reshape(act), g_w_qkv[None], g_b_qkv[None], g_w_out[None], jnp.sum(dbo, axis=0)[None],
                jnp.sum(dln, axis=1)[None], g_w_fc1[None], jnp.sum(db1, axis=0)[None], g_w_fc2[None], jnp.sum(db2, axis=0)[None])

    act_spec = P(None, "dp", None, None)
    arg_specs = (act_spec, act_spec,
                 P("pp", None, None, "tp", None), P("pp", None, "tp", None), P("pp", "tp", None, None),
                 P("pp", None), P("pp", None, None), P("pp", None, "tp"), P("pp", "tp"),
                 P("pp", "tp", None), P("pp", None))
    stage_spec = P("pp", None, "dp", None, None)
    grad_axes = ("dp", "pp")
    result_specs = (stage_spec, stage_spec,
                    P(grad_axes, None, None, "tp", None), P(grad_axes, None, "tp", None), P(grad_axes, "tp", None, None),
                    P(grad_axes, None), P(grad_axes, None, None), P(grad_axes, None, "tp"), P(grad_axes, "tp"),
                    P(grad_axes, "tp", None), P(grad_axes, None))
    return jax.shard_map(stage_program, mesh=mesh, in_specs=arg_specs, out_specs=result_specs, check_vma=False)
```

```python
import functools

import jax
import jax.numpy as jnp
from jax import lax
from jax.experimental import pallas as pl
from jax.experimental.pallas import tpu as pltpu
from jax.sharding import PartitionSpec as P

LN_EPS = 1e-5
F32 = jnp.float32
BF16 = jnp.bfloat16
MESH = pl.DeviceIdType.MESH
NEG = -1e30
ROW_CHUNK = 32
GELU_C = 0.7978845608028654
GELU_K = 0.044715
LOG2_E = 1.4426950408889634
SOFT_ROWS = 64
RING = 4

WINDOWS = ((0, 128, 0), (0, 256, 96), (128, 256, 64), (256, 128, 32))


def dot_nn(lhs, rhs):
    return lax.dot_general(lhs, rhs, (((1,), (0,)), ((), ())), preferred_element_type=F32)


def dot_nt(lhs, rhs):
    return lax.dot_general(lhs, rhs, (((1,), (1,)), ((), ())), preferred_element_type=F32)


def dot_tn(lhs, rhs):
    return lax.dot_general(lhs, rhs, (((0,), (0,)), ((), ())), preferred_element_type=F32)


def head_only(window, offset, width):
    lane = lax.broadcasted_iota(jnp.int32, window.shape, 1)
    return jnp.where((lane >= offset) & (lane < offset + width), window, jnp.zeros_like(window))


def join_heads(parts, width):
    lane = lax.broadcasted_iota(jnp.int32, (parts[0].shape[0], 128), 1)
    first = jnp.where(lane < width, parts[0], parts[1][:, :128])
    second = jnp.where(lane < 2 * width - 128, parts[1][:, 128:], parts[2][:, :128])
    third = jnp.where(lane < 3 * width - 256, parts[2][:, 128:], parts[3])
    return first, second, third


def norm_stats(x_wide):
    centered = x_wide - jnp.mean(x_wide, axis=-1, keepdims=True)
    inv_std = lax.rsqrt(jnp.mean(centered * centered, axis=-1, keepdims=True) + LN_EPS)
    return centered * inv_std, inv_std


def fold_rows(block):
    rows, cols = block.shape
    return jnp.sum(block.reshape(rows // 8, 8, cols), axis=0)


def neighbour_barrier(stage, tp_peer, stages):
    barrier = pltpu.get_barrier_semaphore()
    pl.semaphore_signal(barrier, inc=1, device_id={"tp": tp_peer}, device_id_type=MESH)
    pl.semaphore_signal(barrier, inc=1, device_id={"pp": lax.rem(stage + 1, stages)}, device_id_type=MESH)
    pl.semaphore_signal(barrier, inc=1, device_id={"pp": lax.rem(stage + stages - 1, stages)}, device_id_type=MESH)
    pl.semaphore_wait(barrier, 3)


def fwd_kernel(subs, stages, width, tile,
               x_in, wq_h, wq_p, wo_h, wo_p, w1_h, w2_h, bq, bo, ln, b1, b2,
               x_all, qkv_all, o_all, mid_all, h1_all, h2_all, s_all, a_all, y_all,
               wq, wo, w1, w2, xb, h1b, qkvb, ob, midb, h2b, slb, ab, partb, peerb, yb, sb, pb,
               w_sem, in_sem, out_sem, mid_sem, y_sem, part_send, part_recv, y_send, x_recv):
    stage = lax.axis_index("pp")
    tp_me = lax.axis_index("tp")
    tp_peer = 1 - tp_me
    last_stage = stages - 1
    rows, d_model = xb.shape
    half = d_model // 2
    ff = slb.shape[1]
    scale = width ** -0.5
    log2_scale = scale * LOG2_E

    mine = pl.ds(pl.multiple_of(tp_me * half, 128), half)
    theirs = pl.ds(pl.multiple_of(tp_peer * half, 128), half)
    mine_q = pl.ds(pl.multiple_of(tp_me * (3 * half), 128), 3 * half)
    theirs_q = pl.ds(pl.multiple_of(tp_peer * (3 * half), 128), 3 * half)
    loads = [pltpu.make_async_copy(src, dst, w_sem.at[i]) for i, (src, dst) in enumerate((
        (wq_h, wq.at[:, mine_q]), (wq_p, wq.at[:, theirs_q]), (wo_h, wo.at[mine, :]), (wo_p, wo.at[theirs, :]), (w1_h, w1), (w2_h, w2)))]
    for load in loads:
        load.start()
    pb[:, :, 0:128, 128:rows] = jnp.zeros((2, 4, 128, rows - 128), BF16)
    neighbour_barrier(stage, tp_peer, stages)

    def outs(m):
        return (pltpu.make_async_copy(h1b, h1_all.at[m], out_sem.at[0]),
                pltpu.make_async_copy(qkvb, qkv_all.at[m], out_sem.at[1]),
                pltpu.make_async_copy(ob.at[:, pl.ds(pl.multiple_of(tp_me * half, 128), half)], o_all.at[m], out_sem.at[2]),
                pltpu.make_async_copy(h2b, h2_all.at[m], out_sem.at[3]),
                pltpu.make_async_copy(slb, s_all.at[m], out_sem.at[4]),
                pltpu.make_async_copy(ab, a_all.at[m], out_sem.at[5]),
                pltpu.make_async_copy(xb, x_all.at[m], out_sem.at[6]))

    def mid_out(m):
        slot = lax.rem(m, 2)
        return pltpu.make_async_copy(midb.at[slot], mid_all.at[m], mid_sem.at[slot])

    def y_out(m):
        slot = lax.rem(m, 2)
        return pltpu.make_async_copy(yb.at[slot], y_all.at[m], y_sem.at[slot])

    def part_copy(m):
        slot = lax.rem(m, 2)
        return pltpu.make_async_remote_copy(src_ref=partb.at[slot], dst_ref=peerb.at[lax.rem(m, RING)], send_sem=part_send.at[slot], recv_sem=part_recv.at[m],
                                            device_id={"tp": tp_peer}, device_id_type=MESH)

    def next_copy(m):
        slot = lax.rem(m, 2)
        return pltpu.make_async_remote_copy(src_ref=yb.at[slot], dst_ref=x_all.at[m], send_sem=y_send.at[slot], recv_sem=x_recv.at[m],
                                            device_id={"pp": jnp.minimum(stage + 1, last_stage)}, device_id_type=MESH)

    def layer_norm(src, dst, gain, shift):
        for r in range(0, rows, ROW_CHUNK):
            normed, _ = norm_stats(src[r:r + ROW_CHUNK, :].astype(F32))
            dst[r:r + ROW_CHUNK, :] = (normed * gain + shift).astype(BF16)

    def group_base(group):
        return (group // 2) * (3 * half) + (group % 2) * (4 * width)

    def attend():
        def scores(group):
            base = group_base(group)
            for j, (start, size, offset) in enumerate(WINDOWS):
                query = head_only(qkvb[:, base + start:base + start + size], offset, width)
                key = qkvb[:, base + half + start:base + half + start + size]
                sb[group % 2, j] = dot_nt(query, key)

        def softmax(group):
            for j in range(4):
                for r0 in range(0, rows, SOFT_ROWS):
                    keys = 128 * (r0 // 128 + 1)
                    row = lax.broadcasted_iota(jnp.int32, (SOFT_ROWS, keys), 0) + r0
                    col = lax.broadcasted_iota(jnp.int32, (SOFT_ROWS, keys), 1)
                    score = jnp.where(row >= col, sb[group % 2, j, r0:r0 + SOFT_ROWS, 0:keys], NEG)
                    weight = jnp.exp2((score - jnp.max(score, axis=1, keepdims=True)) * log2_scale)
                    inv = 1.0 / jnp.sum(weight, axis=1, keepdims=True)
                    pb[group % 2, j, r0:r0 + SOFT_ROWS, 0:keys] = (weight * inv).astype(BF16)

        def values(group):
            base = group_base(group) + 2 * half
            parts = [dot_nn(pb[group % 2, j], qkvb[:, base + start:base + start + size]) for j, (start, size, _) in enumerate(WINDOWS)]
            for i, piece in enumerate(join_heads(parts, width)):
                first = group * (4 * width) + i * 128
                ob[:, first:first + 128] = piece.astype(BF16)

        groups = d_model // (4 * width)
        scores(0)
        for group in range(groups):
            if group + 1 < groups:
                scores(group + 1)
            softmax(group)
            values(group)

    def finish(m):
        slot = lax.rem(m, 2)
        peer_slot = lax.rem(m, RING)
        part_copy(m).wait_recv()

        @pl.when(m >= 2)
        def _():
            y_out(m - 2).wait()

            @pl.when(stage < last_stage)
            def _():
                next_copy(m - 2).wait_send()

        for r in range(0, rows, ROW_CHUNK):
            both = partb[slot, r:r + ROW_CHUNK, :].astype(F32) + peerb[peer_slot, r:r + ROW_CHUNK, :].astype(F32)
            yb[slot, r:r + ROW_CHUNK, :] = (midb[slot, r:r + ROW_CHUNK, :].astype(F32) + both + b2[...]).astype(BF16)

        @pl.when(stage < last_stage)
        def _():
            next_copy(m).start()

        y_out(m).start()
        part_copy(m).wait_send()

    def attn_part(m):
        slot = lax.rem(m, 2)
        prev = jnp.maximum(m - 1, 0)
        h1_o, qkv_o, o_o, h2_o, _, _, x_o = outs(m)
        h1_p, qkv_p, o_p, h2_p, _, _, x_p = outs(prev)

        @pl.when(stage == 0)
        def _():
            @pl.when(m > 0)
            def _():
                x_p.wait()

            load = pltpu.make_async_copy(x_in.at[m], xb, in_sem)
            load.start()
            load.wait()
            x_o.start()

        @pl.when(stage > 0)
        def _():
            next_copy(m).wait_recv()
            load = pltpu.make_async_copy(x_all.at[m], xb, in_sem)
            load.start()
            load.wait()

        @pl.when(m > 0)
        def _():
            h1_p.wait()
            qkv_p.wait()
            o_p.wait()
            h2_p.wait()

        layer_norm(xb, h1b, ln[0:1, :], ln[1:2, :])
        h1_o.start()

        @pl.when(m == 0)
        def _():
            loads[0].wait()
            loads[1].wait()

        for n in range(0, 3 * d_model, tile):
            qkvb[:, n:n + tile] = (dot_nn(h1b[...], wq[:, n:n + tile]) + bq[:, n:n + tile]).astype(BF16)
        qkv_o.start()
        attend()
        o_o.start()

        @pl.when(m == 0)
        def _():
            for load in loads[2:]:
                load.wait()

        @pl.when(m >= 2)
        def _():
            mid_out(m - 2).wait()

        for n in range(0, d_model, tile):
            midb[slot, :, n:n + tile] = (xb[:, n:n + tile].astype(F32) + dot_nn(ob[...], wo[:, n:n + tile]) + bo[:, n:n + tile]).astype(BF16)
        mid_out(m).start()
        layer_norm(midb.at[slot], h2b, ln[2:3, :], ln[3:4, :])
        h2_o.start()

    def mlp_part(m):
        slot = lax.rem(m, 2)
        _, _, _, _, s_o, a_o, _ = outs(m)
        _, _, _, _, s_p, a_p, _ = outs(jnp.maximum(m - 1, 0))

        @pl.when(m > 0)
        def _():
            s_p.wait()
            a_p.wait()

        for n in range(0, ff, tile):
            pre = dot_nn(h2b[...], w1[:, n:n + tile]) + b1[:, n:n + tile]
            square = pre * pre
            bend = jnp.tanh(pre * (GELU_C + (GELU_C * GELU_K) * square))
            cdf = 0.5 + 0.5 * bend
            ab[:, n:n + tile] = (pre * cdf).astype(BF16)
            slb[:, n:n + tile] = cdf + (0.5 * pre) * (1.0 - bend * bend) * (GELU_C + (3.0 * GELU_C * GELU_K) * square)
        s_o.start()
        a_o.start()
        for n in range(0, d_model, tile):
            partb[slot, :, n:n + tile] = dot_nn(ab[...], w2[:, n:n + tile]).astype(BF16)
        part_copy(m).start()

    def step(m, carry):
        @pl.when(m < subs)
        def _():
            attn_part(m)

        @pl.when(m > 0)
        def _():
            finish(m - 1)

        @pl.when(m < subs)
        def _():
            mlp_part(m)

        return carry

    lax.fori_loop(0, subs + 1, step, 0)
    h1_o, qkv_o, o_o, h2_o, s_o, a_o, x_o = outs(subs - 1)
    for copy in (h1_o, qkv_o, o_o, h2_o, s_o, a_o):
        copy.wait()

    @pl.when(stage == 0)
    def _():
        x_o.wait()

    for m in (subs - 2, subs - 1):
        mid_out(m).wait()
        y_out(m).wait()

        @pl.when(stage < last_stage)
        def _():
            next_copy(m).wait_send()


def bwd_kernel(subs, stages, width, tile,
               dy_in, x_all, mid_all, s_all, qkv_all, w2t_h, w1t_h, wot_h, wot_p, wqt_h, wqt_p, ln,
               dy_all, dpre_all, gmid_all, dqkv_all, gin_all, db1, db2, dbo, dbq, dln,
               w2t, w1t, wot, wqt, dyb, slb, dpb, partb, peerb, rb, midb, xb, gmb, qkvb, gib, sb, db, pb, dsb,
               w_sem, in_sem, pre_sem, out_sem, dy_sem, gi_sem, part_send, part_recv, gi_send, dy_recv, dy_free):
    stage = lax.axis_index("pp")
    tp_me = lax.axis_index("tp")
    tp_peer = 1 - tp_me
    last_stage = stages - 1
    rows, d_model = xb.shape
    half = d_model // 2
    ff = slb.shape[1]
    scale = width ** -0.5
    log2_scale = scale * LOG2_E

    mine = pl.ds(pl.multiple_of(tp_me * half, 128), half)
    theirs = pl.ds(pl.multiple_of(tp_peer * half, 128), half)
    mine_q = pl.ds(pl.multiple_of(tp_me * (3 * half), 128), 3 * half)
    theirs_q = pl.ds(pl.multiple_of(tp_peer * (3 * half), 128), 3 * half)
    loads = [pltpu.make_async_copy(src, dst, w_sem.at[i]) for i, (src, dst) in enumerate((
        (w2t_h, w2t), (w1t_h, w1t), (wot_h, wot.at[:, mine]), (wot_p, wot.at[:, theirs]), (wqt_h, wqt.at[mine_q, :]), (wqt_p, wqt.at[theirs_q, :])))]
    for load in loads:
        load.start()

    def fetch(m):
        return (pltpu.make_async_copy(s_all.at[m], slb, pre_sem.at[0]),
                pltpu.make_async_copy(mid_all.at[m], midb, pre_sem.at[1]),
                pltpu.make_async_copy(qkv_all.at[m], qkvb, pre_sem.at[2]),
                pltpu.make_async_copy(x_all.at[m], xb, pre_sem.at[3]))

    for copy in fetch(0):
        copy.start()
    for acc in (db1, db2, dbo, dbq, dln):
        acc[...] = jnp.zeros_like(acc)
    for acc in (pb, dsb):
        acc[:, 128:rows, 0:128] = jnp.zeros((4, rows - 128, 128), BF16)
    neighbour_barrier(stage, tp_peer, stages)

    def outs(m):
        return (pltpu.make_async_copy(dpb, dpre_all.at[m], out_sem.at[0]),
                pltpu.make_async_copy(gmb, gmid_all.at[m], out_sem.at[1]),
                pltpu.make_async_copy(qkvb.at[:, pl.ds(pl.multiple_of(tp_me * (3 * half), 128), 3 * half)], dqkv_all.at[m], out_sem.at[2]))

    def dy_load(m):
        return pltpu.make_async_copy(dy_in.at[m], dyb.at[lax.rem(m, RING)], in_sem.at[lax.rem(m, 2)])

    def dy_out(m):
        return pltpu.make_async_copy(dyb.at[lax.rem(m, RING)], dy_all.at[m], dy_sem.at[lax.rem(m, 2)])

    def gi_out(m):
        slot = lax.rem(m, 2)
        return pltpu.make_async_copy(gib.at[slot], gin_all.at[m], gi_sem.at[slot])

    def part_copy(m):
        slot = lax.rem(m, 2)
        return pltpu.make_async_remote_copy(src_ref=partb.at[slot], dst_ref=peerb.at[lax.rem(m, RING)], send_sem=part_send.at[slot], recv_sem=part_recv.at[m],
                                            device_id={"tp": tp_peer}, device_id_type=MESH)

    def prev_copy(m):
        slot = lax.rem(m, 2)
        return pltpu.make_async_remote_copy(src_ref=gib.at[slot], dst_ref=dyb.at[lax.rem(m, RING)], send_sem=gi_send.at[slot], recv_sem=dy_recv.at[m],
                                            device_id={"pp": jnp.maximum(stage - 1, 0)}, device_id_type=MESH)

    @pl.when(stage == last_stage)
    def _():
        dy_load(0).start()

    def norm_grad(x_rows, grad, gain, which):
        normed, inv_std = norm_stats(x_rows)
        dln[which] += fold_rows(grad * normed)
        dln[which + 1] += fold_rows(grad)
        scaled = grad * gain
        mean_scaled = jnp.mean(scaled, axis=-1, keepdims=True)
        mean_proj = jnp.mean(scaled * normed, axis=-1, keepdims=True)
        return inv_std * (scaled - mean_scaled - normed * mean_proj)

    def mlp_part(m):
        slot = lax.rem(m, 2)
        slope_f = fetch(m)[0]

        dy_slot = lax.rem(m, RING)

        @pl.when(stage == last_stage)
        def _():
            dy_load(m).wait()

            @pl.when(m + 1 < subs)
            def _():
                dy_load(m + 1).start()

        @pl.when(stage < last_stage)
        def _():
            prev_copy(m).wait_recv()

        dy_out(m).start()

        @pl.when(m == 0)
        def _():
            loads[0].wait()
            loads[1].wait()

        @pl.when(m > 0)
        def _():
            outs(m - 1)[0].wait()

        slope_f.wait()
        for n in range(0, ff, tile):
            grad = dot_nn(dyb[dy_slot], w2t[:, n:n + tile]).astype(BF16).astype(F32) * slb[:, n:n + tile]
            db1[:, n:n + tile] += fold_rows(grad)
            dpb[:, n:n + tile] = grad.astype(BF16)
        outs(m)[0].start()

        @pl.when(m + 1 < subs)
        def _():
            fetch(m + 1)[0].start()

        for n in range(0, d_model, tile):
            partb[slot, :, n:n + tile] = dot_nn(dpb[...], w1t[:, n:n + tile]).astype(BF16)
        part_copy(m).start()

    def attend_grad():
        def window(base, spec):
            start, size, offset = spec
            return slice(base + start, base + start + size), offset

        def scores(group, base):
            for j, spec in enumerate(WINDOWS):
                q_lanes, offset = window(base, spec)
                k_lanes, _ = window(base + half, spec)
                v_lanes, _ = window(base + 2 * half, spec)
                d_lanes, _ = window(group * (4 * width), spec)
                sb[j] = dot_nt(qkvb[:, k_lanes], head_only(qkvb[:, q_lanes], offset, width))
                db[j] = dot_nt(qkvb[:, v_lanes], head_only(rb[:, d_lanes], offset, width))

        def softmax():
            for j in range(4):
                for q0 in range(0, rows, 128):
                    keys, lanes = q0 + 128, slice(q0, q0 + 128)
                    krow = lax.broadcasted_iota(jnp.int32, (keys, 128), 0)
                    qcol = lax.broadcasted_iota(jnp.int32, (keys, 128), 1) + q0
                    score = jnp.where(qcol >= krow, sb[j, 0:keys, lanes], NEG)
                    weight = jnp.exp2((score - jnp.max(score, axis=0, keepdims=True)) * log2_scale)
                    prob = weight * (1.0 / jnp.sum(weight, axis=0, keepdims=True))
                    pb[j, 0:keys, lanes] = prob.astype(BF16)
                    d_prob = db[j, 0:keys, lanes]
                    d_score = prob * (d_prob - jnp.sum(prob * d_prob, axis=0, keepdims=True))
                    dsb[j, 0:keys, lanes] = d_score.astype(BF16)

        def products(group, base):
            d_query, d_key, d_value = [], [], []
            for j, spec in enumerate(WINDOWS):
                q_lanes, _ = window(base, spec)
                k_lanes, _ = window(base + half, spec)
                d_lanes, _ = window(group * (4 * width), spec)
                d_value.append(dot_nn(pb[j], rb[:, d_lanes]))
                d_key.append(dot_nn(dsb[j], qkvb[:, q_lanes]) * scale)
                d_query.append(dot_tn(dsb[j], qkvb[:, k_lanes]) * scale)
            for c, parts in enumerate((d_query, d_key, d_value)):
                for i, piece in enumerate(join_heads(parts, width)):
                    piece = piece.astype(BF16)
                    first = base + c * half + i * 128
                    qkvb[:, first:first + 128] = piece
                    dbq[:, first:first + 128] += fold_rows(piece.astype(F32))

        for group in range(d_model // (4 * width)):
            base = (group // 2) * (3 * half) + (group % 2) * (4 * width)
            scores(group, base)
            softmax()
            products(group, base)

    def attn_part(m):
        slot = lax.rem(m, 2)
        _, mid_f, qkv_f, x_f = fetch(m)
        _, gm_o, dq_o = outs(m)
        peer_slot = lax.rem(m, RING)
        dy_slot = lax.rem(m, RING)
        mid_f.wait()

        @pl.when(m > 0)
        def _():
            outs(m - 1)[1].wait()

        @pl.when(m == 0)
        def _():
            for load in loads[2:]:
                load.wait()

        part_copy(m).wait_recv()
        for r in range(0, rows, ROW_CHUNK):
            rr = slice(r, r + ROW_CHUNK)
            grad = (partb[slot, rr, :].astype(F32) + peerb[peer_slot, rr, :].astype(F32)).astype(BF16).astype(F32)
            d_y = dyb[dy_slot, rr, :].astype(F32)
            db2[...] += fold_rows(d_y)
            total = d_y + norm_grad(midb[rr, :].astype(F32), grad, ln[2:3, :], 2)
            gmb[rr, :] = total.astype(BF16)
            dbo[...] += fold_rows(total)
        gm_o.start()
        dy_out(m).wait()

        @pl.when((stage < last_stage) & (m < subs - RING))
        def _():
            pl.semaphore_signal(dy_free, inc=1, device_id={"pp": jnp.minimum(stage + 1, last_stage)}, device_id_type=MESH)

        @pl.when(m + 1 < subs)
        def _():
            fetch(m + 1)[1].start()

        for n in range(0, d_model, tile):
            rb[:, n:n + tile] = dot_nn(gmb[...], wot[:, n:n + tile]).astype(BF16)
        qkv_f.wait()
        attend_grad()
        dq_o.start()
        part_copy(m).wait_send()
        for n in range(0, d_model, tile):
            rb[:, n:n + tile] = dot_nn(qkvb[...], wqt[:, n:n + tile]).astype(BF16)
        x_f.wait()

        @pl.when(m >= 2)
        def _():
            gi_out(m - 2).wait()

            @pl.when(stage > 0)
            def _():
                prev_copy(m - 2).wait_send()

        for r in range(0, rows, ROW_CHUNK):
            rr = slice(r, r + ROW_CHUNK)
            total = gmb[rr, :].astype(F32) + norm_grad(xb[rr, :].astype(F32), rb[rr, :].astype(F32), ln[0:1, :], 0)
            gib[slot, rr, :] = total.astype(BF16)

        @pl.when(stage > 0)
        def _():
            @pl.when(m >= RING)
            def _():
                pl.semaphore_wait(dy_free, 1)

            prev_copy(m).start()

        gi_out(m).start()
        dq_o.wait()

        @pl.when(m + 1 < subs)
        def _():
            fetch(m + 1)[2].start()
            fetch(m + 1)[3].start()

    def step(m, carry):
        @pl.when(m < subs)
        def _():
            mlp_part(m)

        @pl.when(m > 0)
        def _():
            attn_part(m - 1)

        return carry

    lax.fori_loop(0, subs + 1, step, 0)
    for copy in outs(subs - 1)[:2]:
        copy.wait()
    for m in (subs - 2, subs - 1):
        gi_out(m).wait()

        @pl.when(stage > 0)
        def _():
            prev_copy(m).wait_send()


ANY = pl.BlockSpec(memory_space=pl.ANY)
VMEM = pl.BlockSpec(memory_space=pltpu.VMEM)
DMA = pltpu.SemaphoreType.DMA
VMEM_LIMIT = 67043328


def fwd_call(stages, width, tile, x_in, wq_own, wq_peer, wo_own, wo_peer, w1, w2, bq, bo, ln, b1, b2):
    subs, rows, d_model = x_in.shape
    ff = w1.shape[1]
    half = d_model // 2

    def hbm(cols, dtype=BF16):
        return jax.ShapeDtypeStruct((subs, rows, cols), dtype)

    def buf(cols, dtype=BF16):
        return pltpu.VMEM((rows, cols), dtype)

    def two(cols):
        return pltpu.VMEM((2, rows, cols), BF16)

    weights = 2 * (4 * d_model * d_model + 2 * d_model * ff)
    return pl.pallas_call(
        functools.partial(fwd_kernel, subs, stages, width, tile),
        name="fwd_stage",
        out_shape=(hbm(d_model), hbm(3 * d_model), hbm(half), hbm(d_model), hbm(d_model), hbm(d_model), hbm(ff, F32), hbm(ff), hbm(d_model)),
        in_specs=[ANY] * 7 + [VMEM] * 5,
        out_specs=[ANY] * 9,
        scratch_shapes=[
            pltpu.VMEM((d_model, 3 * d_model), BF16), pltpu.VMEM((d_model, d_model), BF16), pltpu.VMEM(w1.shape, BF16), pltpu.VMEM(w2.shape, BF16),
            buf(d_model), buf(d_model), buf(3 * d_model), buf(d_model), two(d_model), buf(d_model), buf(ff, F32), buf(ff), two(d_model), pltpu.VMEM((RING, rows, d_model), BF16), two(d_model),
            pltpu.VMEM((2, 4, rows, rows), F32), pltpu.VMEM((2, 4, rows, rows), BF16),
            DMA((6,)), DMA, DMA((7,)), DMA((2,)), DMA((2,)), DMA((2,)), DMA((subs,)), DMA((2,)), DMA((subs,)),
        ],
        cost_estimate=pl.CostEstimate(flops=subs * rows * weights, bytes_accessed=weights + subs * rows * d_model * 30, transcendentals=subs * rows * (ff + rows * 16)),
        compiler_params=pltpu.CompilerParams(collective_id=0, has_side_effects=True, vmem_limit_bytes=VMEM_LIMIT),
    )(x_in, wq_own, wq_peer, wo_own, wo_peer, w1, w2, bq, bo, ln, b1, b2)


def bwd_call(stages, width, tile, dy_in, x_all, mid_all, s_all, qkv_all, w2t, w1t, wot_own, wot_peer, wqt_own, wqt_peer, ln):
    subs, rows, d_model = dy_in.shape
    ff = s_all.shape[2]
    half = d_model // 2

    def hbm(cols, dtype=BF16):
        return jax.ShapeDtypeStruct((subs, rows, cols), dtype)

    def buf(cols, dtype=BF16):
        return pltpu.VMEM((rows, cols), dtype)

    def two(cols):
        return pltpu.VMEM((2, rows, cols), BF16)

    ring = pltpu.VMEM((RING, rows, d_model), BF16)

    def acc(*shape):
        return jax.ShapeDtypeStruct(shape, F32)

    weights = 2 * (4 * d_model * d_model + 2 * d_model * ff)
    return pl.pallas_call(
        functools.partial(bwd_kernel, subs, stages, width, tile),
        name="bwd_stage",
        out_shape=(hbm(d_model), hbm(ff), hbm(d_model), hbm(3 * half), hbm(d_model),
                   acc(8, ff), acc(8, d_model), acc(8, d_model), acc(8, 3 * d_model), acc(4, 8, d_model)),
        in_specs=[ANY] * 11 + [VMEM],
        out_specs=[ANY] * 5 + [VMEM] * 5,
        scratch_shapes=[
            pltpu.VMEM(w2t.shape, BF16), pltpu.VMEM(w1t.shape, BF16), pltpu.VMEM((d_model, d_model), BF16), pltpu.VMEM((3 * d_model, d_model), BF16),
            ring, buf(ff, F32), buf(ff), two(d_model), ring, buf(d_model), buf(d_model), buf(d_model), buf(d_model), buf(3 * d_model), two(d_model),
            pltpu.VMEM((4, rows, rows), F32), pltpu.VMEM((4, rows, rows), F32), pltpu.VMEM((4, rows, rows), BF16), pltpu.VMEM((4, rows, rows), BF16),
            DMA((6,)), DMA((2,)), DMA((4,)), DMA((3,)), DMA((2,)), DMA((2,)), DMA((2,)), DMA((subs,)), DMA((2,)), DMA((subs,)), pltpu.SemaphoreType.REGULAR,
        ],
        cost_estimate=pl.CostEstimate(flops=subs * rows * weights, bytes_accessed=weights + subs * rows * d_model * 30, transcendentals=subs * rows * (ff + rows * 16)),
        compiler_params=pltpu.CompilerParams(collective_id=1, has_side_effects=True, vmem_limit_bytes=VMEM_LIMIT),
    )(dy_in, x_all, mid_all, s_all, qkv_all, w2t, w1t, wot_own, wot_peer, wqt_own, wqt_peer, ln)


def grad_kernel(n_tile, left, right, *refs):
    if len(refs) == 3:
        kept, out, kept_out = refs
        kept_out[...] = kept[...]
    else:
        out, = refs

    @pl.when(pl.program_id(1) == 0)
    def _():
        out[...] = jnp.zeros_like(out)

    for n in range(0, out.shape[1], n_tile):
        lanes = slice(n, n + n_tile)
        out[:, lanes] += dot_tn(left[...], right[:, lanes])


def grad_call(left, right, m_block, n_block, k_block, kept=None):
    tokens, m_size = left.shape
    n_size = right.shape[1]
    m_count = m_size // m_block
    grid = (m_count * (n_size // n_block), tokens // k_block)
    in_specs = [pl.BlockSpec((k_block, m_block), lambda i, k: (k, i % m_count)), pl.BlockSpec((k_block, n_block), lambda i, k: (k, i // m_count))]
    out_specs = [pl.BlockSpec((m_block, n_block), lambda i, k: (i % m_count, i // m_count))]
    out_shape = [jax.ShapeDtypeStruct((m_size, n_size), F32)]
    args = [left, right]
    if kept is not None:
        steps = grid[0] * grid[1]
        assert kept.shape[0] % steps == 0
        spec = pl.BlockSpec((kept.shape[0] // steps,) + kept.shape[1:], lambda i, k: (i * grid[1] + k, 0, 0))
        in_specs.append(spec)
        out_specs.append(spec)
        out_shape.append(jax.ShapeDtypeStruct(kept.shape, kept.dtype))
        args.append(kept)
    moved = 2 * tokens * (m_size * (n_size // n_block) + n_size * m_count) + 4 * m_size * n_size
    return pl.pallas_call(
        functools.partial(grad_kernel, 512),
        name="weight_grad",
        grid=grid,
        in_specs=in_specs,
        out_specs=out_specs,
        out_shape=out_shape,
        cost_estimate=pl.CostEstimate(flops=2 * tokens * m_size * n_size, bytes_accessed=moved, transcendentals=0),
        compiler_params=pltpu.CompilerParams(dimension_semantics=("arbitrary", "arbitrary"), vmem_limit_bytes=VMEM_LIMIT),
    )(*args)


def solution(mesh):
    stages = mesh.shape["pp"]
    swap = [(0, 1), (1, 0)]

    def stage_program(x_in, dy_out, w_qkv, b_qkv, w_out, b_out, ln_par, w_fc1, b_fc1, w_fc2, b_fc2):
        micro, batch, rows, d_model = x_in.shape
        heads, width = w_qkv.shape[3:]
        half = heads * width
        subs = micro * batch
        tile = half
        tp_me = lax.axis_index("tp")

        wqt_own = jnp.transpose(w_qkv[0], (0, 2, 3, 1)).reshape(3 * half, d_model)
        wo_own = w_out[0].reshape(half, d_model)
        wo_peer = lax.ppermute(wo_own, "tp", swap)
        wqt_peer = lax.ppermute(wqt_own, "tp", swap)
        bq_own = b_qkv[0].reshape(1, 3 * half)
        bq_peer = lax.ppermute(bq_own, "tp", swap)
        bq = jnp.concatenate([jnp.where(tp_me == 0, bq_own, bq_peer), jnp.where(tp_me == 0, bq_peer, bq_own)], axis=1).astype(F32)
        w1, w2 = w_fc1[0], w_fc2[0]
        ln = ln_par[0].astype(F32)
        x_all, qkv_all, o_all, mid_all, h1_all, h2_all, s_all, a_all, y_all = fwd_call(
            stages, width, tile, x_in.reshape(subs, rows, d_model), wqt_own.T, wqt_peer.T, wo_own, wo_peer, w1, w2, bq, b_out.astype(F32), ln, b_fc1.astype(F32), b_fc2.astype(F32))
        dy_all, dpre_all, gmid_all, dqkv_all, gin_all, db1, db2, dbo, dbq, dln = bwd_call(
            stages, width, tile, dy_out.reshape(subs, rows, d_model), x_all, mid_all, s_all, qkv_all, w2.T, w1.T, wo_own.T, wo_peer.T, wqt_own, wqt_peer, ln)

        def flat(stack):
            return stack.reshape(subs * rows, -1)

        g_w_fc2, h_out = grad_call(flat(a_all), flat(dy_all), 1024, d_model, 768, y_all)
        g_w_fc1, g_in = grad_call(flat(h2_all), flat(dpre_all), d_model, 1024, 768, gin_all)
        g_w_out, = grad_call(flat(o_all), flat(gmid_all), half, d_model, 768)
        g_w_qkv, = grad_call(flat(dqkv_all), flat(h1_all), half, d_model, 768)
        g_w_out = g_w_out.reshape(heads, width, d_model)
        g_w_qkv = jnp.transpose(g_w_qkv.reshape(3, heads, width, d_model), (0, 3, 1, 2))
        g_b_qkv = lax.dynamic_slice_in_dim(jnp.sum(dbq, axis=0), tp_me * (3 * half), 3 * half).reshape(3, heads, width)
        act = (1, micro, batch, rows, d_model)
        return (h_out.reshape(act), g_in.reshape(act), g_w_qkv[None], g_b_qkv[None], g_w_out[None], jnp.sum(dbo, axis=0)[None],
                jnp.sum(dln, axis=1)[None], g_w_fc1[None], jnp.sum(db1, axis=0)[None], g_w_fc2[None], jnp.sum(db2, axis=0)[None])

    act_spec = P(None, "dp", None, None)
    arg_specs = (act_spec, act_spec,
                 P("pp", None, None, "tp", None), P("pp", None, "tp", None), P("pp", "tp", None, None),
                 P("pp", None), P("pp", None, None), P("pp", None, "tp"), P("pp", "tp"),
                 P("pp", "tp", None), P("pp", None))
    stage_spec = P("pp", None, "dp", None, None)
    grad_axes = ("dp", "pp")
    result_specs = (stage_spec, stage_spec,
                    P(grad_axes, None, None, "tp", None), P(grad_axes, None, "tp", None), P(grad_axes, "tp", None, None),
                    P(grad_axes, None), P(grad_axes, None, None), P(grad_axes, None, "tp"), P(grad_axes, "tp"),
                    P(grad_axes, "tp", None), P(grad_axes, None))
    return jax.shard_map(stage_program, mesh=mesh, in_specs=arg_specs, out_specs=result_specs, check_vma=False)
```

```python
import functools

import jax
import jax.numpy as jnp
from jax import lax
from jax.experimental import pallas as pl
from jax.experimental.pallas import tpu as pltpu
from jax.sharding import PartitionSpec as P

LN_EPS = 1e-5
F32 = jnp.float32
BF16 = jnp.bfloat16
MESH = pl.DeviceIdType.MESH
NEG = -1e30
ROW_CHUNK = 32
GELU_C = 0.7978845608028654
GELU_K = 0.044715
LOG2_E = 1.4426950408889634
SOFT_ROWS = 64
RING = 4

WINDOWS = ((0, 128, 0), (0, 256, 96), (128, 256, 64), (256, 128, 32))


def dot_nn(lhs, rhs):
    return lax.dot_general(lhs, rhs, (((1,), (0,)), ((), ())), preferred_element_type=F32)


def dot_nt(lhs, rhs):
    return lax.dot_general(lhs, rhs, (((1,), (1,)), ((), ())), preferred_element_type=F32)


def dot_tn(lhs, rhs):
    return lax.dot_general(lhs, rhs, (((0,), (0,)), ((), ())), preferred_element_type=F32)


def head_only(window, offset, width):
    lane = lax.broadcasted_iota(jnp.int32, window.shape, 1)
    return jnp.where((lane >= offset) & (lane < offset + width), window, jnp.zeros_like(window))


def join_heads(parts, width):
    lane = lax.broadcasted_iota(jnp.int32, (parts[0].shape[0], 128), 1)
    first = jnp.where(lane < width, parts[0], parts[1][:, :128])
    second = jnp.where(lane < 2 * width - 128, parts[1][:, 128:], parts[2][:, :128])
    third = jnp.where(lane < 3 * width - 256, parts[2][:, 128:], parts[3])
    return first, second, third


def norm_stats(x_wide):
    centered = x_wide - jnp.mean(x_wide, axis=-1, keepdims=True)
    inv_std = lax.rsqrt(jnp.mean(centered * centered, axis=-1, keepdims=True) + LN_EPS)
    return centered * inv_std, inv_std


def fold_rows(block):
    rows, cols = block.shape
    return jnp.sum(block.reshape(rows // 8, 8, cols), axis=0)


def neighbour_barrier(stage, tp_peer, stages):
    barrier = pltpu.get_barrier_semaphore()
    pl.semaphore_signal(barrier, inc=1, device_id={"tp": tp_peer}, device_id_type=MESH)
    pl.semaphore_signal(barrier, inc=1, device_id={"pp": lax.rem(stage + 1, stages)}, device_id_type=MESH)
    pl.semaphore_signal(barrier, inc=1, device_id={"pp": lax.rem(stage + stages - 1, stages)}, device_id_type=MESH)
    pl.semaphore_wait(barrier, 3)


def fwd_kernel(subs, stages, width, tile,
               x_in, wq_h, wq_p, wo_h, wo_p, w1_h, w2_h, bq, bo, ln, b1, b2,
               x_all, qkv_all, o_all, mid_all, h1_all, h2_all, s_all, a_all, y_all,
               wq, wo, w1, w2, xr, h1b, qkvb, ob, midb, h2b, slb, ab, partb, peerb, yb, sb, pb,
               w_sem, in_sem, out_sem, mid_sem, y_sem, part_send, part_recv, y_send, x_recv, x_free):
    stage = lax.axis_index("pp")
    tp_me = lax.axis_index("tp")
    tp_peer = 1 - tp_me
    last_stage = stages - 1
    _, rows, d_model = xr.shape
    half = d_model // 2
    ff = slb.shape[1]
    scale = width ** -0.5
    log2_scale = scale * LOG2_E

    mine = pl.ds(pl.multiple_of(tp_me * half, 128), half)
    theirs = pl.ds(pl.multiple_of(tp_peer * half, 128), half)
    mine_q = pl.ds(pl.multiple_of(tp_me * (3 * half), 128), 3 * half)
    theirs_q = pl.ds(pl.multiple_of(tp_peer * (3 * half), 128), 3 * half)
    loads = [pltpu.make_async_copy(src, dst, w_sem.at[i]) for i, (src, dst) in enumerate((
        (wq_h, wq.at[:, mine_q]), (wq_p, wq.at[:, theirs_q]), (wo_h, wo.at[mine, :]), (wo_p, wo.at[theirs, :]), (w1_h, w1), (w2_h, w2)))]
    for load in loads:
        load.start()
    pb[:, :, 0:128, 128:rows] = jnp.zeros((2, 4, 128, rows - 128), BF16)
    neighbour_barrier(stage, tp_peer, stages)

    def outs(m):
        return (pltpu.make_async_copy(h1b, h1_all.at[m], out_sem.at[0]),
                pltpu.make_async_copy(qkvb, qkv_all.at[m], out_sem.at[1]),
                pltpu.make_async_copy(ob.at[:, pl.ds(pl.multiple_of(tp_me * half, 128), half)], o_all.at[m], out_sem.at[2]),
                pltpu.make_async_copy(h2b, h2_all.at[m], out_sem.at[3]),
                pltpu.make_async_copy(slb, s_all.at[m], out_sem.at[4]),
                pltpu.make_async_copy(ab, a_all.at[m], out_sem.at[5]),
                pltpu.make_async_copy(xr.at[lax.rem(m, RING)], x_all.at[m], out_sem.at[6]))

    def mid_out(m):
        slot = lax.rem(m, 2)
        return pltpu.make_async_copy(midb.at[slot], mid_all.at[m], mid_sem.at[slot])

    def y_out(m):
        slot = lax.rem(m, 2)
        return pltpu.make_async_copy(yb.at[slot], y_all.at[m], y_sem.at[slot])

    def part_copy(m):
        slot = lax.rem(m, 2)
        return pltpu.make_async_remote_copy(src_ref=partb.at[slot], dst_ref=peerb.at[lax.rem(m, RING)], send_sem=part_send.at[slot], recv_sem=part_recv.at[m],
                                            device_id={"tp": tp_peer}, device_id_type=MESH)

    def next_copy(m):
        slot = lax.rem(m, 2)
        return pltpu.make_async_remote_copy(src_ref=yb.at[slot], dst_ref=xr.at[lax.rem(m, RING)], send_sem=y_send.at[slot], recv_sem=x_recv.at[m],
                                            device_id={"pp": jnp.minimum(stage + 1, last_stage)}, device_id_type=MESH)

    def x_load(m):
        return pltpu.make_async_copy(x_in.at[m], xr.at[lax.rem(m, RING)], in_sem.at[lax.rem(m, 2)])

    @pl.when(stage == 0)
    def _():
        x_load(0).start()

    def layer_norm(src, dst, gain, shift):
        for r in range(0, rows, ROW_CHUNK):
            normed, _ = norm_stats(src[r:r + ROW_CHUNK, :].astype(F32))
            dst[r:r + ROW_CHUNK, :] = (normed * gain + shift).astype(BF16)

    def group_base(group):
        return (group // 2) * (3 * half) + (group % 2) * (4 * width)

    def attend():
        def scores(group):
            base = group_base(group)
            for j, (start, size, offset) in enumerate(WINDOWS):
                query = head_only(qkvb[:, base + start:base + start + size], offset, width)
                key = qkvb[:, base + half + start:base + half + start + size]
                sb[group % 2, j] = dot_nt(query, key)

        def softmax(group):
            for j in range(4):
                for r0 in range(0, rows, SOFT_ROWS):
                    keys = 128 * (r0 // 128 + 1)
                    row = lax.broadcasted_iota(jnp.int32, (SOFT_ROWS, keys), 0) + r0
                    col = lax.broadcasted_iota(jnp.int32, (SOFT_ROWS, keys), 1)
                    score = jnp.where(row >= col, sb[group % 2, j, r0:r0 + SOFT_ROWS, 0:keys], NEG)
                    weight = jnp.exp2((score - jnp.max(score, axis=1, keepdims=True)) * log2_scale)
                    inv = 1.0 / jnp.sum(weight, axis=1, keepdims=True)
                    pb[group % 2, j, r0:r0 + SOFT_ROWS, 0:keys] = (weight * inv).astype(BF16)

        def values(group):
            base = group_base(group) + 2 * half
            parts = [dot_nn(pb[group % 2, j], qkvb[:, base + start:base + start + size]) for j, (start, size, _) in enumerate(WINDOWS)]
            for i, piece in enumerate(join_heads(parts, width)):
                first = group * (4 * width) + i * 128
                ob[:, first:first + 128] = piece.astype(BF16)

        groups = d_model // (4 * width)
        scores(0)
        for group in range(groups):
            if group + 1 < groups:
                scores(group + 1)
            softmax(group)
            values(group)

    def finish(m):
        slot = lax.rem(m, 2)
        peer_slot = lax.rem(m, RING)
        part_copy(m).wait_recv()

        @pl.when(m >= 2)
        def _():
            y_out(m - 2).wait()

            @pl.when(stage < last_stage)
            def _():
                next_copy(m - 2).wait_send()

        for r in range(0, rows, ROW_CHUNK):
            both = partb[slot, r:r + ROW_CHUNK, :].astype(F32) + peerb[peer_slot, r:r + ROW_CHUNK, :].astype(F32)
            yb[slot, r:r + ROW_CHUNK, :] = (midb[slot, r:r + ROW_CHUNK, :].astype(F32) + both + b2[...]).astype(BF16)

        @pl.when(stage < last_stage)
        def _():
            @pl.when(m >= RING)
            def _():
                pl.semaphore_wait(x_free, 1)

            next_copy(m).start()

        y_out(m).start()
        part_copy(m).wait_send()

    def attn_part(m):
        slot = lax.rem(m, 2)
        prev = jnp.maximum(m - 1, 0)
        h1_o, qkv_o, o_o, h2_o, _, _, x_o = outs(m)
        h1_p, qkv_p, o_p, h2_p, _, _, x_p = outs(prev)

        @pl.when(stage == 0)
        def _():
            x_load(m).wait()

            @pl.when(m + 1 < subs)
            def _():
                x_load(m + 1).start()

        @pl.when(stage > 0)
        def _():
            next_copy(m).wait_recv()

        x_o.start()
        xb = xr.at[lax.rem(m, RING)]

        @pl.when(m > 0)
        def _():
            h1_p.wait()
            qkv_p.wait()
            o_p.wait()
            h2_p.wait()

        layer_norm(xb, h1b, ln[0:1, :], ln[1:2, :])
        h1_o.start()

        @pl.when(m == 0)
        def _():
            loads[0].wait()
            loads[1].wait()

        for n in range(0, 3 * d_model, tile):
            qkvb[:, n:n + tile] = (dot_nn(h1b[...], wq[:, n:n + tile]) + bq[:, n:n + tile]).astype(BF16)
        qkv_o.start()
        attend()
        o_o.start()

        @pl.when(m == 0)
        def _():
            for load in loads[2:]:
                load.wait()

        @pl.when(m >= 2)
        def _():
            mid_out(m - 2).wait()

        for n in range(0, d_model, tile):
            midb[slot, :, n:n + tile] = (xb[:, n:n + tile].astype(F32) + dot_nn(ob[...], wo[:, n:n + tile]) + bo[:, n:n + tile]).astype(BF16)
        mid_out(m).start()
        x_o.wait()

        @pl.when((stage > 0) & (m < subs - RING))
        def _():
            pl.semaphore_signal(x_free, inc=1, device_id={"pp": jnp.maximum(stage - 1, 0)}, device_id_type=MESH)

        layer_norm(midb.at[slot], h2b, ln[2:3, :], ln[3:4, :])
        h2_o.start()

    def mlp_part(m):
        slot = lax.rem(m, 2)
        _, _, _, _, s_o, a_o, _ = outs(m)
        _, _, _, _, s_p, a_p, _ = outs(jnp.maximum(m - 1, 0))

        @pl.when(m > 0)
        def _():
            s_p.wait()
            a_p.wait()

        for n in range(0, ff, tile):
            pre = dot_nn(h2b[...], w1[:, n:n + tile]) + b1[:, n:n + tile]
            square = pre * pre
            bend = jnp.tanh(pre * (GELU_C + (GELU_C * GELU_K) * square))
            cdf = 0.5 + 0.5 * bend
            ab[:, n:n + tile] = (pre * cdf).astype(BF16)
            slb[:, n:n + tile] = cdf + (0.5 * pre) * (1.0 - bend * bend) * (GELU_C + (3.0 * GELU_C * GELU_K) * square)
        s_o.start()
        a_o.start()
        for n in range(0, d_model, tile):
            partb[slot, :, n:n + tile] = dot_nn(ab[...], w2[:, n:n + tile]).astype(BF16)
        part_copy(m).start()

    def step(m, carry):
        @pl.when(m < subs)
        def _():
            attn_part(m)
            mlp_part(m)

        @pl.when(m > 0)
        def _():
            finish(m - 1)

        return carry

    lax.fori_loop(0, subs + 1, step, 0)
    h1_o, qkv_o, o_o, h2_o, s_o, a_o, x_o = outs(subs - 1)
    for copy in (h1_o, qkv_o, o_o, h2_o, s_o, a_o):
        copy.wait()

    for m in (subs - 2, subs - 1):
        mid_out(m).wait()
        y_out(m).wait()

        @pl.when(stage < last_stage)
        def _():
            next_copy(m).wait_send()


def bwd_kernel(subs, stages, width, tile,
               dy_in, x_all, mid_all, s_all, qkv_all, w2t_h, w1t_h, wot_h, wot_p, wqt_h, wqt_p, ln,
               dy_all, dpre_all, gmid_all, dqkv_all, gin_all, db1_o, db2_o, dbo_o, dbq_o, dln_o,
               w2t, w1t, wot, wqt, dyb, slb, dpb, partb, peerb, rb, midb, xb, gmb, qkvb, gib, sb, db, pb, dsb, db1, db2, dbo, dbq, dln,
               w_sem, in_sem, pre_sem, out_sem, dy_sem, gi_sem, part_send, part_recv, gi_send, dy_recv, dy_free):
    stage = lax.axis_index("pp")
    tp_me = lax.axis_index("tp")
    tp_peer = 1 - tp_me
    last_stage = stages - 1
    rows, d_model = xb.shape
    half = d_model // 2
    ff = slb.shape[1]
    scale = width ** -0.5
    log2_scale = scale * LOG2_E

    mine = pl.ds(pl.multiple_of(tp_me * half, 128), half)
    theirs = pl.ds(pl.multiple_of(tp_peer * half, 128), half)
    mine_q = pl.ds(pl.multiple_of(tp_me * (3 * half), 128), 3 * half)
    theirs_q = pl.ds(pl.multiple_of(tp_peer * (3 * half), 128), 3 * half)
    loads = [pltpu.make_async_copy(src, dst, w_sem.at[i]) for i, (src, dst) in enumerate((
        (w2t_h, w2t), (w1t_h, w1t), (wot_h, wot.at[:, mine]), (wot_p, wot.at[:, theirs]), (wqt_h, wqt.at[mine_q, :]), (wqt_p, wqt.at[theirs_q, :])))]
    for load in loads:
        load.start()

    def fetch(m):
        return (pltpu.make_async_copy(s_all.at[m], slb, pre_sem.at[0]),
                pltpu.make_async_copy(mid_all.at[m], midb, pre_sem.at[1]),
                pltpu.make_async_copy(qkv_all.at[m], qkvb, pre_sem.at[2]),
                pltpu.make_async_copy(x_all.at[m], xb, pre_sem.at[3]))

    for copy in fetch(0):
        copy.start()
    for acc in (db1, db2, dbo, dbq, dln):
        acc[...] = jnp.zeros_like(acc)
    for acc in (pb, dsb):
        acc[:, 128:rows, 0:128] = jnp.zeros((4, rows - 128, 128), BF16)
    neighbour_barrier(stage, tp_peer, stages)

    def outs(m):
        return (pltpu.make_async_copy(dpb, dpre_all.at[m], out_sem.at[0]),
                pltpu.make_async_copy(gmb, gmid_all.at[m], out_sem.at[1]),
                pltpu.make_async_copy(qkvb.at[:, pl.ds(pl.multiple_of(tp_me * (3 * half), 128), 3 * half)], dqkv_all.at[m], out_sem.at[2]))

    def dy_load(m):
        return pltpu.make_async_copy(dy_in.at[m], dyb.at[lax.rem(m, RING)], in_sem.at[lax.rem(m, 2)])

    def dy_out(m):
        return pltpu.make_async_copy(dyb.at[lax.rem(m, RING)], dy_all.at[m], dy_sem.at[lax.rem(m, 2)])

    def gi_out(m):
        slot = lax.rem(m, 2)
        return pltpu.make_async_copy(gib.at[slot], gin_all.at[m], gi_sem.at[slot])

    def part_copy(m):
        slot = lax.rem(m, 2)
        return pltpu.make_async_remote_copy(src_ref=partb.at[slot], dst_ref=peerb.at[lax.rem(m, RING)], send_sem=part_send.at[slot], recv_sem=part_recv.at[m],
                                            device_id={"tp": tp_peer}, device_id_type=MESH)

    def prev_copy(m):
        slot = lax.rem(m, 2)
        return pltpu.make_async_remote_copy(src_ref=gib.at[slot], dst_ref=dyb.at[lax.rem(m, RING)], send_sem=gi_send.at[slot], recv_sem=dy_recv.at[m],
                                            device_id={"pp": jnp.maximum(stage - 1, 0)}, device_id_type=MESH)

    @pl.when(stage == last_stage)
    def _():
        dy_load(0).start()

    def norm_grad(x_rows, grad, gain, which):
        normed, inv_std = norm_stats(x_rows)
        dln[which] += fold_rows(grad * normed)
        dln[which + 1] += fold_rows(grad)
        scaled = grad * gain
        mean_scaled = jnp.mean(scaled, axis=-1, keepdims=True)
        mean_proj = jnp.mean(scaled * normed, axis=-1, keepdims=True)
        return inv_std * (scaled - mean_scaled - normed * mean_proj)

    def mlp_part(m):
        slot = lax.rem(m, 2)
        slope_f = fetch(m)[0]

        dy_slot = lax.rem(m, RING)

        @pl.when(stage == last_stage)
        def _():
            dy_load(m).wait()

            @pl.when(m + 1 < subs)
            def _():
                dy_load(m + 1).start()

        @pl.when(stage < last_stage)
        def _():
            prev_copy(m).wait_recv()

        dy_out(m).start()

        @pl.when(m == 0)
        def _():
            loads[0].wait()
            loads[1].wait()

        @pl.when(m > 0)
        def _():
            outs(m - 1)[0].wait()

        slope_f.wait()
        for n in range(0, ff, tile):
            grad = dot_nn(dyb[dy_slot], w2t[:, n:n + tile]).astype(BF16).astype(F32) * slb[:, n:n + tile]
            db1[:, n:n + tile] += fold_rows(grad)
            dpb[:, n:n + tile] = grad.astype(BF16)
        outs(m)[0].start()

        @pl.when(m + 1 < subs)
        def _():
            fetch(m + 1)[0].start()

        for n in range(0, d_model, tile):
            partb[slot, :, n:n + tile] = dot_nn(dpb[...], w1t[:, n:n + tile]).astype(BF16)
        part_copy(m).start()

    def attend_grad():
        def window(base, spec):
            start, size, offset = spec
            return slice(base + start, base + start + size), offset

        def scores(group, base):
            for j, spec in enumerate(WINDOWS):
                q_lanes, offset = window(base, spec)
                k_lanes, _ = window(base + half, spec)
                v_lanes, _ = window(base + 2 * half, spec)
                d_lanes, _ = window(group * (4 * width), spec)
                sb[j] = dot_nt(qkvb[:, k_lanes], head_only(qkvb[:, q_lanes], offset, width))
                db[j] = dot_nt(qkvb[:, v_lanes], head_only(rb[:, d_lanes], offset, width))

        def softmax():
            for j in range(4):
                for q0 in range(0, rows, 128):
                    keys, lanes = q0 + 128, slice(q0, q0 + 128)
                    krow = lax.broadcasted_iota(jnp.int32, (keys, 128), 0)
                    qcol = lax.broadcasted_iota(jnp.int32, (keys, 128), 1) + q0
                    score = jnp.where(qcol >= krow, sb[j, 0:keys, lanes], NEG)
                    weight = jnp.exp2((score - jnp.max(score, axis=0, keepdims=True)) * log2_scale)
                    prob = weight * (1.0 / jnp.sum(weight, axis=0, keepdims=True))
                    pb[j, 0:keys, lanes] = prob.astype(BF16)
                    d_prob = db[j, 0:keys, lanes]
                    d_score = prob * (d_prob - jnp.sum(prob * d_prob, axis=0, keepdims=True))
                    dsb[j, 0:keys, lanes] = d_score.astype(BF16)

        def products(group, base):
            d_query, d_key, d_value = [], [], []
            for j, spec in enumerate(WINDOWS):
                q_lanes, _ = window(base, spec)
                k_lanes, _ = window(base + half, spec)
                d_lanes, _ = window(group * (4 * width), spec)
                d_value.append(dot_nn(pb[j], rb[:, d_lanes]))
                d_key.append(dot_nn(dsb[j], qkvb[:, q_lanes]) * scale)
                d_query.append(dot_tn(dsb[j], qkvb[:, k_lanes]) * scale)
            for c, parts in enumerate((d_query, d_key, d_value)):
                for i, piece in enumerate(join_heads(parts, width)):
                    piece = piece.astype(BF16)
                    first = base + c * half + i * 128
                    qkvb[:, first:first + 128] = piece
                    dbq[:, first:first + 128] += fold_rows(piece.astype(F32))

        for group in range(d_model // (4 * width)):
            base = (group // 2) * (3 * half) + (group % 2) * (4 * width)
            scores(group, base)
            softmax()
            products(group, base)

    def attn_part(m):
        slot = lax.rem(m, 2)
        _, mid_f, qkv_f, x_f = fetch(m)
        _, gm_o, dq_o = outs(m)
        peer_slot = lax.rem(m, RING)
        dy_slot = lax.rem(m, RING)
        mid_f.wait()

        @pl.when(m > 0)
        def _():
            outs(m - 1)[1].wait()

        @pl.when(m == 0)
        def _():
            for load in loads[2:]:
                load.wait()

        part_copy(m).wait_recv()
        for r in range(0, rows, ROW_CHUNK):
            rr = slice(r, r + ROW_CHUNK)
            grad = (partb[slot, rr, :].astype(F32) + peerb[peer_slot, rr, :].astype(F32)).astype(BF16).astype(F32)
            d_y = dyb[dy_slot, rr, :].astype(F32)
            db2[...] += fold_rows(d_y)
            total = d_y + norm_grad(midb[rr, :].astype(F32), grad, ln[2:3, :], 2)
            gmb[rr, :] = total.astype(BF16)
            dbo[...] += fold_rows(total)
        gm_o.start()
        dy_out(m).wait()

        @pl.when((stage < last_stage) & (m < subs - RING))
        def _():
            pl.semaphore_signal(dy_free, inc=1, device_id={"pp": jnp.minimum(stage + 1, last_stage)}, device_id_type=MESH)

        @pl.when(m + 1 < subs)
        def _():
            fetch(m + 1)[1].start()

        for n in range(0, d_model, tile):
            rb[:, n:n + tile] = dot_nn(gmb[...], wot[:, n:n + tile]).astype(BF16)
        qkv_f.wait()
        attend_grad()
        dq_o.start()
        part_copy(m).wait_send()
        for n in range(0, d_model, tile):
            rb[:, n:n + tile] = dot_nn(qkvb[...], wqt[:, n:n + tile]).astype(BF16)
        x_f.wait()

        @pl.when(m >= 2)
        def _():
            gi_out(m - 2).wait()

            @pl.when(stage > 0)
            def _():
                prev_copy(m - 2).wait_send()

        for r in range(0, rows, ROW_CHUNK):
            rr = slice(r, r + ROW_CHUNK)
            total = gmb[rr, :].astype(F32) + norm_grad(xb[rr, :].astype(F32), rb[rr, :].astype(F32), ln[0:1, :], 0)
            gib[slot, rr, :] = total.astype(BF16)

        @pl.when(stage > 0)
        def _():
            @pl.when(m >= RING)
            def _():
                pl.semaphore_wait(dy_free, 1)

            prev_copy(m).start()

        gi_out(m).start()
        dq_o.wait()

        @pl.when(m + 1 < subs)
        def _():
            fetch(m + 1)[2].start()
            fetch(m + 1)[3].start()

    def step(m, carry):
        @pl.when(m < subs)
        def _():
            mlp_part(m)

        @pl.when(m > 0)
        def _():
            attn_part(m - 1)

        return carry

    lax.fori_loop(0, subs + 1, step, 0)
    for acc, out in ((db1, db1_o), (db2, db2_o), (dbo, dbo_o)):
        out[...] = jnp.sum(acc[...], axis=0, keepdims=True)
    dbq_o[...] = jnp.sum(dbq[:, mine_q], axis=0, keepdims=True)
    dln_o[...] = jnp.sum(dln[...], axis=1)
    for copy in outs(subs - 1)[:2]:
        copy.wait()
    for m in (subs - 2, subs - 1):
        gi_out(m).wait()

        @pl.when(stage > 0)
        def _():
            prev_copy(m).wait_send()


ANY = pl.BlockSpec(memory_space=pl.ANY)
VMEM = pl.BlockSpec(memory_space=pltpu.VMEM)
DMA = pltpu.SemaphoreType.DMA
VMEM_LIMIT = 67043328


def fwd_call(stages, width, tile, x_in, wq_own, wq_peer, wo_own, wo_peer, w1, w2, bq, bo, ln, b1, b2):
    subs, rows, d_model = x_in.shape
    ff = w1.shape[1]
    half = d_model // 2

    def hbm(cols, dtype=BF16):
        return jax.ShapeDtypeStruct((subs, rows, cols), dtype)

    def buf(cols, dtype=BF16):
        return pltpu.VMEM((rows, cols), dtype)

    def two(cols):
        return pltpu.VMEM((2, rows, cols), BF16)

    weights = 2 * (4 * d_model * d_model + 2 * d_model * ff)
    return pl.pallas_call(
        functools.partial(fwd_kernel, subs, stages, width, tile),
        name="fwd_stage",
        out_shape=(hbm(d_model), hbm(3 * d_model), hbm(half), hbm(d_model), hbm(d_model), hbm(d_model), hbm(ff, F32), hbm(ff), hbm(d_model)),
        in_specs=[ANY] * 7 + [VMEM] * 5,
        out_specs=[ANY] * 9,
        scratch_shapes=[
            pltpu.VMEM((d_model, 3 * d_model), BF16), pltpu.VMEM((d_model, d_model), BF16), pltpu.VMEM(w1.shape, BF16), pltpu.VMEM(w2.shape, BF16),
            pltpu.VMEM((RING, rows, d_model), BF16), buf(d_model), buf(3 * d_model), buf(d_model), two(d_model), buf(d_model), buf(ff, F32), buf(ff), two(d_model), pltpu.VMEM((RING, rows, d_model), BF16), two(d_model),
            pltpu.VMEM((2, 4, rows, rows), F32), pltpu.VMEM((2, 4, rows, rows), BF16),
            DMA((6,)), DMA((2,)), DMA((7,)), DMA((2,)), DMA((2,)), DMA((2,)), DMA((subs,)), DMA((2,)), DMA((subs,)), pltpu.SemaphoreType.REGULAR,
        ],
        cost_estimate=pl.CostEstimate(flops=subs * rows * weights, bytes_accessed=weights + subs * rows * d_model * 30, transcendentals=subs * rows * (ff + rows * 16)),
        compiler_params=pltpu.CompilerParams(collective_id=0, has_side_effects=True, vmem_limit_bytes=VMEM_LIMIT),
    )(x_in, wq_own, wq_peer, wo_own, wo_peer, w1, w2, bq, bo, ln, b1, b2)


def bwd_call(stages, width, tile, dy_in, x_all, mid_all, s_all, qkv_all, w2t, w1t, wot_own, wot_peer, wqt_own, wqt_peer, ln):
    subs, rows, d_model = dy_in.shape
    ff = s_all.shape[2]
    half = d_model // 2

    def hbm(cols, dtype=BF16):
        return jax.ShapeDtypeStruct((subs, rows, cols), dtype)

    def buf(cols, dtype=BF16):
        return pltpu.VMEM((rows, cols), dtype)

    def two(cols):
        return pltpu.VMEM((2, rows, cols), BF16)

    ring = pltpu.VMEM((RING, rows, d_model), BF16)

    def acc(*shape):
        return jax.ShapeDtypeStruct(shape, F32)

    weights = 2 * (4 * d_model * d_model + 2 * d_model * ff)
    return pl.pallas_call(
        functools.partial(bwd_kernel, subs, stages, width, tile),
        name="bwd_stage",
        out_shape=(hbm(d_model), hbm(ff), hbm(d_model), hbm(3 * half), hbm(d_model),
                   acc(1, ff), acc(1, d_model), acc(1, d_model), acc(1, 3 * half), acc(4, d_model)),
        in_specs=[ANY] * 11 + [VMEM],
        out_specs=[ANY] * 5 + [VMEM] * 5,
        scratch_shapes=[
            pltpu.VMEM(w2t.shape, BF16), pltpu.VMEM(w1t.shape, BF16), pltpu.VMEM((d_model, d_model), BF16), pltpu.VMEM((3 * d_model, d_model), BF16),
            ring, buf(ff, F32), buf(ff), two(d_model), ring, buf(d_model), buf(d_model), buf(d_model), buf(d_model), buf(3 * d_model), two(d_model),
            pltpu.VMEM((4, rows, rows), F32), pltpu.VMEM((4, rows, rows), F32), pltpu.VMEM((4, rows, rows), BF16), pltpu.VMEM((4, rows, rows), BF16),
            pltpu.VMEM((8, ff), F32), pltpu.VMEM((8, d_model), F32), pltpu.VMEM((8, d_model), F32), pltpu.VMEM((8, 3 * d_model), F32), pltpu.VMEM((4, 8, d_model), F32),
            DMA((6,)), DMA((2,)), DMA((4,)), DMA((3,)), DMA((2,)), DMA((2,)), DMA((2,)), DMA((subs,)), DMA((2,)), DMA((subs,)), pltpu.SemaphoreType.REGULAR,
        ],
        cost_estimate=pl.CostEstimate(flops=subs * rows * weights, bytes_accessed=weights + subs * rows * d_model * 30, transcendentals=subs * rows * (ff + rows * 16)),
        compiler_params=pltpu.CompilerParams(collective_id=1, has_side_effects=True, vmem_limit_bytes=VMEM_LIMIT),
    )(dy_in, x_all, mid_all, s_all, qkv_all, w2t, w1t, wot_own, wot_peer, wqt_own, wqt_peer, ln)


def grad_kernel(n_tile, left, right, *refs):
    if len(refs) == 3:
        kept, out, kept_out = refs
        kept_out[...] = kept[...]
    else:
        out, = refs

    @pl.when(pl.program_id(1) == 0)
    def _():
        out[...] = jnp.zeros_like(out)

    for n in range(0, out.shape[1], n_tile):
        lanes = slice(n, n + n_tile)
        out[:, lanes] += dot_tn(left[...], right[:, lanes])


def grad_call(left, right, m_block, n_block, k_block, kept=None):
    tokens, m_size = left.shape
    n_size = right.shape[1]
    m_count = m_size // m_block
    grid = (m_count * (n_size // n_block), tokens // k_block)
    in_specs = [pl.BlockSpec((k_block, m_block), lambda i, k: (k, i % m_count)), pl.BlockSpec((k_block, n_block), lambda i, k: (k, i // m_count))]
    out_specs = [pl.BlockSpec((m_block, n_block), lambda i, k: (i % m_count, i // m_count))]
    out_shape = [jax.ShapeDtypeStruct((m_size, n_size), F32)]
    args = [left, right]
    if kept is not None:
        steps = grid[0] * grid[1]
        assert kept.shape[0] % steps == 0
        spec = pl.BlockSpec((kept.shape[0] // steps,) + kept.shape[1:], lambda i, k: (i * grid[1] + k, 0, 0))
        in_specs.append(spec)
        out_specs.append(spec)
        out_shape.append(jax.ShapeDtypeStruct(kept.shape, kept.dtype))
        args.append(kept)
    moved = 2 * tokens * (m_size * (n_size // n_block) + n_size * m_count) + 4 * m_size * n_size
    return pl.pallas_call(
        functools.partial(grad_kernel, 512),
        name="weight_grad",
        grid=grid,
        in_specs=in_specs,
        out_specs=out_specs,
        out_shape=out_shape,
        cost_estimate=pl.CostEstimate(flops=2 * tokens * m_size * n_size, bytes_accessed=moved, transcendentals=0),
        compiler_params=pltpu.CompilerParams(dimension_semantics=("arbitrary", "arbitrary"), vmem_limit_bytes=VMEM_LIMIT),
    )(*args)


def solution(mesh):
    stages = mesh.shape["pp"]
    swap = [(0, 1), (1, 0)]

    def stage_program(x_in, dy_out, w_qkv, b_qkv, w_out, b_out, ln_par, w_fc1, b_fc1, w_fc2, b_fc2):
        micro, batch, rows, d_model = x_in.shape
        heads, width = w_qkv.shape[3:]
        half = heads * width
        subs = micro * batch
        tile = half
        tp_me = lax.axis_index("tp")

        wqt_own = jnp.transpose(w_qkv[0], (0, 2, 3, 1)).reshape(3 * half, d_model)
        wo_own = w_out[0].reshape(half, d_model)
        wo_peer = lax.ppermute(wo_own, "tp", swap)
        wqt_peer = lax.ppermute(wqt_own, "tp", swap)
        bq_own = b_qkv[0].reshape(1, 3 * half)
        bq_peer = lax.ppermute(bq_own, "tp", swap)
        bq = jnp.concatenate([jnp.where(tp_me == 0, bq_own, bq_peer), jnp.where(tp_me == 0, bq_peer, bq_own)], axis=1).astype(F32)
        w1, w2 = w_fc1[0], w_fc2[0]
        ln = ln_par[0].astype(F32)
        x_all, qkv_all, o_all, mid_all, h1_all, h2_all, s_all, a_all, y_all = fwd_call(
            stages, width, tile, x_in.reshape(subs, rows, d_model), wqt_own.T, wqt_peer.T, wo_own, wo_peer, w1, w2, bq, b_out.astype(F32), ln, b_fc1.astype(F32), b_fc2.astype(F32))
        dy_all, dpre_all, gmid_all, dqkv_all, gin_all, db1, db2, dbo, dbq, dln = bwd_call(
            stages, width, tile, dy_out.reshape(subs, rows, d_model), x_all, mid_all, s_all, qkv_all, w2.T, w1.T, wo_own.T, wo_peer.T, wqt_own, wqt_peer, ln)

        def flat(stack):
            return stack.reshape(subs * rows, -1)

        g_w_fc2, h_out = grad_call(flat(a_all), flat(dy_all), 1024, d_model, 1536, y_all)
        g_w_fc1, g_in = grad_call(flat(h2_all), flat(dpre_all), d_model, 1024, 1536, gin_all)
        g_w_out, = grad_call(flat(o_all), flat(gmid_all), half, d_model, 1536)
        g_w_qkv = lax.optimization_barrier(dot_tn(flat(dqkv_all), flat(h1_all)))
        g_w_out = g_w_out.reshape(heads, width, d_model)
        g_w_qkv = jnp.transpose(g_w_qkv.reshape(3, heads, width, d_model), (0, 3, 1, 2))
        g_b_qkv = dbq.reshape(3, heads, width)
        act = (1, micro, batch, rows, d_model)
        return (h_out.reshape(act), g_in.reshape(act), g_w_qkv[None], g_b_qkv[None], g_w_out[None], dbo,
                dln[None], g_w_fc1[None], db1, g_w_fc2[None], db2)

    act_spec = P(None, "dp", None, None)
    arg_specs = (act_spec, act_spec,
                 P("pp", None, None, "tp", None), P("pp", None, "tp", None), P("pp", "tp", None, None),
                 P("pp", None), P("pp", None, None), P("pp", None, "tp"), P("pp", "tp"),
                 P("pp", "tp", None), P("pp", None))
    stage_spec = P("pp", None, "dp", None, None)
    grad_axes = ("dp", "pp")
    result_specs = (stage_spec, stage_spec,
                    P(grad_axes, None, None, "tp", None), P(grad_axes, None, "tp", None), P(grad_axes, "tp", None, None),
                    P(grad_axes, None), P(grad_axes, None, None), P(grad_axes, None, "tp"), P(grad_axes, "tp"),
                    P(grad_axes, "tp", None), P(grad_axes, None))
    return jax.shard_map(stage_program, mesh=mesh, in_specs=arg_specs, out_specs=result_specs, check_vma=False)
```

```python
import functools

import jax
import jax.numpy as jnp
from jax import lax
from jax.experimental import pallas as pl
from jax.experimental.pallas import tpu as pltpu
from jax.sharding import PartitionSpec as P

LN_EPS = 1e-5
F32 = jnp.float32
BF16 = jnp.bfloat16
MESH = pl.DeviceIdType.MESH
NEG = -1e30
ROW_CHUNK = 32
GELU_C = 0.7978845608028654
GELU_K = 0.044715
LOG2_E = 1.4426950408889634
SOFT_ROWS = 64
RING = 4
LANES = 128
RELAYED = 2

WINDOWS = ((0, 128, 0), (0, 256, 96), (128, 256, 64), (256, 128, 32))


def parity(m):
    return lax.rem(m, 2)


def ring_slot(m):
    return lax.rem(m, RING)


def dot_nn(lhs, rhs):
    return lax.dot_general(lhs, rhs, (((1,), (0,)), ((), ())), preferred_element_type=F32)


def dot_nt(lhs, rhs):
    return lax.dot_general(lhs, rhs, (((1,), (1,)), ((), ())), preferred_element_type=F32)


def dot_tn(lhs, rhs):
    return lax.dot_general(lhs, rhs, (((0,), (0,)), ((), ())), preferred_element_type=F32)


def head_only(window, offset, width):
    lane = lax.broadcasted_iota(jnp.int32, window.shape, 1)
    return jnp.where((lane >= offset) & (lane < offset + width), window, jnp.zeros_like(window))


def join_heads(parts, width):
    lane = lax.broadcasted_iota(jnp.int32, (parts[0].shape[0], LANES), 1)
    first = jnp.where(lane < width, parts[0], parts[1][:, :LANES])
    second = jnp.where(lane < 2 * width - LANES, parts[1][:, LANES:], parts[2][:, :LANES])
    third = jnp.where(lane < 3 * width - 256, parts[2][:, LANES:], parts[3])
    return first, second, third


def norm_stats(x_wide):
    centered = x_wide - jnp.mean(x_wide, axis=-1, keepdims=True)
    inv_std = lax.rsqrt(jnp.mean(centered * centered, axis=-1, keepdims=True) + LN_EPS)
    return centered * inv_std, inv_std


def fold_rows(block):
    rows, cols = block.shape
    return jnp.sum(block.reshape(rows // 8, 8, cols), axis=0)


def neighbour_barrier(stage, tp_peer, stages):
    barrier = pltpu.get_barrier_semaphore()
    pl.semaphore_signal(barrier, inc=1, device_id={"tp": tp_peer}, device_id_type=MESH)
    for step in range(1, stages):
        pl.semaphore_signal(barrier, inc=1, device_id={"pp": lax.rem(stage + step, stages)}, device_id_type=MESH)
    pl.semaphore_wait(barrier, stages)


def fwd_kernel(subs, stages, width, tile,
               x_in, wqt_h, wo_h, w1_h, w2_h, bq, bo_h, b1_h, b2_h, ln_h,
               x_all, qkv_all, o_all, mid_all, h1_all, h2_all, s_all, a_all, y_all, wqt_p, wot_o, w1t_o, w2t_o, relay_in, relay_out,
               wq, wo, w1, w2, xr, h1b, qkvb, ob, midb, h2b, slb, ab, partb, peerb, yb, sb, pb, bqb, tb, par,
               w_sem, t_sem, wq_send, wq_recv, wo_send, wo_recv, bq_send, bq_recv, relay_send, relay_recv, in_sem, out_sem, mid_sem, y_sem, part_send, part_recv, y_send, x_recv, x_free):
    stage = lax.axis_index("pp")
    tp_me = lax.axis_index("tp")
    tp_peer = 1 - tp_me
    last_stage = stages - 1
    _, rows, d_model = xr.shape
    half = d_model // 2
    ff = slb.shape[1]
    scale = width ** -0.5
    log2_scale = scale * LOG2_E

    first = 0
    rows_of = []
    for row in (bo_h, b1_h, b2_h, *(ln_h.at[i:i + 1, :] for i in range(4))):
        lanes = slice(first, first + row.shape[1])
        par[:, lanes] = row[...].astype(F32)
        rows_of.append(par.at[:, lanes])
        first = lanes.stop
    bo, b1, b2, *ln = rows_of
    mine = pl.ds(pl.multiple_of(tp_me * half, LANES), half)
    piece = 256
    pieces = 3 * half // piece
    peer_id = {"device_id": {"tp": tp_peer}, "device_id_type": MESH}
    loads = [pltpu.make_async_copy(src, dst, w_sem.at[i]) for i, (src, dst) in enumerate(((wo_h, wo.at[mine, :]), (w1_h, w1), (w2_h, w2)))]

    def cut(p):
        return pl.ds(pl.multiple_of(p * piece, piece), piece)

    def wq_copy(p):
        return pltpu.make_async_remote_copy(src_ref=wqt_h.at[cut(p), :], dst_ref=wqt_p.at[cut(p), :], send_sem=wq_send.at[p], recv_sem=wq_recv.at[p], **peer_id)

    wo_copy = pltpu.make_async_remote_copy(src_ref=wo_h, dst_ref=wo.at[mine, :], send_sem=wo_send, recv_sem=wo_recv, **peer_id)
    bq_copy = pltpu.make_async_remote_copy(src_ref=bq, dst_ref=bqb.at[tp_me], send_sem=bq_send, recv_sem=bq_recv, **peer_id)

    column = stages // 2
    direct = pieces - RELAYED

    def relay_copy(leg, r):
        src = (wqt_h.at[cut(direct + r), :], relay_in.at[r], relay_out.at[r])[leg]
        dst = (relay_in.at[r], relay_out.at[r], wqt_p.at[cut(direct + r), :])[leg]
        there = ({"pp": jnp.minimum(stage + column, last_stage)}, {"tp": tp_peer}, {"pp": jnp.maximum(stage - column, 0)})[leg]
        recv_sem = wq_recv.at[direct + r] if leg == 2 else relay_recv.at[leg, r]
        return pltpu.make_async_remote_copy(src_ref=src, dst_ref=dst, send_sem=relay_send.at[leg, r], recv_sem=recv_sem, device_id=there, device_id_type=MESH)

    def moved(src, dst):
        copy = pltpu.make_async_copy(src, dst, t_sem)
        copy.start()
        copy.wait()

    def turn(source, owner, p):
        moved(source.at[cut(p), :], h1b)
        wq[:, pl.ds(pl.multiple_of(owner * (3 * half) + p * piece, LANES), piece)] = jnp.transpose(h1b[...])

    def exchange_weights():
        def send(p, carry):
            wq_copy(p).start()
            return carry

        def own(p, carry):
            turn(wqt_h, tp_me, p)
            return carry

        def turn_w1(p, carry):
            h2b[...] = jnp.transpose(w1[:, cut(p)])
            moved(h2b, w1t_o.at[cut(p), :])
            return carry

        def turn_w2(p, carry):
            tb[...] = jnp.transpose(w2[cut(p), :])
            moved(tb, w2t_o.at[:, cut(p)])
            return carry

        def received(p, carry):
            wq_copy(p).wait_recv()
            turn(wqt_p, tp_peer, p)
            return carry

        bq_copy.start()
        for load in loads:
            load.start()
        lax.fori_loop(0, RELAYED, send, 0)

        @pl.when(stage < column)
        def _():
            for r in range(RELAYED):
                relay_copy(0, r).start()
            lax.fori_loop(RELAYED, direct, send, 0)

        @pl.when(stage >= column)
        def _():
            for r in range(RELAYED):
                relay_copy(0, r).wait_recv()
                relay_copy(1, r).start()
            lax.fori_loop(RELAYED, pieces, send, 0)

        wo_copy.start()
        bqb[tp_me] = bq[...]
        lax.fori_loop(0, pieces, own, 0)
        for load in loads:
            load.wait()
        lax.fori_loop(0, ff // piece, turn_w1, 0)
        lax.fori_loop(0, ff // piece, turn_w2, 0)

        @pl.when(stage >= column)
        def _():
            for r in range(RELAYED):
                relay_copy(1, r).wait_recv()
                relay_copy(2, r).start()

        bq_copy.wait_recv()
        middle = direct // 2
        for first, last in ((0, middle), (direct, pieces), (middle, direct)):
            lax.fori_loop(first, last, received, 0)

    pb[:, :, 0:LANES, LANES:rows] = jnp.zeros((2, 4, LANES, rows - LANES), BF16)
    neighbour_barrier(stage, tp_peer, stages)

    def outs(m):
        return (pltpu.make_async_copy(h1b, h1_all.at[m], out_sem.at[0]),
                pltpu.make_async_copy(qkvb, qkv_all.at[m], out_sem.at[1]),
                pltpu.make_async_copy(ob.at[:, pl.ds(pl.multiple_of(tp_me * half, LANES), half)], o_all.at[m], out_sem.at[2]),
                pltpu.make_async_copy(h2b, h2_all.at[m], out_sem.at[3]),
                pltpu.make_async_copy(slb, s_all.at[m], out_sem.at[4]),
                pltpu.make_async_copy(ab, a_all.at[m], out_sem.at[5]),
                pltpu.make_async_copy(xr.at[ring_slot(m)], x_all.at[m], out_sem.at[6]))

    def mid_out(m):
        slot = parity(m)
        return pltpu.make_async_copy(midb.at[slot], mid_all.at[m], mid_sem.at[slot])

    def y_out(m):
        slot = parity(m)
        return pltpu.make_async_copy(yb.at[slot], y_all.at[m], y_sem.at[slot])

    def part_copy(m):
        slot = parity(m)
        return pltpu.make_async_remote_copy(src_ref=partb.at[slot], dst_ref=peerb.at[ring_slot(m)], send_sem=part_send.at[slot], recv_sem=part_recv.at[m],
                                            device_id={"tp": tp_peer}, device_id_type=MESH)

    def next_copy(m):
        slot = parity(m)
        return pltpu.make_async_remote_copy(src_ref=yb.at[slot], dst_ref=xr.at[ring_slot(m)], send_sem=y_send.at[slot], recv_sem=x_recv.at[m],
                                            device_id={"pp": jnp.minimum(stage + 1, last_stage)}, device_id_type=MESH)

    def x_load(m):
        return pltpu.make_async_copy(x_in.at[m], xr.at[ring_slot(m)], in_sem.at[parity(m)])

    @pl.when(stage == 0)
    def _():
        x_load(0).start()

    def layer_norm(src, dst, gain, shift):
        for r in range(0, rows, ROW_CHUNK):
            normed, _ = norm_stats(src[r:r + ROW_CHUNK, :].astype(F32))
            dst[r:r + ROW_CHUNK, :] = (normed * gain + shift).astype(BF16)

    def group_base(group):
        return (group // 2) * (3 * half) + (group % 2) * (4 * width)

    def attend():
        def scores(group):
            base = group_base(group)
            for j, (start, size, offset) in enumerate(WINDOWS):
                query = head_only(qkvb[:, base + start:base + start + size], offset, width)
                key = qkvb[:, base + half + start:base + half + start + size]
                sb[group % 2, j] = dot_nt(query, key)

        def softmax(group):
            for j in range(4):
                for r0 in range(0, rows, SOFT_ROWS):
                    keys = LANES * (r0 // LANES + 1)
                    row = lax.broadcasted_iota(jnp.int32, (SOFT_ROWS, keys), 0) + r0
                    col = lax.broadcasted_iota(jnp.int32, (SOFT_ROWS, keys), 1)
                    score = jnp.where(row >= col, sb[group % 2, j, r0:r0 + SOFT_ROWS, 0:keys], NEG)
                    weight = jnp.exp2((score - jnp.max(score, axis=1, keepdims=True)) * log2_scale)
                    inv = 1.0 / jnp.sum(weight, axis=1, keepdims=True)
                    pb[group % 2, j, r0:r0 + SOFT_ROWS, 0:keys] = (weight * inv).astype(BF16)

        def values(group):
            base = group_base(group) + 2 * half
            parts = [dot_nn(pb[group % 2, j], qkvb[:, base + start:base + start + size]) for j, (start, size, _) in enumerate(WINDOWS)]
            for i, piece in enumerate(join_heads(parts, width)):
                first = group * (4 * width) + i * LANES
                ob[:, first:first + LANES] = piece.astype(BF16)

        groups = d_model // (4 * width)
        scores(0)
        for group in range(groups):
            if group + 1 < groups:
                scores(group + 1)
            softmax(group)
            values(group)

    def finish(m):
        slot = parity(m)
        peer_slot = ring_slot(m)
        part_copy(m).wait_recv()

        @pl.when(m >= 2)
        def _():
            y_out(m - 2).wait()

            @pl.when(stage < last_stage)
            def _():
                next_copy(m - 2).wait_send()

        for r in range(0, rows, ROW_CHUNK):
            both = partb[slot, r:r + ROW_CHUNK, :].astype(F32) + peerb[peer_slot, r:r + ROW_CHUNK, :].astype(F32)
            yb[slot, r:r + ROW_CHUNK, :] = (midb[slot, r:r + ROW_CHUNK, :].astype(F32) + both + b2[...]).astype(BF16)

        @pl.when(stage < last_stage)
        def _():
            @pl.when(m >= RING)
            def _():
                pl.semaphore_wait(x_free, 1)

            next_copy(m).start()

        y_out(m).start()
        part_copy(m).wait_send()

    def attn_part(m):
        slot = parity(m)
        prev = jnp.maximum(m - 1, 0)
        h1_o, qkv_o, o_o, h2_o, _, _, x_o = outs(m)
        h1_p, qkv_p, o_p, h2_p, _, _, x_p = outs(prev)

        @pl.when(stage == 0)
        def _():
            x_load(m).wait()

            @pl.when(m + 1 < subs)
            def _():
                x_load(m + 1).start()

        @pl.when(stage > 0)
        def _():
            next_copy(m).wait_recv()

        x_o.start()
        xb = xr.at[ring_slot(m)]

        @pl.when(m > 0)
        def _():
            h1_p.wait()
            qkv_p.wait()
            o_p.wait()
            h2_p.wait()

        layer_norm(xb, h1b, ln[0][...], ln[1][...])
        h1_o.start()

        for n in range(0, 3 * d_model, tile):
            owner, lane = divmod(n, 3 * half)
            qkvb[:, n:n + tile] = (dot_nn(h1b[...], wq[:, n:n + tile]) + bqb[owner, :, lane:lane + tile].astype(F32)).astype(BF16)
        qkv_o.start()
        attend()
        o_o.start()

        @pl.when(m == 0)
        def _():
            wo_copy.wait_recv()

        @pl.when(m >= 2)
        def _():
            mid_out(m - 2).wait()

        for n in range(0, d_model, tile):
            midb[slot, :, n:n + tile] = (xb[:, n:n + tile].astype(F32) + dot_nn(ob[...], wo[:, n:n + tile]) + bo[:, n:n + tile]).astype(BF16)
        mid_out(m).start()
        x_o.wait()

        @pl.when((stage > 0) & (m < subs - RING))
        def _():
            pl.semaphore_signal(x_free, inc=1, device_id={"pp": jnp.maximum(stage - 1, 0)}, device_id_type=MESH)

        layer_norm(midb.at[slot], h2b, ln[2][...], ln[3][...])
        h2_o.start()

    def mlp_part(m):
        slot = parity(m)
        _, _, _, _, s_o, a_o, _ = outs(m)
        _, _, _, _, s_p, a_p, _ = outs(jnp.maximum(m - 1, 0))

        @pl.when(m > 0)
        def _():
            s_p.wait()
            a_p.wait()

        for n in range(0, ff, tile):
            pre = dot_nn(h2b[...], w1[:, n:n + tile]) + b1[:, n:n + tile]
            square = pre * pre
            bend = jnp.tanh(pre * (GELU_C + (GELU_C * GELU_K) * square))
            cdf = 0.5 + 0.5 * bend
            ab[:, n:n + tile] = (pre * cdf).astype(BF16)
            slb[:, n:n + tile] = cdf + (0.5 * pre) * (1.0 - bend * bend) * (GELU_C + (3.0 * GELU_C * GELU_K) * square)
        s_o.start()
        a_o.start()
        for n in range(0, d_model, tile):
            partb[slot, :, n:n + tile] = dot_nn(ab[...], w2[:, n:n + tile]).astype(BF16)
        part_copy(m).start()

    def step(m, carry):
        @pl.when(m < subs)
        def _():
            attn_part(m)
            mlp_part(m)

        @pl.when((m >= 1) & (m <= d_model // piece))
        def _():
            tb[...] = jnp.transpose(wo[cut(m - 1), :])
            moved(tb, wot_o.at[:, cut(m - 1)])

        @pl.when(m > 0)
        def _():
            finish(m - 1)

        return carry

    exchange_weights()
    lax.fori_loop(0, subs + 1, step, 0)

    def sent(p, carry):
        wq_copy(p).wait_send()
        return carry

    lax.fori_loop(0, direct, sent, 0)

    @pl.when(stage < column)
    def _():
        for r in range(RELAYED):
            relay_copy(0, r).wait_send()

    @pl.when(stage >= column)
    def _():
        lax.fori_loop(direct, pieces, sent, 0)
        for r in range(RELAYED):
            relay_copy(1, r).wait_send()
            relay_copy(2, r).wait_send()

    wo_copy.wait_send()
    bq_copy.wait_send()
    h1_o, qkv_o, o_o, h2_o, s_o, a_o, x_o = outs(subs - 1)
    for copy in (h1_o, qkv_o, o_o, h2_o, s_o, a_o):
        copy.wait()

    for m in (subs - 2, subs - 1):
        mid_out(m).wait()
        y_out(m).wait()

        @pl.when(stage < last_stage)
        def _():
            next_copy(m).wait_send()


def bwd_kernel(subs, stages, width, tile,
               dy_in, x_all, mid_all, s_all, qkv_all, w2t_h, w1t_h, wot_h, wqt_h, wqt_p, ln_h,
               dy_all, dpre_all, gmid_all, dqkv_all, gin_all, db1_o, db2_o, dbo_o, dbq_o, dln_o,
               w2t, w1t, wot, wqt, dyb, slb, dpb, partb, peerb, rb, midb, xb, gmb, qkvb, gib, sb, db, pb, dsb, db1, db2, dbo, dbq, dln, ln,
               w_sem, in_sem, pre_sem, out_sem, dy_sem, gi_sem, part_send, part_recv, gi_send, dy_recv, dy_free):
    stage = lax.axis_index("pp")
    tp_me = lax.axis_index("tp")
    tp_peer = 1 - tp_me
    last_stage = stages - 1
    rows, d_model = xb.shape
    half = d_model // 2
    ff = slb.shape[1]
    scale = width ** -0.5
    log2_scale = scale * LOG2_E

    ln[...] = ln_h[...].astype(F32)
    mine_q = pl.ds(pl.multiple_of(tp_me * (3 * half), LANES), 3 * half)
    theirs_q = pl.ds(pl.multiple_of(tp_peer * (3 * half), LANES), 3 * half)
    loads = [pltpu.make_async_copy(src, dst, w_sem.at[i]) for i, (src, dst) in enumerate((
        (w2t_h, w2t), (w1t_h, w1t), (wot_h, wot), (wqt_h, wqt.at[mine_q, :]), (wqt_p, wqt.at[theirs_q, :])))]

    def fetch(m):
        return (pltpu.make_async_copy(s_all.at[m], slb, pre_sem.at[0]),
                pltpu.make_async_copy(mid_all.at[m], midb, pre_sem.at[1]),
                pltpu.make_async_copy(qkv_all.at[m], qkvb, pre_sem.at[2]),
                pltpu.make_async_copy(x_all.at[m], xb, pre_sem.at[3]))

    fetch(0)[0].start()
    for load in loads[:2]:
        load.start()
    for copy in fetch(0)[1:]:
        copy.start()
    for acc in (db1, db2, dbo, dbq, dln):
        acc[...] = jnp.zeros_like(acc)
    for acc in (pb, dsb):
        acc[:, LANES:rows, 0:LANES] = jnp.zeros((4, rows - LANES, LANES), BF16)
    neighbour_barrier(stage, tp_peer, stages)

    def outs(m):
        return (pltpu.make_async_copy(dpb, dpre_all.at[m], out_sem.at[0]),
                pltpu.make_async_copy(gmb, gmid_all.at[m], out_sem.at[1]),
                pltpu.make_async_copy(qkvb.at[:, pl.ds(pl.multiple_of(tp_me * (3 * half), LANES), 3 * half)], dqkv_all.at[m], out_sem.at[2]))

    def dy_load(m):
        return pltpu.make_async_copy(dy_in.at[m], dyb.at[ring_slot(m)], in_sem.at[parity(m)])

    def dy_out(m):
        return pltpu.make_async_copy(dyb.at[ring_slot(m)], dy_all.at[m], dy_sem.at[parity(m)])

    def gi_out(m):
        slot = parity(m)
        return pltpu.make_async_copy(gib.at[slot], gin_all.at[m], gi_sem.at[slot])

    def part_copy(m):
        slot = parity(m)
        return pltpu.make_async_remote_copy(src_ref=partb.at[slot], dst_ref=peerb.at[ring_slot(m)], send_sem=part_send.at[slot], recv_sem=part_recv.at[m],
                                            device_id={"tp": tp_peer}, device_id_type=MESH)

    def prev_copy(m):
        slot = parity(m)
        return pltpu.make_async_remote_copy(src_ref=gib.at[slot], dst_ref=dyb.at[ring_slot(m)], send_sem=gi_send.at[slot], recv_sem=dy_recv.at[m],
                                            device_id={"pp": jnp.maximum(stage - 1, 0)}, device_id_type=MESH)

    @pl.when(stage == last_stage)
    def _():
        dy_load(0).start()

    def norm_grad(x_rows, grad, gain, which):
        normed, inv_std = norm_stats(x_rows)
        dln[which] += fold_rows(grad * normed)
        dln[which + 1] += fold_rows(grad)
        scaled = grad * gain
        mean_scaled = jnp.mean(scaled, axis=-1, keepdims=True)
        mean_proj = jnp.mean(scaled * normed, axis=-1, keepdims=True)
        return inv_std * (scaled - mean_scaled - normed * mean_proj)

    def mlp_part(m):
        slot = parity(m)
        slope_f = fetch(m)[0]

        dy_slot = ring_slot(m)

        @pl.when(stage == last_stage)
        def _():
            dy_load(m).wait()

            @pl.when(m + 1 < subs)
            def _():
                dy_load(m + 1).start()

        @pl.when(stage < last_stage)
        def _():
            prev_copy(m).wait_recv()

        dy_out(m).start()

        @pl.when(m == 0)
        def _():
            loads[0].wait()
            for load in loads[2:]:
                load.start()

        @pl.when(m > 0)
        def _():
            outs(m - 1)[0].wait()

        slope_f.wait()
        for n in range(0, ff, tile):
            grad = dot_nn(dyb[dy_slot], w2t[:, n:n + tile]).astype(BF16).astype(F32) * slb[:, n:n + tile]
            db1[:, n:n + tile] += fold_rows(grad)
            dpb[:, n:n + tile] = grad.astype(BF16)
        outs(m)[0].start()

        @pl.when(m + 1 < subs)
        def _():
            fetch(m + 1)[0].start()

        @pl.when(m == 0)
        def _():
            loads[1].wait()

        for n in range(0, d_model, tile):
            partb[slot, :, n:n + tile] = dot_nn(dpb[...], w1t[:, n:n + tile]).astype(BF16)
        part_copy(m).start()

    def attend_grad():
        def window(base, spec):
            start, size, offset = spec
            return slice(base + start, base + start + size), offset

        def scores(group, base):
            for j, spec in enumerate(WINDOWS):
                q_lanes, offset = window(base, spec)
                k_lanes, _ = window(base + half, spec)
                v_lanes, _ = window(base + 2 * half, spec)
                d_lanes, _ = window(group * (4 * width), spec)
                sb[j] = dot_nt(qkvb[:, k_lanes], head_only(qkvb[:, q_lanes], offset, width))
                db[j] = dot_nt(qkvb[:, v_lanes], head_only(rb[:, d_lanes], offset, width))

        def softmax():
            for j in range(4):
                for q0 in range(0, rows, LANES):
                    keys, lanes = q0 + LANES, slice(q0, q0 + LANES)
                    krow = lax.broadcasted_iota(jnp.int32, (keys, LANES), 0)
                    qcol = lax.broadcasted_iota(jnp.int32, (keys, LANES), 1) + q0
                    score = jnp.where(qcol >= krow, sb[j, 0:keys, lanes], NEG)
                    weight = jnp.exp2((score - jnp.max(score, axis=0, keepdims=True)) * log2_scale)
                    prob = weight * (1.0 / jnp.sum(weight, axis=0, keepdims=True))
                    pb[j, 0:keys, lanes] = prob.astype(BF16)
                    d_prob = db[j, 0:keys, lanes]
                    d_score = prob * (d_prob - jnp.sum(prob * d_prob, axis=0, keepdims=True))
                    dsb[j, 0:keys, lanes] = d_score.astype(BF16)

        def products(group, base):
            d_query, d_key, d_value = [], [], []
            for j, spec in enumerate(WINDOWS):
                q_lanes, _ = window(base, spec)
                k_lanes, _ = window(base + half, spec)
                d_lanes, _ = window(group * (4 * width), spec)
                d_value.append(dot_nn(pb[j], rb[:, d_lanes]))
                d_key.append(dot_nn(dsb[j], qkvb[:, q_lanes]) * scale)
                d_query.append(dot_tn(dsb[j], qkvb[:, k_lanes]) * scale)
            for c, parts in enumerate((d_query, d_key, d_value)):
                for i, piece in enumerate(join_heads(parts, width)):
                    piece = piece.astype(BF16)
                    first = base + c * half + i * LANES
                    qkvb[:, first:first + LANES] = piece
                    dbq[:, first:first + LANES] += fold_rows(piece.astype(F32))

        for group in range(d_model // (4 * width)):
            base = (group // 2) * (3 * half) + (group % 2) * (4 * width)
            scores(group, base)
            softmax()
            products(group, base)

    def attn_part(m):
        slot = parity(m)
        _, mid_f, qkv_f, x_f = fetch(m)
        _, gm_o, dq_o = outs(m)
        peer_slot = ring_slot(m)
        dy_slot = ring_slot(m)
        mid_f.wait()

        @pl.when(m > 0)
        def _():
            outs(m - 1)[1].wait()

        @pl.when(m == 0)
        def _():
            for load in loads[2:]:
                load.wait()

        part_copy(m).wait_recv()
        for r in range(0, rows, ROW_CHUNK):
            rr = slice(r, r + ROW_CHUNK)
            grad = (partb[slot, rr, :].astype(F32) + peerb[peer_slot, rr, :].astype(F32)).astype(BF16).astype(F32)
            d_y = dyb[dy_slot, rr, :].astype(F32)
            db2[...] += fold_rows(d_y)
            total = d_y + norm_grad(midb[rr, :].astype(F32), grad, ln[2:3, :], 2)
            gmb[rr, :] = total.astype(BF16)
            dbo[...] += fold_rows(total)
        gm_o.start()
        dy_out(m).wait()

        @pl.when((stage < last_stage) & (m < subs - RING))
        def _():
            pl.semaphore_signal(dy_free, inc=1, device_id={"pp": jnp.minimum(stage + 1, last_stage)}, device_id_type=MESH)

        @pl.when(m + 1 < subs)
        def _():
            fetch(m + 1)[1].start()

        for n in range(0, d_model, tile):
            rb[:, n:n + tile] = dot_nn(gmb[...], wot[:, n:n + tile]).astype(BF16)
        qkv_f.wait()
        attend_grad()
        dq_o.start()
        part_copy(m).wait_send()
        for n in range(0, d_model, tile):
            rb[:, n:n + tile] = dot_nn(qkvb[...], wqt[:, n:n + tile]).astype(BF16)
        x_f.wait()

        @pl.when(m >= 2)
        def _():
            gi_out(m - 2).wait()

            @pl.when(stage > 0)
            def _():
                prev_copy(m - 2).wait_send()

        for r in range(0, rows, ROW_CHUNK):
            rr = slice(r, r + ROW_CHUNK)
            total = gmb[rr, :].astype(F32) + norm_grad(xb[rr, :].astype(F32), rb[rr, :].astype(F32), ln[0:1, :], 0)
            gib[slot, rr, :] = total.astype(BF16)

        @pl.when(stage > 0)
        def _():
            @pl.when(m >= RING)
            def _():
                pl.semaphore_wait(dy_free, 1)

            prev_copy(m).start()

        gi_out(m).start()
        dq_o.wait()

        @pl.when(m + 1 < subs)
        def _():
            fetch(m + 1)[2].start()
            fetch(m + 1)[3].start()

    def step(m, carry):
        @pl.when(m < subs)
        def _():
            mlp_part(m)

        @pl.when(m > 0)
        def _():
            attn_part(m - 1)

        return carry

    lax.fori_loop(0, subs + 1, step, 0)
    for acc, out in ((db1, db1_o), (db2, db2_o), (dbo, dbo_o)):
        out[...] = jnp.sum(acc[...], axis=0, keepdims=True)
    dbq_o[...] = jnp.sum(dbq[:, mine_q], axis=0, keepdims=True)
    dln_o[...] = jnp.sum(dln[...], axis=1)
    for copy in outs(subs - 1)[:2]:
        copy.wait()
    for m in (subs - 2, subs - 1):
        gi_out(m).wait()

        @pl.when(stage > 0)
        def _():
            prev_copy(m).wait_send()


ANY = pl.BlockSpec(memory_space=pl.ANY)
VMEM = pl.BlockSpec(memory_space=pltpu.VMEM)
DMA = pltpu.SemaphoreType.DMA
VMEM_LIMIT = 67043328


def fwd_call(stages, width, tile, x_in, wqt_own, wo_own, w1, w2, bq, bo, b1, b2, ln):
    subs, rows, d_model = x_in.shape
    ff = w1.shape[1]
    half = d_model // 2

    def hbm(cols, dtype=BF16):
        return jax.ShapeDtypeStruct((subs, rows, cols), dtype)

    def buf(cols, dtype=BF16):
        return pltpu.VMEM((rows, cols), dtype)

    def two(cols):
        return pltpu.VMEM((2, rows, cols), BF16)

    weights = 2 * (4 * d_model * d_model + 2 * d_model * ff)
    return pl.pallas_call(
        functools.partial(fwd_kernel, subs, stages, width, tile),
        name="fwd_stage",
        out_shape=(hbm(d_model), hbm(3 * d_model), hbm(half), hbm(d_model), hbm(d_model), hbm(d_model), hbm(ff, F32), hbm(ff), hbm(d_model),
                   jax.ShapeDtypeStruct((3 * half, d_model), BF16), jax.ShapeDtypeStruct((d_model, d_model), BF16), jax.ShapeDtypeStruct((ff, d_model), BF16), jax.ShapeDtypeStruct((d_model, ff), BF16),
                   *[jax.ShapeDtypeStruct((RELAYED, rows, d_model), BF16)] * 2),
        in_specs=[ANY] * 5 + [VMEM] * 5,
        out_specs=[ANY] * 15,
        scratch_shapes=[
            pltpu.VMEM((d_model, 3 * d_model), BF16), pltpu.VMEM((d_model, d_model), BF16), pltpu.VMEM(w1.shape, BF16), pltpu.VMEM(w2.shape, BF16),
            pltpu.VMEM((RING, rows, d_model), BF16), buf(d_model), buf(3 * d_model), buf(d_model), two(d_model), buf(d_model), buf(ff, F32), buf(ff), two(d_model), pltpu.VMEM((RING, rows, d_model), BF16), two(d_model),
            pltpu.VMEM((2, 4, rows, rows), F32), pltpu.VMEM((2, 4, rows, rows), BF16), pltpu.VMEM((2, 1, 3 * half), BF16), pltpu.VMEM((d_model, 256), BF16), pltpu.VMEM((1, ff + 6 * d_model), F32),
            DMA((3,)), DMA, DMA((3 * half // 256,)), DMA((3 * half // 256,)), DMA, DMA, DMA, DMA, DMA((3, RELAYED)), DMA((2, RELAYED)), DMA((2,)), DMA((7,)), DMA((2,)), DMA((2,)), DMA((2,)), DMA((subs,)), DMA((2,)), DMA((subs,)), pltpu.SemaphoreType.REGULAR,
        ],
        cost_estimate=pl.CostEstimate(flops=subs * rows * weights, bytes_accessed=weights + subs * rows * d_model * 30, transcendentals=subs * rows * (ff + rows * 16)),
        compiler_params=pltpu.CompilerParams(collective_id=0, has_side_effects=True, vmem_limit_bytes=VMEM_LIMIT),
    )(x_in, wqt_own, wo_own, w1, w2, bq, bo, b1, b2, ln)


def bwd_call(stages, width, tile, dy_in, x_all, mid_all, s_all, qkv_all, w2t, w1t, wot, wqt_own, wqt_peer, ln):
    subs, rows, d_model = dy_in.shape
    ff = s_all.shape[2]
    half = d_model // 2

    def hbm(cols, dtype=BF16):
        return jax.ShapeDtypeStruct((subs, rows, cols), dtype)

    def buf(cols, dtype=BF16):
        return pltpu.VMEM((rows, cols), dtype)

    def two(cols):
        return pltpu.VMEM((2, rows, cols), BF16)

    ring = pltpu.VMEM((RING, rows, d_model), BF16)

    def acc(*shape):
        return jax.ShapeDtypeStruct(shape, F32)

    weights = 2 * (4 * d_model * d_model + 2 * d_model * ff)
    return pl.pallas_call(
        functools.partial(bwd_kernel, subs, stages, width, tile),
        name="bwd_stage",
        out_shape=(hbm(d_model), hbm(ff), hbm(d_model), hbm(3 * half), hbm(d_model),
                   acc(1, ff), acc(1, d_model), acc(1, d_model), acc(1, 3 * half), acc(4, d_model)),
        in_specs=[ANY] * 10 + [VMEM],
        out_specs=[ANY] * 5 + [VMEM] * 5,
        scratch_shapes=[
            pltpu.VMEM(w2t.shape, BF16), pltpu.VMEM(w1t.shape, BF16), pltpu.VMEM((d_model, d_model), BF16), pltpu.VMEM((3 * d_model, d_model), BF16),
            ring, buf(ff, F32), buf(ff), two(d_model), ring, buf(d_model), buf(d_model), buf(d_model), buf(d_model), buf(3 * d_model), two(d_model),
            pltpu.VMEM((4, rows, rows), F32), pltpu.VMEM((4, rows, rows), F32), pltpu.VMEM((4, rows, rows), BF16), pltpu.VMEM((4, rows, rows), BF16),
            pltpu.VMEM((8, ff), F32), pltpu.VMEM((8, d_model), F32), pltpu.VMEM((8, d_model), F32), pltpu.VMEM((8, 3 * d_model), F32), pltpu.VMEM((4, 8, d_model), F32), pltpu.VMEM((4, d_model), F32),
            DMA((5,)), DMA((2,)), DMA((4,)), DMA((3,)), DMA((2,)), DMA((2,)), DMA((2,)), DMA((subs,)), DMA((2,)), DMA((subs,)), pltpu.SemaphoreType.REGULAR,
        ],
        cost_estimate=pl.CostEstimate(flops=subs * rows * weights, bytes_accessed=weights + subs * rows * d_model * 30, transcendentals=subs * rows * (ff + rows * 16)),
        compiler_params=pltpu.CompilerParams(collective_id=1, has_side_effects=True, vmem_limit_bytes=VMEM_LIMIT),
    )(dy_in, x_all, mid_all, s_all, qkv_all, w2t, w1t, wot, wqt_own, wqt_peer, ln)


def grad_kernel(n_tile, left, right, *refs):
    if len(refs) == 3:
        kept, out, kept_out = refs
        kept_out[...] = kept[...]
    else:
        out, = refs

    @pl.when(pl.program_id(1) == 0)
    def _():
        out[...] = jnp.zeros_like(out)

    for n in range(0, out.shape[1], n_tile):
        lanes = slice(n, n + n_tile)
        out[:, lanes] += dot_tn(left[...], right[:, lanes])


def grad_call(left, right, m_block, n_block, k_block, kept=None):
    tokens, m_size = left.shape
    n_size = right.shape[1]
    m_count = m_size // m_block
    grid = (m_count * (n_size // n_block), tokens // k_block)
    in_specs = [pl.BlockSpec((k_block, m_block), lambda i, k: (k, i % m_count)), pl.BlockSpec((k_block, n_block), lambda i, k: (k, i // m_count))]
    out_specs = [pl.BlockSpec((m_block, n_block), lambda i, k: (i % m_count, i // m_count))]
    out_shape = [jax.ShapeDtypeStruct((m_size, n_size), F32)]
    args = [left, right]
    if kept is not None:
        steps = grid[0] * grid[1]
        assert kept.shape[0] % steps == 0
        spec = pl.BlockSpec((kept.shape[0] // steps,) + kept.shape[1:], lambda i, k: (i * grid[1] + k, 0, 0))
        in_specs.append(spec)
        out_specs.append(spec)
        out_shape.append(jax.ShapeDtypeStruct(kept.shape, kept.dtype))
        args.append(kept)
    moved = 2 * tokens * (m_size * (n_size // n_block) + n_size * m_count) + 4 * m_size * n_size
    return pl.pallas_call(
        functools.partial(grad_kernel, 512),
        name="weight_grad",
        grid=grid,
        in_specs=in_specs,
        out_specs=out_specs,
        out_shape=out_shape,
        cost_estimate=pl.CostEstimate(flops=2 * tokens * m_size * n_size, bytes_accessed=moved, transcendentals=0),
        compiler_params=pltpu.CompilerParams(dimension_semantics=("arbitrary", "arbitrary"), vmem_limit_bytes=VMEM_LIMIT),
    )(*args)


def solution(mesh):
    stages = mesh.shape["pp"]

    def stage_program(x_in, dy_out, w_qkv, b_qkv, w_out, b_out, ln_par, w_fc1, b_fc1, w_fc2, b_fc2):
        micro, batch, rows, d_model = x_in.shape
        heads, width = w_qkv.shape[3:]
        half = heads * width
        subs = micro * batch
        tile = half

        wqt_own = jnp.transpose(w_qkv[0], (0, 2, 3, 1)).reshape(3 * half, d_model)
        ln = ln_par[0]
        x_all, qkv_all, o_all, mid_all, h1_all, h2_all, s_all, a_all, y_all, wqt_peer, wot, w1t, w2t, _, _ = fwd_call(
            stages, width, tile, x_in.reshape(subs, rows, d_model), wqt_own, w_out[0].reshape(half, d_model), w_fc1[0], w_fc2[0], b_qkv.reshape(1, -1), b_out, b_fc1, b_fc2, ln)
        dy_all, dpre_all, gmid_all, dqkv_all, gin_all, db1, db2, dbo, dbq, dln = bwd_call(
            stages, width, tile, dy_out.reshape(subs, rows, d_model), x_all, mid_all, s_all, qkv_all, w2t, w1t, wot, wqt_own, wqt_peer, ln)

        def flat(stack):
            return stack.reshape(subs * rows, -1)

        g_w_fc2, h_out = grad_call(flat(a_all), flat(dy_all), 1024, d_model, 1536, y_all)
        g_w_fc1, g_in = grad_call(flat(h2_all), flat(dpre_all), d_model, 1024, 1536, gin_all)
        g_w_out, = grad_call(flat(o_all), flat(gmid_all), half, d_model, 1536)
        g_w_qkv = lax.optimization_barrier(dot_tn(flat(dqkv_all), flat(h1_all)))
        g_w_out = g_w_out.reshape(heads, width, d_model)
        g_w_qkv = jnp.transpose(g_w_qkv.reshape(3, heads, width, d_model), (0, 3, 1, 2))
        g_b_qkv = dbq.reshape(3, heads, width)
        act = (1, micro, batch, rows, d_model)
        return (h_out.reshape(act), g_in.reshape(act), g_w_qkv[None], g_b_qkv[None], g_w_out[None], dbo,
                dln[None], g_w_fc1[None], db1, g_w_fc2[None], db2)

    act_spec = P(None, "dp", None, None)
    arg_specs = (act_spec, act_spec,
                 P("pp", None, None, "tp", None), P("pp", None, "tp", None), P("pp", "tp", None, None),
                 P("pp", None), P("pp", None, None), P("pp", None, "tp"), P("pp", "tp"),
                 P("pp", "tp", None), P("pp", None))
    stage_spec = P("pp", None, "dp", None, None)
    grad_axes = ("dp", "pp")
    result_specs = (stage_spec, stage_spec,
                    P(grad_axes, None, None, "tp", None), P(grad_axes, None, "tp", None), P(grad_axes, "tp", None, None),
                    P(grad_axes, None), P(grad_axes, None, None), P(grad_axes, None, "tp"), P(grad_axes, "tp"),
                    P(grad_axes, "tp", None), P(grad_axes, None))
    return jax.shard_map(stage_program, mesh=mesh, in_specs=arg_specs, out_specs=result_specs, check_vma=False)
```

```python
import functools

import jax
import jax.numpy as jnp
from jax import lax
from jax.experimental import pallas as pl
from jax.experimental.pallas import tpu as pltpu
from jax.sharding import PartitionSpec as P

LN_EPS = 1e-5
F32 = jnp.float32
BF16 = jnp.bfloat16
MESH = pl.DeviceIdType.MESH
NEG = -1e30
ROW_CHUNK = 32
GELU_C = 0.7978845608028654
GELU_K = 0.044715
LOG2_E = 1.4426950408889634
SOFT_ROWS = 64
RING = 4
LANES = 128
RELAYED = 2

WINDOWS = ((0, 128, 0), (0, 256, 96), (128, 256, 64), (256, 128, 32))


def starts(total, step):
    return range(0, total, step)


def parity(m):
    return lax.rem(m, 2)


def ring_slot(m):
    return lax.rem(m, RING)


def dot_nn(lhs, rhs):
    return lax.dot_general(lhs, rhs, (((1,), (0,)), ((), ())), preferred_element_type=F32)


def dot_nt(lhs, rhs):
    return lax.dot_general(lhs, rhs, (((1,), (1,)), ((), ())), preferred_element_type=F32)


def dot_tn(lhs, rhs):
    return lax.dot_general(lhs, rhs, (((0,), (0,)), ((), ())), preferred_element_type=F32)


def head_only(window, offset, width):
    lane = lax.broadcasted_iota(jnp.int32, window.shape, 1)
    return jnp.where((lane >= offset) & (lane < offset + width), window, jnp.zeros_like(window))


def join_heads(parts, width):
    lane = lax.broadcasted_iota(jnp.int32, (parts[0].shape[0], LANES), 1)
    first = jnp.where(lane < width, parts[0], parts[1][:, :LANES])
    second = jnp.where(lane < 2 * width - LANES, parts[1][:, LANES:], parts[2][:, :LANES])
    third = jnp.where(lane < 3 * width - 256, parts[2][:, LANES:], parts[3])
    return first, second, third


def norm_stats(x_wide):
    centered = x_wide - jnp.mean(x_wide, axis=-1, keepdims=True)
    inv_std = lax.rsqrt(jnp.mean(centered * centered, axis=-1, keepdims=True) + LN_EPS)
    return centered * inv_std, inv_std


def fold_rows(block):
    rows, cols = block.shape
    return jnp.sum(block.reshape(rows // 8, 8, cols), axis=0)


def neighbour_barrier(stage, tp_peer, stages):
    barrier = pltpu.get_barrier_semaphore()
    pl.semaphore_signal(barrier, inc=1, device_id={"tp": tp_peer}, device_id_type=MESH)
    for step in range(1, stages):
        pl.semaphore_signal(barrier, inc=1, device_id={"pp": lax.rem(stage + step, stages)}, device_id_type=MESH)
    pl.semaphore_wait(barrier, stages)


def fwd_kernel(subs, stages, width, tile,
               x_in, wqt_h, wo_h, w1_h, w2_h, bq, bo_h, b1_h, b2_h, ln_h,
               x_all, qkv_all, o_all, mid_all, h1_all, h2_all, s_all, a_all, y_all, part_all, wqt_p, wot_o, w1t_o, w2t_o, relay_in, relay_out,
               wq, wo, w1, w2, xr, h1b, qkvb, ob, midb, h2b, slb, ab, partb, peerb, yb, sb, pb, bqb, tb, par,
               w_sem, t_sem, wq_send, wq_recv, wo_send, wo_recv, bq_send, bq_recv, relay_send, relay_recv, in_sem, out_sem, mid_sem, y_sem, part_send, part_recv, y_send, x_recv, x_free):
    stage = lax.axis_index("pp")
    tp_me = lax.axis_index("tp")
    tp_peer = 1 - tp_me
    last_stage = stages - 1
    _, rows, d_model = xr.shape
    half = d_model // 2
    trio = 3 * half
    ff = slb.shape[1]
    scale = width ** -0.5
    log2_scale = scale * LOG2_E

    first = 0
    rows_of = []
    for row in (bo_h, b1_h, b2_h, *(ln_h.at[i:i + 1, :] for i in range(4))):
        lanes = slice(first, first + row.shape[1])
        par[:, lanes] = row[...].astype(F32)
        rows_of.append(par.at[:, lanes])
        first = lanes.stop
    bo, b1, b2, *ln = rows_of
    mine = pl.ds(pl.multiple_of(tp_me * half, LANES), half)
    piece = 256
    pieces = trio // piece
    peer_id = {"device_id": {"tp": tp_peer}, "device_id_type": MESH}
    loads = [pltpu.make_async_copy(src, dst, w_sem.at[i]) for i, (src, dst) in enumerate(((wo_h, wo.at[mine, :]), (w1_h, w1), (w2_h, w2)))]

    def cut(p):
        return pl.ds(pl.multiple_of(p * piece, piece), piece)

    def wq_copy(p):
        return pltpu.make_async_remote_copy(src_ref=wqt_h.at[cut(p), :], dst_ref=wqt_p.at[cut(p), :], send_sem=wq_send.at[p], recv_sem=wq_recv.at[p], **peer_id)

    wo_copy = pltpu.make_async_remote_copy(src_ref=wo_h, dst_ref=wo.at[mine, :], send_sem=wo_send, recv_sem=wo_recv, **peer_id)
    bq_copy = pltpu.make_async_remote_copy(src_ref=bq, dst_ref=bqb.at[tp_me], send_sem=bq_send, recv_sem=bq_recv, **peer_id)

    column = stages // 2
    direct = pieces - RELAYED

    def relay_copy(leg, r):
        src = (wqt_h.at[cut(direct + r), :], relay_in.at[r], relay_out.at[r])[leg]
        dst = (relay_in.at[r], relay_out.at[r], wqt_p.at[cut(direct + r), :])[leg]
        there = ({"pp": jnp.minimum(stage + column, last_stage)}, {"tp": tp_peer}, {"pp": jnp.maximum(stage - column, 0)})[leg]
        recv_sem = wq_recv.at[direct + r] if leg == 2 else relay_recv.at[leg, r]
        return pltpu.make_async_remote_copy(src_ref=src, dst_ref=dst, send_sem=relay_send.at[leg, r], recv_sem=recv_sem, device_id=there, device_id_type=MESH)

    def moved(src, dst):
        copy = pltpu.make_async_copy(src, dst, t_sem)
        copy.start()
        copy.wait()

    def turn(source, owner, p):
        moved(source.at[cut(p), :], h1b)
        wq[:, pl.ds(pl.multiple_of(owner * trio + p * piece, LANES), piece)] = jnp.transpose(h1b[...])

    def exchange_weights():
        def send(p, carry):
            wq_copy(p).start()
            return carry

        def own(p, carry):
            turn(wqt_h, tp_me, p)
            return carry

        def turn_w1(p, carry):
            h2b[...] = jnp.transpose(w1[:, cut(p)])
            moved(h2b, w1t_o.at[cut(p), :])
            return carry

        def turn_w2(p, carry):
            tb[...] = jnp.transpose(w2[cut(p), :])
            moved(tb, w2t_o.at[:, cut(p)])
            return carry

        def received(p, carry):
            wq_copy(p).wait_recv()
            turn(wqt_p, tp_peer, p)
            return carry

        bq_copy.start()
        for load in loads:
            load.start()
        lax.fori_loop(0, RELAYED, send, 0)

        @pl.when(stage < column)
        def _():
            for r in range(RELAYED):
                relay_copy(0, r).start()
            lax.fori_loop(RELAYED, direct, send, 0)

        @pl.when(stage >= column)
        def _():
            for r in range(RELAYED):
                relay_copy(0, r).wait_recv()
                relay_copy(1, r).start()
            lax.fori_loop(RELAYED, pieces, send, 0)

        wo_copy.start()
        bqb[tp_me] = bq[...]
        lax.fori_loop(0, pieces, own, 0)
        for load in loads:
            load.wait()
        lax.fori_loop(0, ff // piece, turn_w1, 0)
        lax.fori_loop(0, ff // piece, turn_w2, 0)

        @pl.when(stage >= column)
        def _():
            for r in range(RELAYED):
                relay_copy(1, r).wait_recv()
                relay_copy(2, r).start()

        bq_copy.wait_recv()
        middle = direct // 2
        for first, last in ((0, middle), (direct, pieces), (middle, direct)):
            lax.fori_loop(first, last, received, 0)

    pb[:, :, 0:LANES, LANES:rows] = jnp.zeros((2, 4, LANES, rows - LANES), BF16)
    neighbour_barrier(stage, tp_peer, stages)

    def outs(m):
        return (pltpu.make_async_copy(h1b, h1_all.at[m], out_sem.at[0]),
                pltpu.make_async_copy(qkvb, qkv_all.at[m], out_sem.at[1]),
                pltpu.make_async_copy(ob.at[:, pl.ds(pl.multiple_of(tp_me * half, LANES), half)], o_all.at[m], out_sem.at[2]),
                pltpu.make_async_copy(h2b, h2_all.at[m], out_sem.at[3]),
                pltpu.make_async_copy(slb, s_all.at[m], out_sem.at[4]),
                pltpu.make_async_copy(ab, a_all.at[m], out_sem.at[5]),
                pltpu.make_async_copy(xr.at[ring_slot(m)], x_all.at[m], out_sem.at[6]))

    def mid_out(m):
        slot = parity(m)
        return pltpu.make_async_copy(midb.at[slot], mid_all.at[m], mid_sem.at[slot])

    def y_out(m):
        slot = parity(m)
        return pltpu.make_async_copy(yb.at[slot], y_all.at[m], y_sem.at[slot])

    def part_copy(m):
        slot = parity(m)
        return pltpu.make_async_remote_copy(src_ref=partb.at[slot], dst_ref=peerb.at[ring_slot(m)], send_sem=part_send.at[slot], recv_sem=part_recv.at[m],
                                            device_id={"tp": tp_peer}, device_id_type=MESH)

    def part_out(m):
        slot = parity(m)
        return pltpu.make_async_copy(partb.at[slot], part_all.at[m], y_sem.at[slot])

    def next_copy(m):
        slot = parity(m)
        return pltpu.make_async_remote_copy(src_ref=yb.at[slot], dst_ref=xr.at[ring_slot(m)], send_sem=y_send.at[slot], recv_sem=x_recv.at[m],
                                            device_id={"pp": jnp.minimum(stage + 1, last_stage)}, device_id_type=MESH)

    def x_load(m):
        return pltpu.make_async_copy(x_in.at[m], xr.at[ring_slot(m)], in_sem.at[parity(m)])

    @pl.when(stage == 0)
    def _():
        x_load(0).start()

    def layer_norm(src, dst, gain, shift):
        for r in starts(rows, ROW_CHUNK):
            normed, _ = norm_stats(src[r:r + ROW_CHUNK, :].astype(F32))
            dst[r:r + ROW_CHUNK, :] = (normed * gain + shift).astype(BF16)

    def group_base(group):
        return (group // 2) * trio + (group % 2) * (4 * width)

    def attend():
        def scores(group):
            base = group_base(group)
            for j, (start, size, offset) in enumerate(WINDOWS):
                query = head_only(qkvb[:, base + start:base + start + size], offset, width)
                key = qkvb[:, base + half + start:base + half + start + size]
                sb[group % 2, j] = dot_nt(query, key)

        def softmax(group):
            for j in range(4):
                for r0 in starts(rows, SOFT_ROWS):
                    keys = LANES * (r0 // LANES + 1)
                    row = lax.broadcasted_iota(jnp.int32, (SOFT_ROWS, keys), 0) + r0
                    col = lax.broadcasted_iota(jnp.int32, (SOFT_ROWS, keys), 1)
                    score = jnp.where(row >= col, sb[group % 2, j, r0:r0 + SOFT_ROWS, 0:keys], NEG)
                    weight = jnp.exp2((score - jnp.max(score, axis=1, keepdims=True)) * log2_scale)
                    inv = 1.0 / jnp.sum(weight, axis=1, keepdims=True)
                    pb[group % 2, j, r0:r0 + SOFT_ROWS, 0:keys] = (weight * inv).astype(BF16)

        def values(group):
            base = group_base(group) + 2 * half
            parts = [dot_nn(pb[group % 2, j], qkvb[:, base + start:base + start + size]) for j, (start, size, _) in enumerate(WINDOWS)]
            for i, piece in enumerate(join_heads(parts, width)):
                first = group * (4 * width) + i * LANES
                ob[:, first:first + LANES] = piece.astype(BF16)

        groups = d_model // (4 * width)
        scores(0)
        for group in range(groups):
            if group + 1 < groups:
                scores(group + 1)
            softmax(group)
            values(group)

    def finish(m):
        slot = parity(m)
        peer_slot = ring_slot(m)
        part_copy(m).wait_recv()

        @pl.when(m >= 2)
        def _():
            y_out(m - 2).wait()
            next_copy(m - 2).wait_send()

        for r in starts(rows, ROW_CHUNK):
            both = partb[slot, r:r + ROW_CHUNK, :].astype(F32) + peerb[peer_slot, r:r + ROW_CHUNK, :].astype(F32)
            yb[slot, r:r + ROW_CHUNK, :] = (midb[slot, r:r + ROW_CHUNK, :].astype(F32) + both + b2[...]).astype(BF16)

        @pl.when(m >= RING)
        def _():
            pl.semaphore_wait(x_free, 1)

        next_copy(m).start()
        y_out(m).start()
        part_copy(m).wait_send()

    def attn_part(m):
        slot = parity(m)
        prev = jnp.maximum(m - 1, 0)
        h1_o, qkv_o, o_o, h2_o, _, _, x_o = outs(m)
        h1_p, qkv_p, o_p, h2_p, _, _, x_p = outs(prev)

        @pl.when(stage == 0)
        def _():
            x_load(m).wait()

            @pl.when(m + 1 < subs)
            def _():
                x_load(m + 1).start()

        @pl.when(stage > 0)
        def _():
            next_copy(m).wait_recv()

        x_o.start()
        xb = xr.at[ring_slot(m)]

        @pl.when(m > 0)
        def _():
            h1_p.wait()
            qkv_p.wait()
            o_p.wait()
            h2_p.wait()

        layer_norm(xb, h1b, ln[0][...], ln[1][...])
        h1_o.start()

        for n in starts(3 * d_model, tile):
            owner, lane = divmod(n, trio)
            qkvb[:, n:n + tile] = (dot_nn(h1b[...], wq[:, n:n + tile]) + bqb[owner, :, lane:lane + tile].astype(F32)).astype(BF16)
        qkv_o.start()
        attend()
        o_o.start()

        @pl.when(m == 0)
        def _():
            wo_copy.wait_recv()

        @pl.when(m >= 2)
        def _():
            mid_out(m - 2).wait()

        for n in starts(d_model, tile):
            midb[slot, :, n:n + tile] = (xb[:, n:n + tile].astype(F32) + dot_nn(ob[...], wo[:, n:n + tile]) + bo[:, n:n + tile]).astype(BF16)
        mid_out(m).start()
        x_o.wait()

        @pl.when((stage > 0) & (m < subs - RING))
        def _():
            pl.semaphore_signal(x_free, inc=1, device_id={"pp": jnp.maximum(stage - 1, 0)}, device_id_type=MESH)

        layer_norm(midb.at[slot], h2b, ln[2][...], ln[3][...])
        h2_o.start()

    def mlp_part(m):
        slot = parity(m)
        _, _, _, _, s_o, a_o, _ = outs(m)
        _, _, _, _, s_p, a_p, _ = outs(jnp.maximum(m - 1, 0))

        @pl.when(m > 0)
        def _():
            s_p.wait()
            a_p.wait()

        for n in starts(ff, tile):
            pre = dot_nn(h2b[...], w1[:, n:n + tile]) + b1[:, n:n + tile]
            square = pre * pre
            bend = jnp.tanh(pre * (GELU_C + (GELU_C * GELU_K) * square))
            cdf = 0.5 + 0.5 * bend
            ab[:, n:n + tile] = (pre * cdf).astype(BF16)
            slb[:, n:n + tile] = cdf + (0.5 * pre) * (1.0 - bend * bend) * (GELU_C + (3.0 * GELU_C * GELU_K) * square)
        s_o.start()
        a_o.start()

        @pl.when((stage == last_stage) & (m >= 2))
        def _():
            part_out(m - 2).wait()

        for n in starts(d_model, tile):
            partb[slot, :, n:n + tile] = dot_nn(ab[...], w2[:, n:n + tile]).astype(BF16)

        @pl.when(stage < last_stage)
        def _():
            part_copy(m).start()

        @pl.when(stage == last_stage)
        def _():
            part_out(m).start()

    def step(m, carry):
        @pl.when(m < subs)
        def _():
            attn_part(m)
            mlp_part(m)

        @pl.when((m >= 1) & (m <= d_model // piece))
        def _():
            tb[...] = jnp.transpose(wo[cut(m - 1), :])
            moved(tb, wot_o.at[:, cut(m - 1)])

        @pl.when((m > 0) & (stage < last_stage))
        def _():
            finish(m - 1)

        return carry

    exchange_weights()
    lax.fori_loop(0, subs + 1, step, 0)

    def sent(p, carry):
        wq_copy(p).wait_send()
        return carry

    lax.fori_loop(0, direct, sent, 0)

    @pl.when(stage < column)
    def _():
        for r in range(RELAYED):
            relay_copy(0, r).wait_send()

    @pl.when(stage >= column)
    def _():
        lax.fori_loop(direct, pieces, sent, 0)
        for r in range(RELAYED):
            relay_copy(1, r).wait_send()
            relay_copy(2, r).wait_send()

    wo_copy.wait_send()
    bq_copy.wait_send()
    h1_o, qkv_o, o_o, h2_o, s_o, a_o, x_o = outs(subs - 1)
    for copy in (h1_o, qkv_o, o_o, h2_o, s_o, a_o):
        copy.wait()

    for m in (subs - 2, subs - 1):
        mid_out(m).wait()

        @pl.when(stage < last_stage)
        def _():
            y_out(m).wait()
            next_copy(m).wait_send()

        @pl.when(stage == last_stage)
        def _():
            part_out(m).wait()


def bwd_kernel(subs, stages, width, tile,
               dy_in, x_all, mid_all, s_all, qkv_all, w2t_h, w1t_h, wot_h, wqt_h, wqt_p, ln_h,
               dy_all, dpre_all, gmid_all, dqkv_all, gin_all, db1_o, db2_o, dbo_o, dbq_o, dln_o,
               w2t, w1t, wot, wqt, dyb, slb, dpb, partb, peerb, rb, midb, xb, gmb, qkvb, gib, sb, db, pb, dsb, db1, db2, dbo, dbq, dln, ln,
               w_sem, in_sem, pre_sem, out_sem, dy_sem, gi_sem, part_send, part_recv, gi_send, dy_recv, dy_free):
    stage = lax.axis_index("pp")
    tp_me = lax.axis_index("tp")
    tp_peer = 1 - tp_me
    last_stage = stages - 1
    rows, d_model = xb.shape
    half = d_model // 2
    trio = 3 * half
    ff = slb.shape[1]
    scale = width ** -0.5
    log2_scale = scale * LOG2_E

    ln[...] = ln_h[...].astype(F32)
    mine_q = pl.ds(pl.multiple_of(tp_me * trio, LANES), trio)
    theirs_q = pl.ds(pl.multiple_of(tp_peer * trio, LANES), trio)
    loads = [pltpu.make_async_copy(src, dst, w_sem.at[i]) for i, (src, dst) in enumerate((
        (w2t_h, w2t), (w1t_h, w1t), (wot_h, wot), (wqt_h, wqt.at[mine_q, :]), (wqt_p, wqt.at[theirs_q, :])))]

    def fetch(m):
        return (pltpu.make_async_copy(s_all.at[m], slb, pre_sem.at[0]),
                pltpu.make_async_copy(mid_all.at[m], midb, pre_sem.at[1]),
                pltpu.make_async_copy(qkv_all.at[m], qkvb, pre_sem.at[2]),
                pltpu.make_async_copy(x_all.at[m], xb, pre_sem.at[3]))

    fetch(0)[0].start()
    for load in loads[:2]:
        load.start()
    for copy in fetch(0)[1:]:
        copy.start()
    for acc in (db1, db2, dbo, dbq, dln):
        acc[...] = jnp.zeros_like(acc)
    for acc in (pb, dsb):
        acc[:, LANES:rows, 0:LANES] = jnp.zeros((4, rows - LANES, LANES), BF16)
    neighbour_barrier(stage, tp_peer, stages)

    def outs(m):
        return (pltpu.make_async_copy(dpb, dpre_all.at[m], out_sem.at[0]),
                pltpu.make_async_copy(gmb, gmid_all.at[m], out_sem.at[1]),
                pltpu.make_async_copy(qkvb.at[:, pl.ds(pl.multiple_of(tp_me * trio, LANES), trio)], dqkv_all.at[m], out_sem.at[2]))

    def dy_load(m):
        return pltpu.make_async_copy(dy_in.at[m], dyb.at[ring_slot(m)], in_sem.at[parity(m)])

    def dy_out(m):
        return pltpu.make_async_copy(dyb.at[ring_slot(m)], dy_all.at[m], dy_sem.at[parity(m)])

    def gi_out(m):
        slot = parity(m)
        return pltpu.make_async_copy(gib.at[slot], gin_all.at[m], gi_sem.at[slot])

    def part_copy(m):
        slot = parity(m)
        return pltpu.make_async_remote_copy(src_ref=partb.at[slot], dst_ref=peerb.at[ring_slot(m)], send_sem=part_send.at[slot], recv_sem=part_recv.at[m],
                                            device_id={"tp": tp_peer}, device_id_type=MESH)

    def prev_copy(m):
        slot = parity(m)
        return pltpu.make_async_remote_copy(src_ref=gib.at[slot], dst_ref=dyb.at[ring_slot(m)], send_sem=gi_send.at[slot], recv_sem=dy_recv.at[m],
                                            device_id={"pp": jnp.maximum(stage - 1, 0)}, device_id_type=MESH)

    @pl.when(stage == last_stage)
    def _():
        dy_load(0).start()

    def norm_grad(x_rows, grad, gain, which):
        normed, inv_std = norm_stats(x_rows)
        dln[which] += fold_rows(grad * normed)
        dln[which + 1] += fold_rows(grad)
        scaled = grad * gain
        mean_scaled = jnp.mean(scaled, axis=-1, keepdims=True)
        mean_proj = jnp.mean(scaled * normed, axis=-1, keepdims=True)
        return inv_std * (scaled - mean_scaled - normed * mean_proj)

    def mlp_part(m):
        slot = parity(m)
        slope_f = fetch(m)[0]

        dy_slot = ring_slot(m)

        @pl.when(stage == last_stage)
        def _():
            dy_load(m).wait()

            @pl.when(m + 1 < subs)
            def _():
                dy_load(m + 1).start()

        @pl.when(stage < last_stage)
        def _():
            prev_copy(m).wait_recv()

        dy_out(m).start()

        @pl.when(m == 0)
        def _():
            loads[0].wait()
            for load in loads[2:]:
                load.start()

        @pl.when(m > 0)
        def _():
            outs(m - 1)[0].wait()

        slope_f.wait()
        for n in starts(ff, tile):
            grad = dot_nn(dyb[dy_slot], w2t[:, n:n + tile]).astype(BF16).astype(F32) * slb[:, n:n + tile]
            db1[:, n:n + tile] += fold_rows(grad)
            dpb[:, n:n + tile] = grad.astype(BF16)
        outs(m)[0].start()

        @pl.when(m + 1 < subs)
        def _():
            fetch(m + 1)[0].start()

        @pl.when(m == 0)
        def _():
            loads[1].wait()

        for n in starts(d_model, tile):
            partb[slot, :, n:n + tile] = dot_nn(dpb[...], w1t[:, n:n + tile]).astype(BF16)
        part_copy(m).start()

    def attend_grad():
        def window(base, spec):
            start, size, offset = spec
            return slice(base + start, base + start + size), offset

        def scores(group, base):
            for j, spec in enumerate(WINDOWS):
                q_lanes, offset = window(base, spec)
                k_lanes, _ = window(base + half, spec)
                v_lanes, _ = window(base + 2 * half, spec)
                d_lanes, _ = window(group * (4 * width), spec)
                sb[j] = dot_nt(qkvb[:, k_lanes], head_only(qkvb[:, q_lanes], offset, width))
                db[j] = dot_nt(qkvb[:, v_lanes], head_only(rb[:, d_lanes], offset, width))

        def softmax():
            for j in range(4):
                for q0 in starts(rows, LANES):
                    keys, lanes = q0 + LANES, slice(q0, q0 + LANES)
                    krow = lax.broadcasted_iota(jnp.int32, (keys, LANES), 0)
                    qcol = lax.broadcasted_iota(jnp.int32, (keys, LANES), 1) + q0
                    score = jnp.where(qcol >= krow, sb[j, 0:keys, lanes], NEG)
                    weight = jnp.exp2((score - jnp.max(score, axis=0, keepdims=True)) * log2_scale)
                    prob = weight * (1.0 / jnp.sum(weight, axis=0, keepdims=True))
                    pb[j, 0:keys, lanes] = prob.astype(BF16)
                    d_prob = db[j, 0:keys, lanes]
                    d_score = prob * (d_prob - jnp.sum(prob * d_prob, axis=0, keepdims=True))
                    dsb[j, 0:keys, lanes] = d_score.astype(BF16)

        def products(group, base):
            d_query, d_key, d_value = [], [], []
            for j, spec in enumerate(WINDOWS):
                q_lanes, _ = window(base, spec)
                k_lanes, _ = window(base + half, spec)
                d_lanes, _ = window(group * (4 * width), spec)
                d_value.append(dot_nn(pb[j], rb[:, d_lanes]))
                d_key.append(dot_nn(dsb[j], qkvb[:, q_lanes]) * scale)
                d_query.append(dot_tn(dsb[j], qkvb[:, k_lanes]) * scale)
            for c, parts in enumerate((d_query, d_key, d_value)):
                for i, piece in enumerate(join_heads(parts, width)):
                    piece = piece.astype(BF16)
                    first = base + c * half + i * LANES
                    qkvb[:, first:first + LANES] = piece
                    dbq[:, first:first + LANES] += fold_rows(piece.astype(F32))

        for group in range(d_model // (4 * width)):
            base = (group // 2) * trio + (group % 2) * (4 * width)
            scores(group, base)
            softmax()
            products(group, base)

    def attn_part(m):
        slot = parity(m)
        _, mid_f, qkv_f, x_f = fetch(m)
        _, gm_o, dq_o = outs(m)
        peer_slot = ring_slot(m)
        dy_slot = ring_slot(m)
        mid_f.wait()

        @pl.when(m > 0)
        def _():
            outs(m - 1)[1].wait()

        @pl.when(m == 0)
        def _():
            for load in loads[2:]:
                load.wait()

        part_copy(m).wait_recv()
        for r in starts(rows, ROW_CHUNK):
            rr = slice(r, r + ROW_CHUNK)
            grad = (partb[slot, rr, :].astype(F32) + peerb[peer_slot, rr, :].astype(F32)).astype(BF16).astype(F32)
            d_y = dyb[dy_slot, rr, :].astype(F32)
            db2[...] += fold_rows(d_y)
            total = d_y + norm_grad(midb[rr, :].astype(F32), grad, ln[2:3, :], 2)
            gmb[rr, :] = total.astype(BF16)
            dbo[...] += fold_rows(total)
        gm_o.start()
        dy_out(m).wait()

        @pl.when((stage < last_stage) & (m < subs - RING))
        def _():
            pl.semaphore_signal(dy_free, inc=1, device_id={"pp": jnp.minimum(stage + 1, last_stage)}, device_id_type=MESH)

        @pl.when(m + 1 < subs)
        def _():
            fetch(m + 1)[1].start()

        for n in starts(d_model, tile):
            rb[:, n:n + tile] = dot_nn(gmb[...], wot[:, n:n + tile]).astype(BF16)
        qkv_f.wait()
        attend_grad()
        dq_o.start()
        part_copy(m).wait_send()
        for n in starts(d_model, tile):
            rb[:, n:n + tile] = dot_nn(qkvb[...], wqt[:, n:n + tile]).astype(BF16)
        x_f.wait()

        @pl.when(m >= 2)
        def _():
            gi_out(m - 2).wait()

            @pl.when(stage > 0)
            def _():
                prev_copy(m - 2).wait_send()

        for r in starts(rows, ROW_CHUNK):
            rr = slice(r, r + ROW_CHUNK)
            total = gmb[rr, :].astype(F32) + norm_grad(xb[rr, :].astype(F32), rb[rr, :].astype(F32), ln[0:1, :], 0)
            gib[slot, rr, :] = total.astype(BF16)

        @pl.when(stage > 0)
        def _():
            @pl.when(m >= RING)
            def _():
                pl.semaphore_wait(dy_free, 1)

            prev_copy(m).start()

        gi_out(m).start()
        dq_o.wait()

        @pl.when(m + 1 < subs)
        def _():
            fetch(m + 1)[2].start()
            fetch(m + 1)[3].start()

    def step(m, carry):
        @pl.when(m < subs)
        def _():
            mlp_part(m)

        @pl.when(m > 0)
        def _():
            attn_part(m - 1)

        return carry

    lax.fori_loop(0, subs + 1, step, 0)
    for acc, out in ((db1, db1_o), (db2, db2_o), (dbo, dbo_o)):
        out[...] = jnp.sum(acc[...], axis=0, keepdims=True)
    dbq_o[...] = jnp.sum(dbq[:, mine_q], axis=0, keepdims=True)
    dln_o[...] = jnp.sum(dln[...], axis=1)
    for copy in outs(subs - 1)[:2]:
        copy.wait()
    for m in (subs - 2, subs - 1):
        gi_out(m).wait()

        @pl.when(stage > 0)
        def _():
            prev_copy(m).wait_send()


ANY = pl.BlockSpec(memory_space=pl.ANY)
VMEM = pl.BlockSpec(memory_space=pltpu.VMEM)
DMA = pltpu.SemaphoreType.DMA
VMEM_LIMIT = 67043328


def fwd_call(stages, width, tile, x_in, wqt_own, wo_own, w1, w2, bq, bo, b1, b2, ln):
    subs, rows, d_model = x_in.shape
    ff = w1.shape[1]
    half = d_model // 2
    trio = 3 * half

    def hbm(cols, dtype=BF16):
        return jax.ShapeDtypeStruct((subs, rows, cols), dtype)

    def buf(cols, dtype=BF16):
        return pltpu.VMEM((rows, cols), dtype)

    def two(cols):
        return pltpu.VMEM((2, rows, cols), BF16)

    weights = 2 * (4 * d_model * d_model + 2 * d_model * ff)
    return pl.pallas_call(
        functools.partial(fwd_kernel, subs, stages, width, tile),
        name="fwd_stage",
        out_shape=(hbm(d_model), hbm(3 * d_model), hbm(half), hbm(d_model), hbm(d_model), hbm(d_model), hbm(ff, F32), hbm(ff), hbm(d_model), hbm(d_model),
                   jax.ShapeDtypeStruct((trio, d_model), BF16), jax.ShapeDtypeStruct((d_model, d_model), BF16), jax.ShapeDtypeStruct((ff, d_model), BF16), jax.ShapeDtypeStruct((d_model, ff), BF16),
                   *[jax.ShapeDtypeStruct((RELAYED, rows, d_model), BF16)] * 2),
        in_specs=[ANY] * 5 + [VMEM] * 5,
        out_specs=[ANY] * 16,
        scratch_shapes=[
            pltpu.VMEM((d_model, 3 * d_model), BF16), pltpu.VMEM((d_model, d_model), BF16), pltpu.VMEM(w1.shape, BF16), pltpu.VMEM(w2.shape, BF16),
            pltpu.VMEM((RING, rows, d_model), BF16), buf(d_model), buf(3 * d_model), buf(d_model), two(d_model), buf(d_model), buf(ff, F32), buf(ff), two(d_model), pltpu.VMEM((RING, rows, d_model), BF16), two(d_model),
            pltpu.VMEM((2, 4, rows, rows), F32), pltpu.VMEM((2, 4, rows, rows), BF16), pltpu.VMEM((2, 1, trio), BF16), pltpu.VMEM((d_model, 256), BF16), pltpu.VMEM((1, ff + 6 * d_model), F32),
            DMA((3,)), DMA, DMA((trio // 256,)), DMA((trio // 256,)), DMA, DMA, DMA, DMA, DMA((3, RELAYED)), DMA((2, RELAYED)), DMA((2,)), DMA((7,)), DMA((2,)), DMA((2,)), DMA((2,)), DMA((subs,)), DMA((2,)), DMA((subs,)), pltpu.SemaphoreType.REGULAR,
        ],
        cost_estimate=pl.CostEstimate(flops=subs * rows * weights, bytes_accessed=weights + subs * rows * d_model * 30, transcendentals=subs * rows * (ff + rows * 16)),
        compiler_params=pltpu.CompilerParams(collective_id=0, has_side_effects=True, vmem_limit_bytes=VMEM_LIMIT),
    )(x_in, wqt_own, wo_own, w1, w2, bq, bo, b1, b2, ln)


def bwd_call(stages, width, tile, dy_in, x_all, mid_all, s_all, qkv_all, w2t, w1t, wot, wqt_own, wqt_peer, ln):
    subs, rows, d_model = dy_in.shape
    ff = s_all.shape[2]
    half = d_model // 2
    trio = 3 * half

    def hbm(cols, dtype=BF16):
        return jax.ShapeDtypeStruct((subs, rows, cols), dtype)

    def buf(cols, dtype=BF16):
        return pltpu.VMEM((rows, cols), dtype)

    def two(cols):
        return pltpu.VMEM((2, rows, cols), BF16)

    ring = pltpu.VMEM((RING, rows, d_model), BF16)

    def acc(*shape):
        return jax.ShapeDtypeStruct(shape, F32)

    weights = 2 * (4 * d_model * d_model + 2 * d_model * ff)
    return pl.pallas_call(
        functools.partial(bwd_kernel, subs, stages, width, tile),
        name="bwd_stage",
        out_shape=(hbm(d_model), hbm(ff), hbm(d_model), hbm(trio), hbm(d_model),
                   acc(1, ff), acc(1, d_model), acc(1, d_model), acc(1, trio), acc(4, d_model)),
        in_specs=[ANY] * 10 + [VMEM],
        out_specs=[ANY] * 5 + [VMEM] * 5,
        scratch_shapes=[
            pltpu.VMEM(w2t.shape, BF16), pltpu.VMEM(w1t.shape, BF16), pltpu.VMEM((d_model, d_model), BF16), pltpu.VMEM((3 * d_model, d_model), BF16),
            ring, buf(ff, F32), buf(ff), two(d_model), ring, buf(d_model), buf(d_model), buf(d_model), buf(d_model), buf(3 * d_model), two(d_model),
            pltpu.VMEM((4, rows, rows), F32), pltpu.VMEM((4, rows, rows), F32), pltpu.VMEM((4, rows, rows), BF16), pltpu.VMEM((4, rows, rows), BF16),
            pltpu.VMEM((8, ff), F32), pltpu.VMEM((8, d_model), F32), pltpu.VMEM((8, d_model), F32), pltpu.VMEM((8, 3 * d_model), F32), pltpu.VMEM((4, 8, d_model), F32), pltpu.VMEM((4, d_model), F32),
            DMA((5,)), DMA((2,)), DMA((4,)), DMA((3,)), DMA((2,)), DMA((2,)), DMA((2,)), DMA((subs,)), DMA((2,)), DMA((subs,)), pltpu.SemaphoreType.REGULAR,
        ],
        cost_estimate=pl.CostEstimate(flops=subs * rows * weights, bytes_accessed=weights + subs * rows * d_model * 30, transcendentals=subs * rows * (ff + rows * 16)),
        compiler_params=pltpu.CompilerParams(collective_id=1, has_side_effects=True, vmem_limit_bytes=VMEM_LIMIT),
    )(dy_in, x_all, mid_all, s_all, qkv_all, w2t, w1t, wot, wqt_own, wqt_peer, ln)


def grad_kernel(last_stage, extra_count, stage, left, right, *refs):
    extras, out, passed = refs[:extra_count], refs[extra_count], refs[extra_count + 1:]
    if len(extras) == len(passed):
        for src, dst in zip(extras, passed):
            dst[...] = src[...]
    else:
        y, mid, own, peer, b2 = extras

        @pl.when(stage[0] < last_stage)
        def _():
            passed[0][...] = y[...]

        @pl.when(stage[0] == last_stage)
        def _():
            both = own[...].astype(F32) + peer[...].astype(F32)
            passed[0][...] = (mid[...].astype(F32) + both + b2[...].astype(F32)).astype(BF16)

    @pl.when(pl.program_id(1) == 0)
    def _():
        out[...] = jnp.zeros_like(out)

    n_tile = 512
    for n in starts(out.shape[1], n_tile):
        out[:, n:n + n_tile] += dot_tn(left[...], right[:, n:n + n_tile])


def grad_call(stage, last_stage, left, right, m_block, n_block, k_block, extras=(), passed=0):
    tokens, m_size = left.shape
    n_size = right.shape[1]
    m_count = m_size // m_block
    grid = (m_count * (n_size // n_block), tokens // k_block)
    steps = grid[0] * grid[1]

    def spec(array, used=lambda s: 1):
        if array.ndim == 2:
            return pl.BlockSpec(array.shape, lambda i, k, s: (0, 0))
        block = (array.shape[0] // steps,) + array.shape[1:]
        return pl.BlockSpec(block, lambda i, k, s: ((i * grid[1] + k) * used(s), 0, 0))

    in_specs = [pl.BlockSpec((k_block, m_block), lambda i, k, s: (k, i % m_count)), pl.BlockSpec((k_block, n_block), lambda i, k, s: (k, i // m_count))]
    if len(extras) > passed:
        in_specs += [spec(extras[0], lambda s: 1 - s[0] // last_stage)] + [spec(array, lambda s: s[0] // last_stage) for array in extras[1:]]
    else:
        in_specs += [spec(array) for array in extras]
    moved = 2 * tokens * (m_size * (n_size // n_block) + n_size * m_count) + 4 * m_size * n_size
    return pl.pallas_call(
        functools.partial(grad_kernel, last_stage, len(extras)),
        name="weight_grad",
        grid_spec=pltpu.PrefetchScalarGridSpec(
            num_scalar_prefetch=1, grid=grid, in_specs=in_specs,
            out_specs=[pl.BlockSpec((m_block, n_block), lambda i, k, s: (i % m_count, i // m_count))] + [spec(array) for array in extras[:passed]]),
        out_shape=[jax.ShapeDtypeStruct((m_size, n_size), F32)] + [jax.ShapeDtypeStruct(array.shape, array.dtype) for array in extras[:passed]],
        cost_estimate=pl.CostEstimate(flops=2 * tokens * m_size * n_size, bytes_accessed=moved, transcendentals=0),
        compiler_params=pltpu.CompilerParams(dimension_semantics=("arbitrary", "arbitrary"), vmem_limit_bytes=VMEM_LIMIT),
    )(stage, left, right, *extras)


def solution(mesh):
    stages = mesh.shape["pp"]

    def stage_program(x_in, dy_out, w_qkv, b_qkv, w_out, b_out, ln_par, w_fc1, b_fc1, w_fc2, b_fc2):
        micro, batch, rows, d_model = x_in.shape
        heads, width = w_qkv.shape[3:]
        half = heads * width
        subs = micro * batch
        tile = half

        wqt_own = jnp.transpose(w_qkv[0], (0, 2, 3, 1)).reshape(3 * half, d_model)
        ln = ln_par[0]
        x_all, qkv_all, o_all, mid_all, h1_all, h2_all, s_all, a_all, y_all, part_all, wqt_peer, wot, w1t, w2t, _, _ = fwd_call(
            stages, width, tile, x_in.reshape(subs, rows, d_model), wqt_own, w_out[0].reshape(half, d_model), w_fc1[0], w_fc2[0], b_qkv.reshape(1, -1), b_out, b_fc1, b_fc2, ln)
        dy_all, dpre_all, gmid_all, dqkv_all, gin_all, db1, db2, dbo, dbq, dln = bwd_call(
            stages, width, tile, dy_out.reshape(subs, rows, d_model), x_all, mid_all, s_all, qkv_all, w2t, w1t, wot, wqt_own, wqt_peer, ln)

        def flat(stack):
            return stack.reshape(subs * rows, -1)

        last_stage = stages - 1
        stage = lax.axis_index("pp").reshape(1)
        held, _ = lax.optimization_barrier((part_all, gin_all))
        peer_part = lax.ppermute(held, ("tp", "pp"), [(last_stage, stages + last_stage), (stages + last_stage, last_stage)])
        g_w_out, dbo, dln, db1, db2 = grad_call(stage, last_stage, flat(o_all), flat(gmid_all), half, d_model, d_model, (dbo, dln, db1, db2), 4)
        g_w_fc1, g_in = grad_call(stage, last_stage, flat(h2_all), flat(dpre_all), d_model, 1024, d_model, (gin_all,), 1)
        g_w_fc2, h_out = grad_call(stage, last_stage, flat(a_all), flat(dy_all), 1024, d_model, d_model, (y_all, mid_all, part_all, peer_part, b_fc2), 1)
        g_w_qkv = lax.optimization_barrier(dot_tn(flat(dqkv_all), flat(h1_all)))
        g_w_out = g_w_out.reshape(heads, width, d_model)
        g_w_qkv = jnp.transpose(g_w_qkv.reshape(3, heads, width, d_model), (0, 3, 1, 2))
        g_b_qkv = dbq.reshape(3, heads, width)
        act = (1, micro, batch, rows, d_model)
        return (h_out.reshape(act), g_in.reshape(act), g_w_qkv[None], g_b_qkv[None], g_w_out[None], dbo,
                dln[None], g_w_fc1[None], db1, g_w_fc2[None], db2)

    act_spec = P(None, "dp", None, None)
    arg_specs = (act_spec, act_spec,
                 P("pp", None, None, "tp", None), P("pp", None, "tp", None), P("pp", "tp", None, None),
                 P("pp", None), P("pp", None, None), P("pp", None, "tp"), P("pp", "tp"),
                 P("pp", "tp", None), P("pp", None))
    stage_spec = P("pp", None, "dp", None, None)
    grad_axes = ("dp", "pp")
    result_specs = (stage_spec, stage_spec,
                    P(grad_axes, None, None, "tp", None), P(grad_axes, None, "tp", None), P(grad_axes, "tp", None, None),
                    P(grad_axes, None), P(grad_axes, None, None), P(grad_axes, None, "tp"), P(grad_axes, "tp"),
                    P(grad_axes, "tp", None), P(grad_axes, None))
    return jax.shard_map(stage_program, mesh=mesh, in_specs=arg_specs, out_specs=result_specs, check_vma=False)
```

```python
import functools

import jax
import jax.numpy as jnp
from jax import lax
from jax.experimental import pallas as pl
from jax.experimental.pallas import tpu as pltpu
from jax.sharding import PartitionSpec as P

LN_EPS = 1e-5
F32 = jnp.float32
BF16 = jnp.bfloat16
MESH = pl.DeviceIdType.MESH
NEG = -1e30
ROW_CHUNK = 32
GELU_C = 0.7978845608028654
GELU_K = 0.044715
LOG2_E = 1.4426950408889634
SOFT_ROWS = 64
RING = 4
LANES = 128
RELAYED = 3

WINDOWS = ((0, 128, 0), (0, 256, 96), (128, 256, 64), (256, 128, 32))


def starts(total, step):
    return range(0, total, step)


def parity(m):
    return lax.rem(m, 2)


def ring_slot(m):
    return lax.rem(m, RING)


def dot_nn(lhs, rhs):
    return lax.dot_general(lhs, rhs, (((1,), (0,)), ((), ())), preferred_element_type=F32)


def dot_nt(lhs, rhs):
    return lax.dot_general(lhs, rhs, (((1,), (1,)), ((), ())), preferred_element_type=F32)


def dot_tn(lhs, rhs):
    return lax.dot_general(lhs, rhs, (((0,), (0,)), ((), ())), preferred_element_type=F32)


def head_only(window, offset, width):
    lane = lax.broadcasted_iota(jnp.int32, window.shape, 1)
    return jnp.where((lane >= offset) & (lane < offset + width), window, jnp.zeros_like(window))


def join_heads(parts, width):
    lane = lax.broadcasted_iota(jnp.int32, (parts[0].shape[0], LANES), 1)
    first = jnp.where(lane < width, parts[0], parts[1][:, :LANES])
    second = jnp.where(lane < 2 * width - LANES, parts[1][:, LANES:], parts[2][:, :LANES])
    third = jnp.where(lane < 3 * width - 256, parts[2][:, LANES:], parts[3])
    return first, second, third


def norm_stats(x_wide):
    centered = x_wide - jnp.mean(x_wide, axis=-1, keepdims=True)
    inv_std = lax.rsqrt(jnp.mean(centered * centered, axis=-1, keepdims=True) + LN_EPS)
    return centered * inv_std, inv_std


def fold_rows(block):
    rows, cols = block.shape
    return jnp.sum(block.reshape(rows // 8, 8, cols), axis=0)


def neighbour_barrier(stage, tp_peer, stages):
    barrier = pltpu.get_barrier_semaphore()
    pl.semaphore_signal(barrier, inc=1, device_id={"tp": tp_peer}, device_id_type=MESH)
    for step in range(1, stages):
        pl.semaphore_signal(barrier, inc=1, device_id={"pp": lax.rem(stage + step, stages)}, device_id_type=MESH)
    pl.semaphore_wait(barrier, stages)


def fwd_kernel(subs, stages, width, tile,
               x_in, wqt_h, wo_h, w1_h, w2_h, bq, bo_h, b1_h, b2_h, ln_h,
               x_all, qkv_all, o_all, mid_all, h1_all, h2_all, s_all, a_all, y_all, part_all, wqt_p, wot_o, w1t_o, w2t_o, relay_in, relay_out,
               wq, wo, w1, w2, xr, h1b, qkvb, ob, midb, h2b, slb, ab, partb, peerb, yb, sb, pb, bqb, tb, par,
               w_sem, t_sem, wq_send, wq_recv, wo_send, wo_recv, bq_send, bq_recv, relay_send, relay_recv, in_sem, out_sem, mid_sem, y_sem, part_send, part_recv, y_send, x_recv, x_free):
    stage = lax.axis_index("pp")
    tp_me = lax.axis_index("tp")
    tp_peer = 1 - tp_me
    last_stage = stages - 1
    _, rows, d_model = xr.shape
    half = d_model // 2
    trio = 3 * half
    ff = slb.shape[1]
    scale = width ** -0.5
    log2_scale = scale * LOG2_E

    first = 0
    rows_of = []
    for row in (bo_h, b1_h, b2_h, *(ln_h.at[i:i + 1, :] for i in range(4))):
        lanes = slice(first, first + row.shape[1])
        par[:, lanes] = row[...].astype(F32)
        rows_of.append(par.at[:, lanes])
        first = lanes.stop
    bo, b1, b2, *ln = rows_of
    mine = pl.ds(pl.multiple_of(tp_me * half, LANES), half)
    piece = 256
    pieces = trio // piece
    peer_id = {"device_id": {"tp": tp_peer}, "device_id_type": MESH}
    loads = [pltpu.make_async_copy(src, dst, w_sem.at[i]) for i, (src, dst) in enumerate(((wo_h, wo.at[mine, :]), (w1_h, w1), (w2_h, w2)))]

    def cut(p):
        return pl.ds(pl.multiple_of(p * piece, piece), piece)

    def wq_copy(p):
        return pltpu.make_async_remote_copy(src_ref=wqt_h.at[cut(p), :], dst_ref=wqt_p.at[cut(p), :], send_sem=wq_send.at[p], recv_sem=wq_recv.at[p], **peer_id)

    wo_copy = pltpu.make_async_remote_copy(src_ref=wo_h, dst_ref=wo.at[mine, :], send_sem=wo_send, recv_sem=wo_recv, **peer_id)
    bq_copy = pltpu.make_async_remote_copy(src_ref=bq, dst_ref=bqb.at[tp_me], send_sem=bq_send, recv_sem=bq_recv, **peer_id)

    column = stages // 2
    direct = pieces - RELAYED

    def relay_copy(leg, r):
        src = (wqt_h.at[cut(direct + r), :], relay_in.at[r], relay_out.at[r])[leg]
        dst = (relay_in.at[r], relay_out.at[r], wqt_p.at[cut(direct + r), :])[leg]
        there = ({"pp": jnp.minimum(stage + column, last_stage)}, {"tp": tp_peer}, {"pp": jnp.maximum(stage - column, 0)})[leg]
        recv_sem = wq_recv.at[direct + r] if leg == 2 else relay_recv.at[leg, r]
        return pltpu.make_async_remote_copy(src_ref=src, dst_ref=dst, send_sem=relay_send.at[leg, r], recv_sem=recv_sem, device_id=there, device_id_type=MESH)

    def moved(src, dst):
        copy = pltpu.make_async_copy(src, dst, t_sem)
        copy.start()
        copy.wait()

    def turn(source, owner, p):
        moved(source.at[cut(p), :], h1b)
        wq[:, pl.ds(pl.multiple_of(owner * trio + p * piece, LANES), piece)] = jnp.transpose(h1b[...])

    def exchange_weights():
        def send(p, carry):
            wq_copy(p).start()
            return carry

        def own(p, carry):
            turn(wqt_h, tp_me, p)
            return carry

        def turn_w1(p, carry):
            h2b[...] = jnp.transpose(w1[:, cut(p)])
            moved(h2b, w1t_o.at[cut(p), :])
            return carry

        def turn_w2(p, carry):
            tb[...] = jnp.transpose(w2[cut(p), :])
            moved(tb, w2t_o.at[:, cut(p)])
            return carry

        def received(p, carry):
            wq_copy(p).wait_recv()
            turn(wqt_p, tp_peer, p)
            return carry

        bq_copy.start()
        for load in loads:
            load.start()
        lax.fori_loop(0, RELAYED, send, 0)

        @pl.when(stage < column)
        def _():
            for r in range(RELAYED):
                relay_copy(0, r).start()
            lax.fori_loop(RELAYED, direct, send, 0)

        @pl.when(stage >= column)
        def _():
            for r in range(RELAYED):
                relay_copy(0, r).wait_recv()
                relay_copy(1, r).start()
            lax.fori_loop(RELAYED, pieces, send, 0)

        wo_copy.start()
        bqb[tp_me] = bq[...]
        lax.fori_loop(0, pieces, own, 0)
        for load in loads:
            load.wait()
        lax.fori_loop(0, ff // piece, turn_w1, 0)
        lax.fori_loop(0, ff // piece, turn_w2, 0)

        @pl.when(stage >= column)
        def _():
            for r in range(RELAYED):
                relay_copy(1, r).wait_recv()
                relay_copy(2, r).start()

        bq_copy.wait_recv()
        middle = direct // 2
        for first, last in ((0, middle), (direct, pieces), (middle, direct)):
            lax.fori_loop(first, last, received, 0)

    pb[:, :, 0:LANES, LANES:rows] = jnp.zeros((2, 4, LANES, rows - LANES), BF16)
    neighbour_barrier(stage, tp_peer, stages)

    def outs(m):
        return (pltpu.make_async_copy(h1b, h1_all.at[m], out_sem.at[0]),
                pltpu.make_async_copy(qkvb, qkv_all.at[m], out_sem.at[1]),
                pltpu.make_async_copy(ob.at[:, pl.ds(pl.multiple_of(tp_me * half, LANES), half)], o_all.at[m], out_sem.at[2]),
                pltpu.make_async_copy(h2b, h2_all.at[m], out_sem.at[3]),
                pltpu.make_async_copy(slb, s_all.at[m], out_sem.at[4]),
                pltpu.make_async_copy(ab, a_all.at[m], out_sem.at[5]),
                pltpu.make_async_copy(xr.at[ring_slot(m)], x_all.at[m], out_sem.at[6]))

    def mid_out(m):
        slot = parity(m)
        return pltpu.make_async_copy(midb.at[slot], mid_all.at[m], mid_sem.at[slot])

    def y_out(m):
        slot = parity(m)
        return pltpu.make_async_copy(yb.at[slot], y_all.at[m], y_sem.at[slot])

    def part_copy(m):
        slot = parity(m)
        return pltpu.make_async_remote_copy(src_ref=partb.at[slot], dst_ref=peerb.at[ring_slot(m)], send_sem=part_send.at[slot], recv_sem=part_recv.at[m],
                                            device_id={"tp": tp_peer}, device_id_type=MESH)

    def part_out(m):
        slot = parity(m)
        return pltpu.make_async_copy(partb.at[slot], part_all.at[m], y_sem.at[slot])

    def next_copy(m):
        slot = parity(m)
        return pltpu.make_async_remote_copy(src_ref=yb.at[slot], dst_ref=xr.at[ring_slot(m)], send_sem=y_send.at[slot], recv_sem=x_recv.at[m],
                                            device_id={"pp": jnp.minimum(stage + 1, last_stage)}, device_id_type=MESH)

    def x_load(m):
        return pltpu.make_async_copy(x_in.at[m], xr.at[ring_slot(m)], in_sem.at[parity(m)])

    @pl.when(stage == 0)
    def _():
        x_load(0).start()

    def layer_norm(src, dst, gain, shift):
        for r in starts(rows, ROW_CHUNK):
            normed, _ = norm_stats(src[r:r + ROW_CHUNK, :].astype(F32))
            dst[r:r + ROW_CHUNK, :] = (normed * gain + shift).astype(BF16)

    def group_base(group):
        return (group // 2) * trio + (group % 2) * (4 * width)

    def attend():
        def scores(group):
            base = group_base(group)
            for j, (start, size, offset) in enumerate(WINDOWS):
                query = head_only(qkvb[:, base + start:base + start + size], offset, width)
                key = qkvb[:, base + half + start:base + half + start + size]
                sb[group % 2, j] = dot_nt(query, key)

        def softmax(group):
            for j in range(4):
                for r0 in starts(rows, SOFT_ROWS):
                    keys = LANES * (r0 // LANES + 1)
                    row = lax.broadcasted_iota(jnp.int32, (SOFT_ROWS, keys), 0) + r0
                    col = lax.broadcasted_iota(jnp.int32, (SOFT_ROWS, keys), 1)
                    score = jnp.where(row >= col, sb[group % 2, j, r0:r0 + SOFT_ROWS, 0:keys], NEG)
                    weight = jnp.exp2((score - jnp.max(score, axis=1, keepdims=True)) * log2_scale)
                    inv = 1.0 / jnp.sum(weight, axis=1, keepdims=True)
                    pb[group % 2, j, r0:r0 + SOFT_ROWS, 0:keys] = (weight * inv).astype(BF16)

        def values(group):
            base = group_base(group) + 2 * half
            parts = [dot_nn(pb[group % 2, j], qkvb[:, base + start:base + start + size]) for j, (start, size, _) in enumerate(WINDOWS)]
            for i, piece in enumerate(join_heads(parts, width)):
                first = group * (4 * width) + i * LANES
                ob[:, first:first + LANES] = piece.astype(BF16)

        groups = d_model // (4 * width)
        scores(0)
        for group in range(groups):
            if group + 1 < groups:
                scores(group + 1)
            softmax(group)
            values(group)

    def finish(m):
        slot = parity(m)
        peer_slot = ring_slot(m)
        part_copy(m).wait_recv()

        @pl.when(m >= 2)
        def _():
            y_out(m - 2).wait()
            next_copy(m - 2).wait_send()

        for r in starts(rows, ROW_CHUNK):
            both = partb[slot, r:r + ROW_CHUNK, :].astype(F32) + peerb[peer_slot, r:r + ROW_CHUNK, :].astype(F32)
            yb[slot, r:r + ROW_CHUNK, :] = (midb[slot, r:r + ROW_CHUNK, :].astype(F32) + both + b2[...]).astype(BF16)

        @pl.when(m >= RING)
        def _():
            pl.semaphore_wait(x_free, 1)

        next_copy(m).start()
        y_out(m).start()
        part_copy(m).wait_send()

    def attn_part(m):
        slot = parity(m)
        prev = jnp.maximum(m - 1, 0)
        h1_o, qkv_o, o_o, h2_o, _, _, x_o = outs(m)
        h1_p, qkv_p, o_p, h2_p, _, _, x_p = outs(prev)

        @pl.when(stage == 0)
        def _():
            x_load(m).wait()

            @pl.when(m + 1 < subs)
            def _():
                x_load(m + 1).start()

        @pl.when(stage > 0)
        def _():
            next_copy(m).wait_recv()

        x_o.start()
        xb = xr.at[ring_slot(m)]

        @pl.when(m > 0)
        def _():
            h1_p.wait()
            qkv_p.wait()
            o_p.wait()
            h2_p.wait()

        layer_norm(xb, h1b, ln[0][...], ln[1][...])
        h1_o.start()

        for n in starts(3 * d_model, tile):
            owner, lane = divmod(n, trio)
            qkvb[:, n:n + tile] = (dot_nn(h1b[...], wq[:, n:n + tile]) + bqb[owner, :, lane:lane + tile].astype(F32)).astype(BF16)
        qkv_o.start()
        attend()
        o_o.start()

        @pl.when(m == 0)
        def _():
            wo_copy.wait_recv()

        @pl.when(m >= 2)
        def _():
            mid_out(m - 2).wait()

        for n in starts(d_model, tile):
            midb[slot, :, n:n + tile] = (xb[:, n:n + tile].astype(F32) + dot_nn(ob[...], wo[:, n:n + tile]) + bo[:, n:n + tile]).astype(BF16)
        mid_out(m).start()
        x_o.wait()

        @pl.when((stage > 0) & (m < subs - RING))
        def _():
            pl.semaphore_signal(x_free, inc=1, device_id={"pp": jnp.maximum(stage - 1, 0)}, device_id_type=MESH)

        layer_norm(midb.at[slot], h2b, ln[2][...], ln[3][...])
        h2_o.start()

    def mlp_part(m):
        slot = parity(m)
        _, _, _, _, s_o, a_o, _ = outs(m)
        _, _, _, _, s_p, a_p, _ = outs(jnp.maximum(m - 1, 0))

        @pl.when(m > 0)
        def _():
            s_p.wait()
            a_p.wait()

        for n in starts(ff, tile):
            pre = dot_nn(h2b[...], w1[:, n:n + tile]) + b1[:, n:n + tile]
            square = pre * pre
            bend = jnp.tanh(pre * (GELU_C + (GELU_C * GELU_K) * square))
            cdf = 0.5 + 0.5 * bend
            ab[:, n:n + tile] = (pre * cdf).astype(BF16)
            slb[:, n:n + tile] = cdf + (0.5 * pre) * (1.0 - bend * bend) * (GELU_C + (3.0 * GELU_C * GELU_K) * square)
        s_o.start()
        a_o.start()

        @pl.when((stage == last_stage) & (m >= 2))
        def _():
            part_out(m - 2).wait()

        for n in starts(d_model, tile):
            partb[slot, :, n:n + tile] = dot_nn(ab[...], w2[:, n:n + tile]).astype(BF16)

        @pl.when(stage < last_stage)
        def _():
            part_copy(m).start()

        @pl.when(stage == last_stage)
        def _():
            part_out(m).start()

    def step(m, carry):
        @pl.when(m < subs)
        def _():
            attn_part(m)

        @pl.when((m > 0) & (stage == last_stage - 1))
        def _():
            finish(m - 1)

        @pl.when(m < subs)
        def _():
            mlp_part(m)

        @pl.when((m >= 1) & (m <= d_model // piece))
        def _():
            tb[...] = jnp.transpose(wo[cut(m - 1), :])
            moved(tb, wot_o.at[:, cut(m - 1)])

        @pl.when((m > 0) & (stage < last_stage - 1))
        def _():
            finish(m - 1)

        return carry

    exchange_weights()
    lax.fori_loop(0, subs + 1, step, 0)

    def sent(p, carry):
        wq_copy(p).wait_send()
        return carry

    lax.fori_loop(0, direct, sent, 0)

    @pl.when(stage < column)
    def _():
        for r in range(RELAYED):
            relay_copy(0, r).wait_send()

    @pl.when(stage >= column)
    def _():
        lax.fori_loop(direct, pieces, sent, 0)
        for r in range(RELAYED):
            relay_copy(1, r).wait_send()
            relay_copy(2, r).wait_send()

    wo_copy.wait_send()
    bq_copy.wait_send()
    h1_o, qkv_o, o_o, h2_o, s_o, a_o, x_o = outs(subs - 1)
    for copy in (h1_o, qkv_o, o_o, h2_o, s_o, a_o):
        copy.wait()

    for m in (subs - 2, subs - 1):
        mid_out(m).wait()

        @pl.when(stage < last_stage)
        def _():
            y_out(m).wait()
            next_copy(m).wait_send()

        @pl.when(stage == last_stage)
        def _():
            part_out(m).wait()


def bwd_kernel(subs, stages, width, tile,
               dy_in, x_all, mid_all, s_all, qkv_all, w2t_h, w1t_h, wot_h, wqt_h, wqt_p, ln_h,
               dy_all, dpre_all, gmid_all, dqkv_all, gin_all, db1_o, db2_o, dbo_o, dbq_o, dln_o,
               w2t, w1t, wot, wqt, dyb, slb, dpb, partb, peerb, rb, midb, xb, gmb, qkvb, gib, sb, db, pb, dsb, db1, db2, dbo, dbq, dln, ln,
               w_sem, in_sem, pre_sem, out_sem, dy_sem, gi_sem, part_send, part_recv, gi_send, dy_recv, dy_free):
    stage = lax.axis_index("pp")
    tp_me = lax.axis_index("tp")
    tp_peer = 1 - tp_me
    last_stage = stages - 1
    rows, d_model = xb.shape
    half = d_model // 2
    trio = 3 * half
    ff = slb.shape[1]
    scale = width ** -0.5
    log2_scale = scale * LOG2_E

    ln[...] = ln_h[...].astype(F32)
    mine_q = pl.ds(pl.multiple_of(tp_me * trio, LANES), trio)
    theirs_q = pl.ds(pl.multiple_of(tp_peer * trio, LANES), trio)
    loads = [pltpu.make_async_copy(src, dst, w_sem.at[i]) for i, (src, dst) in enumerate((
        (w2t_h, w2t), (w1t_h, w1t), (wot_h, wot), (wqt_h, wqt.at[mine_q, :]), (wqt_p, wqt.at[theirs_q, :])))]

    def fetch(m):
        return (pltpu.make_async_copy(s_all.at[m], slb, pre_sem.at[0]),
                pltpu.make_async_copy(mid_all.at[m], midb, pre_sem.at[1]),
                pltpu.make_async_copy(qkv_all.at[m], qkvb, pre_sem.at[2]),
                pltpu.make_async_copy(x_all.at[m], xb, pre_sem.at[3]))

    fetch(0)[0].start()
    for load in loads[:2]:
        load.start()
    for copy in fetch(0)[1:]:
        copy.start()
    for acc in (db1, db2, dbo, dbq, dln):
        acc[...] = jnp.zeros_like(acc)
    for acc in (pb, dsb):
        acc[:, LANES:rows, 0:LANES] = jnp.zeros((4, rows - LANES, LANES), BF16)
    neighbour_barrier(stage, tp_peer, stages)

    def outs(m):
        return (pltpu.make_async_copy(dpb, dpre_all.at[m], out_sem.at[0]),
                pltpu.make_async_copy(gmb, gmid_all.at[m], out_sem.at[1]),
                pltpu.make_async_copy(qkvb.at[:, pl.ds(pl.multiple_of(tp_me * trio, LANES), trio)], dqkv_all.at[m], out_sem.at[2]))

    def dy_load(m):
        return pltpu.make_async_copy(dy_in.at[m], dyb.at[ring_slot(m)], in_sem.at[parity(m)])

    def dy_out(m):
        return pltpu.make_async_copy(dyb.at[ring_slot(m)], dy_all.at[m], dy_sem.at[parity(m)])

    def gi_out(m):
        slot = parity(m)
        return pltpu.make_async_copy(gib.at[slot], gin_all.at[m], gi_sem.at[slot])

    def part_copy(m):
        slot = parity(m)
        return pltpu.make_async_remote_copy(src_ref=partb.at[slot], dst_ref=peerb.at[ring_slot(m)], send_sem=part_send.at[slot], recv_sem=part_recv.at[m],
                                            device_id={"tp": tp_peer}, device_id_type=MESH)

    def prev_copy(m):
        slot = parity(m)
        return pltpu.make_async_remote_copy(src_ref=gib.at[slot], dst_ref=dyb.at[ring_slot(m)], send_sem=gi_send.at[slot], recv_sem=dy_recv.at[m],
                                            device_id={"pp": jnp.maximum(stage - 1, 0)}, device_id_type=MESH)

    @pl.when(stage == last_stage)
    def _():
        dy_load(0).start()

    def norm_grad(x_rows, grad, gain, which):
        normed, inv_std = norm_stats(x_rows)
        dln[which] += fold_rows(grad * normed)
        dln[which + 1] += fold_rows(grad)
        scaled = grad * gain
        mean_scaled = jnp.mean(scaled, axis=-1, keepdims=True)
        mean_proj = jnp.mean(scaled * normed, axis=-1, keepdims=True)
        return inv_std * (scaled - mean_scaled - normed * mean_proj)

    def mlp_part(m):
        slot = parity(m)
        slope_f = fetch(m)[0]

        dy_slot = ring_slot(m)

        @pl.when(stage == last_stage)
        def _():
            dy_load(m).wait()

            @pl.when(m + 1 < subs)
            def _():
                dy_load(m + 1).start()

        @pl.when(stage < last_stage)
        def _():
            prev_copy(m).wait_recv()

        dy_out(m).start()

        @pl.when(m == 0)
        def _():
            loads[0].wait()
            for load in loads[2:]:
                load.start()

        @pl.when(m > 0)
        def _():
            outs(m - 1)[0].wait()

        slope_f.wait()
        for n in starts(ff, tile):
            grad = dot_nn(dyb[dy_slot], w2t[:, n:n + tile]).astype(BF16).astype(F32) * slb[:, n:n + tile]
            db1[:, n:n + tile] += fold_rows(grad)
            dpb[:, n:n + tile] = grad.astype(BF16)
        outs(m)[0].start()

        @pl.when(m + 1 < subs)
        def _():
            fetch(m + 1)[0].start()

        @pl.when(m == 0)
        def _():
            loads[1].wait()

        for n in starts(d_model, tile):
            partb[slot, :, n:n + tile] = dot_nn(dpb[...], w1t[:, n:n + tile]).astype(BF16)
        part_copy(m).start()

    def attend_grad():
        def window(base, spec):
            start, size, offset = spec
            return slice(base + start, base + start + size), offset

        def scores(group, base):
            for j, spec in enumerate(WINDOWS):
                q_lanes, offset = window(base, spec)
                k_lanes, _ = window(base + half, spec)
                v_lanes, _ = window(base + 2 * half, spec)
                d_lanes, _ = window(group * (4 * width), spec)
                sb[j] = dot_nt(qkvb[:, k_lanes], head_only(qkvb[:, q_lanes], offset, width))
                db[j] = dot_nt(qkvb[:, v_lanes], head_only(rb[:, d_lanes], offset, width))

        def softmax():
            for j in range(4):
                for q0 in starts(rows, LANES):
                    keys, lanes = q0 + LANES, slice(q0, q0 + LANES)
                    krow = lax.broadcasted_iota(jnp.int32, (keys, LANES), 0)
                    qcol = lax.broadcasted_iota(jnp.int32, (keys, LANES), 1) + q0
                    score = jnp.where(qcol >= krow, sb[j, 0:keys, lanes], NEG)
                    weight = jnp.exp2((score - jnp.max(score, axis=0, keepdims=True)) * log2_scale)
                    prob = weight * (1.0 / jnp.sum(weight, axis=0, keepdims=True))
                    pb[j, 0:keys, lanes] = prob.astype(BF16)
                    d_prob = db[j, 0:keys, lanes]
                    d_score = prob * (d_prob - jnp.sum(prob * d_prob, axis=0, keepdims=True))
                    dsb[j, 0:keys, lanes] = d_score.astype(BF16)

        def products(group, base):
            d_query, d_key, d_value = [], [], []
            for j, spec in enumerate(WINDOWS):
                q_lanes, _ = window(base, spec)
                k_lanes, _ = window(base + half, spec)
                d_lanes, _ = window(group * (4 * width), spec)
                d_value.append(dot_nn(pb[j], rb[:, d_lanes]))
                d_key.append(dot_nn(dsb[j], qkvb[:, q_lanes]) * scale)
                d_query.append(dot_tn(dsb[j], qkvb[:, k_lanes]) * scale)
            for c, parts in enumerate((d_query, d_key, d_value)):
                for i, piece in enumerate(join_heads(parts, width)):
                    piece = piece.astype(BF16)
                    first = base + c * half + i * LANES
                    qkvb[:, first:first + LANES] = piece
                    dbq[:, first:first + LANES] += fold_rows(piece.astype(F32))

        for group in range(d_model // (4 * width)):
            base = (group // 2) * trio + (group % 2) * (4 * width)
            scores(group, base)
            softmax()
            products(group, base)

    def attn_part(m):
        slot = parity(m)
        _, mid_f, qkv_f, x_f = fetch(m)
        _, gm_o, dq_o = outs(m)
        peer_slot = ring_slot(m)
        dy_slot = ring_slot(m)
        mid_f.wait()

        @pl.when(m > 0)
        def _():
            outs(m - 1)[1].wait()

        @pl.when(m == 0)
        def _():
            for load in loads[2:]:
                load.wait()

        part_copy(m).wait_recv()
        for r in starts(rows, ROW_CHUNK):
            rr = slice(r, r + ROW_CHUNK)
            grad = (partb[slot, rr, :].astype(F32) + peerb[peer_slot, rr, :].astype(F32)).astype(BF16).astype(F32)
            d_y = dyb[dy_slot, rr, :].astype(F32)
            db2[...] += fold_rows(d_y)
            total = d_y + norm_grad(midb[rr, :].astype(F32), grad, ln[2:3, :], 2)
            gmb[rr, :] = total.astype(BF16)
            dbo[...] += fold_rows(total)
        gm_o.start()
        dy_out(m).wait()

        @pl.when((stage < last_stage) & (m < subs - RING))
        def _():
            pl.semaphore_signal(dy_free, inc=1, device_id={"pp": jnp.minimum(stage + 1, last_stage)}, device_id_type=MESH)

        @pl.when(m + 1 < subs)
        def _():
            fetch(m + 1)[1].start()

        for n in starts(d_model, tile):
            rb[:, n:n + tile] = dot_nn(gmb[...], wot[:, n:n + tile]).astype(BF16)
        qkv_f.wait()
        attend_grad()
        dq_o.start()
        part_copy(m).wait_send()
        for n in starts(d_model, tile):
            rb[:, n:n + tile] = dot_nn(qkvb[...], wqt[:, n:n + tile]).astype(BF16)
        x_f.wait()

        @pl.when(m >= 2)
        def _():
            gi_out(m - 2).wait()

            @pl.when(stage > 0)
            def _():
                prev_copy(m - 2).wait_send()

        for r in starts(rows, ROW_CHUNK):
            rr = slice(r, r + ROW_CHUNK)
            total = gmb[rr, :].astype(F32) + norm_grad(xb[rr, :].astype(F32), rb[rr, :].astype(F32), ln[0:1, :], 0)
            gib[slot, rr, :] = total.astype(BF16)

        @pl.when(stage > 0)
        def _():
            @pl.when(m >= RING)
            def _():
                pl.semaphore_wait(dy_free, 1)

            prev_copy(m).start()

        gi_out(m).start()
        dq_o.wait()

        @pl.when(m + 1 < subs)
        def _():
            fetch(m + 1)[2].start()
            fetch(m + 1)[3].start()

    def step(m, carry):
        @pl.when(m < subs)
        def _():
            mlp_part(m)

        @pl.when(m > 0)
        def _():
            attn_part(m - 1)

        return carry

    lax.fori_loop(0, subs + 1, step, 0)
    for acc, out in ((db1, db1_o), (db2, db2_o), (dbo, dbo_o)):
        out[...] = jnp.sum(acc[...], axis=0, keepdims=True)
    dbq_o[...] = jnp.sum(dbq[:, mine_q], axis=0, keepdims=True)
    dln_o[...] = jnp.sum(dln[...], axis=1)
    for copy in outs(subs - 1)[:2]:
        copy.wait()
    for m in (subs - 2, subs - 1):
        gi_out(m).wait()

        @pl.when(stage > 0)
        def _():
            prev_copy(m).wait_send()


ANY = pl.BlockSpec(memory_space=pl.ANY)
VMEM = pl.BlockSpec(memory_space=pltpu.VMEM)
DMA = pltpu.SemaphoreType.DMA
VMEM_LIMIT = 67043328


def fwd_call(stages, width, tile, x_in, wqt_own, wo_own, w1, w2, bq, bo, b1, b2, ln):
    subs, rows, d_model = x_in.shape
    ff = w1.shape[1]
    half = d_model // 2
    trio = 3 * half

    def hbm(cols, dtype=BF16):
        return jax.ShapeDtypeStruct((subs, rows, cols), dtype)

    def buf(cols, dtype=BF16):
        return pltpu.VMEM((rows, cols), dtype)

    def two(cols):
        return pltpu.VMEM((2, rows, cols), BF16)

    weights = 2 * (4 * d_model * d_model + 2 * d_model * ff)
    return pl.pallas_call(
        functools.partial(fwd_kernel, subs, stages, width, tile),
        name="fwd_stage",
        out_shape=(hbm(d_model), hbm(3 * d_model), hbm(half), hbm(d_model), hbm(d_model), hbm(d_model), hbm(ff, F32), hbm(ff), hbm(d_model), hbm(d_model),
                   jax.ShapeDtypeStruct((trio, d_model), BF16), jax.ShapeDtypeStruct((d_model, d_model), BF16), jax.ShapeDtypeStruct((ff, d_model), BF16), jax.ShapeDtypeStruct((d_model, ff), BF16),
                   *[jax.ShapeDtypeStruct((RELAYED, rows, d_model), BF16)] * 2),
        in_specs=[ANY] * 5 + [VMEM] * 5,
        out_specs=[ANY] * 16,
        scratch_shapes=[
            pltpu.VMEM((d_model, 3 * d_model), BF16), pltpu.VMEM((d_model, d_model), BF16), pltpu.VMEM(w1.shape, BF16), pltpu.VMEM(w2.shape, BF16),
            pltpu.VMEM((RING, rows, d_model), BF16), buf(d_model), buf(3 * d_model), buf(d_model), two(d_model), buf(d_model), buf(ff, F32), buf(ff), two(d_model), pltpu.VMEM((RING, rows, d_model), BF16), two(d_model),
            pltpu.VMEM((2, 4, rows, rows), F32), pltpu.VMEM((2, 4, rows, rows), BF16), pltpu.VMEM((2, 1, trio), BF16), pltpu.VMEM((d_model, 256), BF16), pltpu.VMEM((1, ff + 6 * d_model), F32),
            DMA((3,)), DMA, DMA((trio // 256,)), DMA((trio // 256,)), DMA, DMA, DMA, DMA, DMA((3, RELAYED)), DMA((2, RELAYED)), DMA((2,)), DMA((7,)), DMA((2,)), DMA((2,)), DMA((2,)), DMA((subs,)), DMA((2,)), DMA((subs,)), pltpu.SemaphoreType.REGULAR,
        ],
        cost_estimate=pl.CostEstimate(flops=subs * rows * weights, bytes_accessed=weights + subs * rows * d_model * 30, transcendentals=subs * rows * (ff + rows * 16)),
        compiler_params=pltpu.CompilerParams(collective_id=0, has_side_effects=True, vmem_limit_bytes=VMEM_LIMIT),
    )(x_in, wqt_own, wo_own, w1, w2, bq, bo, b1, b2, ln)


def bwd_call(stages, width, tile, dy_in, x_all, mid_all, s_all, qkv_all, w2t, w1t, wot, wqt_own, wqt_peer, ln):
    subs, rows, d_model = dy_in.shape
    ff = s_all.shape[2]
    half = d_model // 2
    trio = 3 * half

    def hbm(cols, dtype=BF16):
        return jax.ShapeDtypeStruct((subs, rows, cols), dtype)

    def buf(cols, dtype=BF16):
        return pltpu.VMEM((rows, cols), dtype)

    def two(cols):
        return pltpu.VMEM((2, rows, cols), BF16)

    ring = pltpu.VMEM((RING, rows, d_model), BF16)

    def acc(*shape):
        return jax.ShapeDtypeStruct(shape, F32)

    weights = 2 * (4 * d_model * d_model + 2 * d_model * ff)
    return pl.pallas_call(
        functools.partial(bwd_kernel, subs, stages, width, tile),
        name="bwd_stage",
        out_shape=(hbm(d_model), hbm(ff), hbm(d_model), hbm(trio), hbm(d_model),
                   acc(1, ff), acc(1, d_model), acc(1, d_model), acc(1, trio), acc(4, d_model)),
        in_specs=[ANY] * 10 + [VMEM],
        out_specs=[ANY] * 5 + [VMEM] * 5,
        scratch_shapes=[
            pltpu.VMEM(w2t.shape, BF16), pltpu.VMEM(w1t.shape, BF16), pltpu.VMEM((d_model, d_model), BF16), pltpu.VMEM((3 * d_model, d_model), BF16),
            ring, buf(ff, F32), buf(ff), two(d_model), ring, buf(d_model), buf(d_model), buf(d_model), buf(d_model), buf(3 * d_model), two(d_model),
            pltpu.VMEM((4, rows, rows), F32), pltpu.VMEM((4, rows, rows), F32), pltpu.VMEM((4, rows, rows), BF16), pltpu.VMEM((4, rows, rows), BF16),
            pltpu.VMEM((8, ff), F32), pltpu.VMEM((8, d_model), F32), pltpu.VMEM((8, d_model), F32), pltpu.VMEM((8, 3 * d_model), F32), pltpu.VMEM((4, 8, d_model), F32), pltpu.VMEM((4, d_model), F32),
            DMA((5,)), DMA((2,)), DMA((4,)), DMA((3,)), DMA((2,)), DMA((2,)), DMA((2,)), DMA((subs,)), DMA((2,)), DMA((subs,)), pltpu.SemaphoreType.REGULAR,
        ],
        cost_estimate=pl.CostEstimate(flops=subs * rows * weights, bytes_accessed=weights + subs * rows * d_model * 30, transcendentals=subs * rows * (ff + rows * 16)),
        compiler_params=pltpu.CompilerParams(collective_id=1, has_side_effects=True, vmem_limit_bytes=VMEM_LIMIT),
    )(dy_in, x_all, mid_all, s_all, qkv_all, w2t, w1t, wot, wqt_own, wqt_peer, ln)


def grad_kernel(last_stage, extra_count, stage, left, right, *refs):
    extras, out, passed = refs[:extra_count], refs[extra_count], refs[extra_count + 1:]
    if len(extras) == len(passed):
        for src, dst in zip(extras, passed):
            dst[...] = src[...]
    else:
        y, mid, own, peer, b2 = extras

        @pl.when(stage[0] < last_stage)
        def _():
            passed[0][...] = y[...]

        @pl.when(stage[0] == last_stage)
        def _():
            both = own[...].astype(F32) + peer[...].astype(F32)
            passed[0][...] = (mid[...].astype(F32) + both + b2[...].astype(F32)).astype(BF16)

    @pl.when(pl.program_id(1) == 0)
    def _():
        out[...] = jnp.zeros_like(out)

    n_tile = 512
    for n in starts(out.shape[1], n_tile):
        out[:, n:n + n_tile] += dot_tn(left[...], right[:, n:n + n_tile])


def grad_call(stage, last_stage, left, right, m_block, n_block, k_block, extras=(), passed=0):
    tokens, m_size = left.shape
    n_size = right.shape[1]
    m_count = m_size // m_block
    grid = (m_count * (n_size // n_block), tokens // k_block)
    steps = grid[0] * grid[1]

    def spec(array, used=lambda s: 1):
        if array.ndim == 2:
            return pl.BlockSpec(array.shape, lambda i, k, s: (0, 0))
        block = (array.shape[0] // steps,) + array.shape[1:]
        return pl.BlockSpec(block, lambda i, k, s: ((i * grid[1] + k) * used(s), 0, 0))

    in_specs = [pl.BlockSpec((k_block, m_block), lambda i, k, s: (k, i % m_count)), pl.BlockSpec((k_block, n_block), lambda i, k, s: (k, i // m_count))]
    if len(extras) > passed:
        in_specs += [spec(extras[0], lambda s: 1 - s[0] // last_stage)] + [spec(array, lambda s: s[0] // last_stage) for array in extras[1:]]
    else:
        in_specs += [spec(array) for array in extras]
    moved = 2 * tokens * (m_size * (n_size // n_block) + n_size * m_count) + 4 * m_size * n_size
    return pl.pallas_call(
        functools.partial(grad_kernel, last_stage, len(extras)),
        name="weight_grad",
        grid_spec=pltpu.PrefetchScalarGridSpec(
            num_scalar_prefetch=1, grid=grid, in_specs=in_specs,
            out_specs=[pl.BlockSpec((m_block, n_block), lambda i, k, s: (i % m_count, i // m_count))] + [spec(array) for array in extras[:passed]]),
        out_shape=[jax.ShapeDtypeStruct((m_size, n_size), F32)] + [jax.ShapeDtypeStruct(array.shape, array.dtype) for array in extras[:passed]],
        cost_estimate=pl.CostEstimate(flops=2 * tokens * m_size * n_size, bytes_accessed=moved, transcendentals=0),
        compiler_params=pltpu.CompilerParams(dimension_semantics=("arbitrary", "arbitrary"), vmem_limit_bytes=VMEM_LIMIT),
    )(stage, left, right, *extras)


def solution(mesh):
    stages = mesh.shape["pp"]

    def stage_program(x_in, dy_out, w_qkv, b_qkv, w_out, b_out, ln_par, w_fc1, b_fc1, w_fc2, b_fc2):
        micro, batch, rows, d_model = x_in.shape
        heads, width = w_qkv.shape[3:]
        half = heads * width
        subs = micro * batch
        tile = half

        wqt_own = jnp.transpose(w_qkv[0], (0, 2, 3, 1)).reshape(3 * half, d_model)
        ln = ln_par[0]
        x_all, qkv_all, o_all, mid_all, h1_all, h2_all, s_all, a_all, y_all, part_all, wqt_peer, wot, w1t, w2t, _, _ = fwd_call(
            stages, width, tile, x_in.reshape(subs, rows, d_model), wqt_own, w_out[0].reshape(half, d_model), w_fc1[0], w_fc2[0], b_qkv.reshape(1, -1), b_out, b_fc1, b_fc2, ln)
        dy_all, dpre_all, gmid_all, dqkv_all, gin_all, db1, db2, dbo, dbq, dln = bwd_call(
            stages, width, tile, dy_out.reshape(subs, rows, d_model), x_all, mid_all, s_all, qkv_all, w2t, w1t, wot, wqt_own, wqt_peer, ln)

        def flat(stack):
            return stack.reshape(subs * rows, -1)

        last_stage = stages - 1
        stage = lax.axis_index("pp").reshape(1)
        held, _ = lax.optimization_barrier((part_all, gin_all))
        peer_part = lax.ppermute(held, ("tp", "pp"), [(i, (i + stages) % (2 * stages) if i % stages == last_stage else i) for i in range(2 * stages)])
        g_w_out, dbo, dln, db1, db2 = grad_call(stage, last_stage, flat(o_all), flat(gmid_all), half, d_model, d_model, (dbo, dln, db1, db2), 4)
        g_w_fc1, g_in = grad_call(stage, last_stage, flat(h2_all), flat(dpre_all), d_model, 1024, d_model, (gin_all,), 1)
        g_w_fc2, h_out = grad_call(stage, last_stage, flat(a_all), flat(dy_all), 1024, d_model, d_model, (y_all, mid_all, part_all, peer_part, b_fc2), 1)
        g_w_qkv = lax.optimization_barrier(dot_tn(flat(dqkv_all), flat(h1_all)))
        g_w_out = g_w_out.reshape(heads, width, d_model)
        g_w_qkv = jnp.transpose(g_w_qkv.reshape(3, heads, width, d_model), (0, 3, 1, 2))
        g_b_qkv = dbq.reshape(3, heads, width)
        act = (1, micro, batch, rows, d_model)
        return (h_out.reshape(act), g_in.reshape(act), g_w_qkv[None], g_b_qkv[None], g_w_out[None], dbo,
                dln[None], g_w_fc1[None], db1, g_w_fc2[None], db2)

    act_spec = P(None, "dp", None, None)
    arg_specs = (act_spec, act_spec,
                 P("pp", None, None, "tp", None), P("pp", None, "tp", None), P("pp", "tp", None, None),
                 P("pp", None), P("pp", None, None), P("pp", None, "tp"), P("pp", "tp"),
                 P("pp", "tp", None), P("pp", None))
    stage_spec = P("pp", None, "dp", None, None)
    grad_axes = ("dp", "pp")
    result_specs = (stage_spec, stage_spec,
                    P(grad_axes, None, None, "tp", None), P(grad_axes, None, "tp", None), P(grad_axes, "tp", None, None),
                    P(grad_axes, None), P(grad_axes, None, None), P(grad_axes, None, "tp"), P(grad_axes, "tp"),
                    P(grad_axes, "tp", None), P(grad_axes, None))
    return jax.shard_map(stage_program, mesh=mesh, in_specs=arg_specs, out_specs=result_specs, check_vma=False)
```

```python
import functools

import jax
import jax.numpy as jnp
from jax import lax
from jax.experimental import pallas as pl
from jax.experimental.pallas import tpu as pltpu
from jax.sharding import PartitionSpec as P

LN_EPS = 1e-5
F32 = jnp.float32
BF16 = jnp.bfloat16
MESH = pl.DeviceIdType.MESH
NEG = -1e30
ROW_CHUNK = 32
GELU_C = 0.7978845608028654
GELU_K = 0.044715
LOG2_E = 1.4426950408889634
SOFT_ROWS = 64
RING = 4
LANES = 128
RELAYED = 3

WINDOWS = ((0, 128, 0), (0, 256, 96), (128, 256, 64), (256, 128, 32))


def starts(total, step):
    return range(0, total, step)


def parity(m):
    return lax.rem(m, 2)


def ring_slot(m):
    return lax.rem(m, RING)


def dot_nn(lhs, rhs):
    return lax.dot_general(lhs, rhs, (((1,), (0,)), ((), ())), preferred_element_type=F32)


def dot_nt(lhs, rhs):
    return lax.dot_general(lhs, rhs, (((1,), (1,)), ((), ())), preferred_element_type=F32)


def dot_tn(lhs, rhs):
    return lax.dot_general(lhs, rhs, (((0,), (0,)), ((), ())), preferred_element_type=F32)


def head_only(window, offset, width):
    lane = lax.broadcasted_iota(jnp.int32, window.shape, 1)
    return jnp.where((lane >= offset) & (lane < offset + width), window, jnp.zeros_like(window))


def join_heads(parts, width):
    lane = lax.broadcasted_iota(jnp.int32, (parts[0].shape[0], LANES), 1)
    first = jnp.where(lane < width, parts[0], parts[1][:, :LANES])
    second = jnp.where(lane < 2 * width - LANES, parts[1][:, LANES:], parts[2][:, :LANES])
    third = jnp.where(lane < 3 * width - 256, parts[2][:, LANES:], parts[3])
    return first, second, third


def norm_stats(x_wide):
    centered = x_wide - jnp.mean(x_wide, axis=-1, keepdims=True)
    inv_std = lax.rsqrt(jnp.mean(centered * centered, axis=-1, keepdims=True) + LN_EPS)
    return centered * inv_std, inv_std


def fold_rows(block):
    rows, cols = block.shape
    return jnp.sum(block.reshape(rows // 8, 8, cols), axis=0)


def neighbour_barrier(stage, tp_peer, stages):
    barrier = pltpu.get_barrier_semaphore()
    pl.semaphore_signal(barrier, inc=1, device_id={"tp": tp_peer}, device_id_type=MESH)
    for step in range(1, stages):
        pl.semaphore_signal(barrier, inc=1, device_id={"pp": lax.rem(stage + step, stages)}, device_id_type=MESH)
    pl.semaphore_wait(barrier, stages)


def fwd_kernel(subs, stages, width, tile,
               x_in, wqt_h, wo_h, w1_h, w2_h, bq, bo_h, b1_h, b2_h, ln_h,
               x_all, qkv_all, o_all, mid_all, h1_all, h2_all, s_all, a_all, y_all, part_all, wqt_p, wot_o, w1t_o, w2t_o, relay_in, relay_out,
               wq, wo, w1, w2, xr, h1b, qkvb, ob, midb, h2b, slb, ab, partb, peerb, yb, sb, pb, bqb, tb, par,
               w_sem, t_sem, wq_send, wq_recv, wo_send, wo_recv, bq_send, bq_recv, relay_send, relay_recv, in_sem, out_sem, mid_sem, y_sem, part_send, part_recv, y_send, x_recv, x_free):
    stage = lax.axis_index("pp")
    tp_me = lax.axis_index("tp")
    tp_peer = 1 - tp_me
    last_stage = stages - 1
    _, rows, d_model = xr.shape
    half = d_model // 2
    trio = 3 * half
    ff = slb.shape[1]
    scale = width ** -0.5
    log2_scale = scale * LOG2_E

    first = 0
    rows_of = []
    for row in (bo_h, b1_h, b2_h, *(ln_h.at[i:i + 1, :] for i in range(4))):
        lanes = slice(first, first + row.shape[1])
        par[:, lanes] = row[...].astype(F32)
        rows_of.append(par.at[:, lanes])
        first = lanes.stop
    bo, b1, b2, *ln = rows_of
    mine = pl.ds(pl.multiple_of(tp_me * half, LANES), half)
    piece = 256
    pieces = trio // piece
    peer_id = {"device_id": {"tp": tp_peer}, "device_id_type": MESH}
    loads = [pltpu.make_async_copy(src, dst, w_sem.at[i]) for i, (src, dst) in enumerate(((wo_h, wo.at[mine, :]), (w1_h, w1), (w2_h, w2)))]

    def cut(p):
        return pl.ds(pl.multiple_of(p * piece, piece), piece)

    def wq_copy(p):
        return pltpu.make_async_remote_copy(src_ref=wqt_h.at[cut(p), :], dst_ref=wqt_p.at[cut(p), :], send_sem=wq_send.at[p], recv_sem=wq_recv.at[p], **peer_id)

    wo_copy = pltpu.make_async_remote_copy(src_ref=wo_h, dst_ref=wo.at[mine, :], send_sem=wo_send, recv_sem=wo_recv, **peer_id)
    bq_copy = pltpu.make_async_remote_copy(src_ref=bq, dst_ref=bqb.at[tp_me], send_sem=bq_send, recv_sem=bq_recv, **peer_id)

    column = stages // 2
    direct = pieces - RELAYED

    def relay_copy(leg, r):
        src = (wqt_h.at[cut(direct + r), :], relay_in.at[r], relay_out.at[r])[leg]
        dst = (relay_in.at[r], relay_out.at[r], wqt_p.at[cut(direct + r), :])[leg]
        there = ({"pp": jnp.minimum(stage + column, last_stage)}, {"tp": tp_peer}, {"pp": jnp.maximum(stage - column, 0)})[leg]
        recv_sem = wq_recv.at[direct + r] if leg == 2 else relay_recv.at[leg, r]
        return pltpu.make_async_remote_copy(src_ref=src, dst_ref=dst, send_sem=relay_send.at[leg, r], recv_sem=recv_sem, device_id=there, device_id_type=MESH)

    def moved(src, dst):
        copy = pltpu.make_async_copy(src, dst, t_sem)
        copy.start()
        copy.wait()

    def turn(source, owner, p):
        moved(source.at[cut(p), :], h1b)
        wq[:, pl.ds(pl.multiple_of(owner * trio + p * piece, LANES), piece)] = jnp.transpose(h1b[...])

    def exchange_weights():
        def send(p, carry):
            wq_copy(p).start()
            return carry

        def own(p, carry):
            turn(wqt_h, tp_me, p)
            return carry

        def turn_w1(p, carry):
            h2b[...] = jnp.transpose(w1[:, cut(p)])
            moved(h2b, w1t_o.at[cut(p), :])
            return carry

        def turn_w2(p, carry):
            tb[...] = jnp.transpose(w2[cut(p), :])
            moved(tb, w2t_o.at[:, cut(p)])
            return carry

        def received(p, carry):
            wq_copy(p).wait_recv()
            turn(wqt_p, tp_peer, p)
            return carry

        bq_copy.start()
        for load in loads:
            load.start()
        lax.fori_loop(0, RELAYED, send, 0)

        @pl.when(stage < column)
        def _():
            for r in range(RELAYED):
                relay_copy(0, r).start()
            lax.fori_loop(RELAYED, direct, send, 0)

        @pl.when(stage >= column)
        def _():
            for r in range(RELAYED):
                relay_copy(0, r).wait_recv()
                relay_copy(1, r).start()
            lax.fori_loop(RELAYED, pieces, send, 0)

        wo_copy.start()
        bqb[tp_me] = bq[...]
        lax.fori_loop(0, pieces, own, 0)
        for load in loads:
            load.wait()
        lax.fori_loop(0, ff // piece, turn_w1, 0)
        lax.fori_loop(0, ff // piece, turn_w2, 0)

        @pl.when(stage >= column)
        def _():
            for r in range(RELAYED):
                relay_copy(1, r).wait_recv()
                relay_copy(2, r).start()

        bq_copy.wait_recv()
        middle = direct // 2
        for first, last in ((0, middle), (direct, pieces), (middle, direct)):
            lax.fori_loop(first, last, received, 0)

    pb[:, :, 0:LANES, LANES:rows] = jnp.zeros((2, 4, LANES, rows - LANES), BF16)
    neighbour_barrier(stage, tp_peer, stages)

    def outs(m):
        return (pltpu.make_async_copy(h1b, h1_all.at[m], out_sem.at[0]),
                pltpu.make_async_copy(qkvb, qkv_all.at[m], out_sem.at[1]),
                pltpu.make_async_copy(ob.at[:, pl.ds(pl.multiple_of(tp_me * half, LANES), half)], o_all.at[m], out_sem.at[2]),
                pltpu.make_async_copy(h2b, h2_all.at[m], out_sem.at[3]),
                pltpu.make_async_copy(slb, s_all.at[m], out_sem.at[4]),
                pltpu.make_async_copy(ab, a_all.at[m], out_sem.at[5]),
                pltpu.make_async_copy(xr.at[ring_slot(m)], x_all.at[m], out_sem.at[6]))

    def mid_out(m):
        slot = parity(m)
        return pltpu.make_async_copy(midb.at[slot], mid_all.at[m], mid_sem.at[slot])

    def y_out(m):
        slot = parity(m)
        return pltpu.make_async_copy(yb.at[slot], y_all.at[m], y_sem.at[slot])

    def part_copy(m):
        slot = parity(m)
        return pltpu.make_async_remote_copy(src_ref=partb.at[slot], dst_ref=peerb.at[ring_slot(m)], send_sem=part_send.at[slot], recv_sem=part_recv.at[m],
                                            device_id={"tp": tp_peer}, device_id_type=MESH)

    def part_out(m):
        slot = parity(m)
        return pltpu.make_async_copy(partb.at[slot], part_all.at[m], y_sem.at[slot])

    def next_copy(m):
        slot = parity(m)
        return pltpu.make_async_remote_copy(src_ref=yb.at[slot], dst_ref=xr.at[ring_slot(m)], send_sem=y_send.at[slot], recv_sem=x_recv.at[m],
                                            device_id={"pp": jnp.minimum(stage + 1, last_stage)}, device_id_type=MESH)

    def x_load(m):
        return pltpu.make_async_copy(x_in.at[m], xr.at[ring_slot(m)], in_sem.at[parity(m)])

    @pl.when(stage == 0)
    def _():
        x_load(0).start()

    def layer_norm(src, dst, gain, shift):
        for r in starts(rows, ROW_CHUNK):
            normed, _ = norm_stats(src[r:r + ROW_CHUNK, :].astype(F32))
            dst[r:r + ROW_CHUNK, :] = (normed * gain + shift).astype(BF16)

    def group_base(group):
        return (group // 2) * trio + (group % 2) * (4 * width)

    def attend():
        def scores(group):
            base = group_base(group)
            for j, (start, size, offset) in enumerate(WINDOWS):
                query = head_only(qkvb[:, base + start:base + start + size], offset, width)
                key = qkvb[:, base + half + start:base + half + start + size]
                sb[group % 2, j] = dot_nt(query, key)

        def softmax(group):
            for j in range(4):
                for r0 in starts(rows, SOFT_ROWS):
                    keys = LANES * (r0 // LANES + 1)
                    row = lax.broadcasted_iota(jnp.int32, (SOFT_ROWS, keys), 0) + r0
                    col = lax.broadcasted_iota(jnp.int32, (SOFT_ROWS, keys), 1)
                    score = jnp.where(row >= col, sb[group % 2, j, r0:r0 + SOFT_ROWS, 0:keys], NEG)
                    weight = jnp.exp2((score - jnp.max(score, axis=1, keepdims=True)) * log2_scale)
                    inv = 1.0 / jnp.sum(weight, axis=1, keepdims=True)
                    pb[group % 2, j, r0:r0 + SOFT_ROWS, 0:keys] = (weight * inv).astype(BF16)

        def values(group):
            base = group_base(group) + 2 * half
            parts = [dot_nn(pb[group % 2, j], qkvb[:, base + start:base + start + size]) for j, (start, size, _) in enumerate(WINDOWS)]
            for i, piece in enumerate(join_heads(parts, width)):
                first = group * (4 * width) + i * LANES
                ob[:, first:first + LANES] = piece.astype(BF16)

        groups = d_model // (4 * width)
        scores(0)
        for group in range(groups):
            if group + 1 < groups:
                scores(group + 1)
            softmax(group)
            values(group)

    def finish(m):
        slot = parity(m)
        peer_slot = ring_slot(m)
        part_copy(m).wait_recv()

        @pl.when(m >= 2)
        def _():
            y_out(m - 2).wait()
            next_copy(m - 2).wait_send()

        for r in starts(rows, ROW_CHUNK):
            both = partb[slot, r:r + ROW_CHUNK, :].astype(F32) + peerb[peer_slot, r:r + ROW_CHUNK, :].astype(F32)
            yb[slot, r:r + ROW_CHUNK, :] = (midb[slot, r:r + ROW_CHUNK, :].astype(F32) + both + b2[...]).astype(BF16)

        @pl.when(m >= RING)
        def _():
            pl.semaphore_wait(x_free, 1)

        next_copy(m).start()
        y_out(m).start()
        part_copy(m).wait_send()

    def attn_part(m):
        slot = parity(m)
        prev = jnp.maximum(m - 1, 0)
        h1_o, qkv_o, o_o, h2_o, _, _, x_o = outs(m)
        h1_p, qkv_p, o_p, h2_p, _, _, x_p = outs(prev)

        @pl.when(stage == 0)
        def _():
            x_load(m).wait()

            @pl.when(m + 1 < subs)
            def _():
                x_load(m + 1).start()

        @pl.when(stage > 0)
        def _():
            next_copy(m).wait_recv()

        x_o.start()
        xb = xr.at[ring_slot(m)]

        @pl.when(m > 0)
        def _():
            h1_p.wait()
            qkv_p.wait()
            o_p.wait()
            h2_p.wait()

        layer_norm(xb, h1b, ln[0][...], ln[1][...])
        h1_o.start()

        for n in starts(3 * d_model, tile):
            owner, lane = divmod(n, trio)
            qkvb[:, n:n + tile] = (dot_nn(h1b[...], wq[:, n:n + tile]) + bqb[owner, :, lane:lane + tile].astype(F32)).astype(BF16)
        qkv_o.start()
        attend()
        o_o.start()

        @pl.when(m == 0)
        def _():
            wo_copy.wait_recv()

        @pl.when(m >= 2)
        def _():
            mid_out(m - 2).wait()

        for n in starts(d_model, tile):
            midb[slot, :, n:n + tile] = (xb[:, n:n + tile].astype(F32) + dot_nn(ob[...], wo[:, n:n + tile]) + bo[:, n:n + tile]).astype(BF16)
        mid_out(m).start()
        x_o.wait()

        @pl.when((stage > 0) & (m < subs - RING))
        def _():
            pl.semaphore_signal(x_free, inc=1, device_id={"pp": jnp.maximum(stage - 1, 0)}, device_id_type=MESH)

        layer_norm(midb.at[slot], h2b, ln[2][...], ln[3][...])
        h2_o.start()

    def mlp_part(m):
        slot = parity(m)
        _, _, _, _, s_o, a_o, _ = outs(m)
        _, _, _, _, s_p, a_p, _ = outs(jnp.maximum(m - 1, 0))

        @pl.when(m > 0)
        def _():
            s_p.wait()
            a_p.wait()

        for n in starts(ff, tile):
            pre = dot_nn(h2b[...], w1[:, n:n + tile]) + b1[:, n:n + tile]
            square = pre * pre
            bend = jnp.tanh(pre * (GELU_C + (GELU_C * GELU_K) * square))
            cdf = 0.5 + 0.5 * bend
            ab[:, n:n + tile] = (pre * cdf).astype(BF16)
            slb[:, n:n + tile] = cdf + (0.5 * pre) * (1.0 - bend * bend) * (GELU_C + (3.0 * GELU_C * GELU_K) * square)
        s_o.start()
        a_o.start()

        @pl.when((stage == last_stage) & (m >= 2))
        def _():
            part_out(m - 2).wait()

        for n in starts(d_model, tile):
            partb[slot, :, n:n + tile] = dot_nn(ab[...], w2[:, n:n + tile]).astype(BF16)

        @pl.when(stage < last_stage)
        def _():
            part_copy(m).start()

        @pl.when(stage == last_stage)
        def _():
            part_out(m).start()

    def step(m, carry):
        @pl.when(m < subs)
        def _():
            attn_part(m)
            mlp_part(m)

        @pl.when((m >= 1) & (m <= d_model // piece))
        def _():
            tb[...] = jnp.transpose(wo[cut(m - 1), :])
            moved(tb, wot_o.at[:, cut(m - 1)])

        @pl.when((m > 0) & (stage < last_stage))
        def _():
            finish(m - 1)

        return carry

    exchange_weights()
    lax.fori_loop(0, subs + 1, step, 0)

    def sent(p, carry):
        wq_copy(p).wait_send()
        return carry

    lax.fori_loop(0, direct, sent, 0)

    @pl.when(stage < column)
    def _():
        for r in range(RELAYED):
            relay_copy(0, r).wait_send()

    @pl.when(stage >= column)
    def _():
        lax.fori_loop(direct, pieces, sent, 0)
        for r in range(RELAYED):
            relay_copy(1, r).wait_send()
            relay_copy(2, r).wait_send()

    wo_copy.wait_send()
    bq_copy.wait_send()
    h1_o, qkv_o, o_o, h2_o, s_o, a_o, x_o = outs(subs - 1)
    for copy in (h1_o, qkv_o, o_o, h2_o, s_o, a_o):
        copy.wait()

    for m in (subs - 2, subs - 1):
        mid_out(m).wait()

        @pl.when(stage < last_stage)
        def _():
            y_out(m).wait()
            next_copy(m).wait_send()

        @pl.when(stage == last_stage)
        def _():
            part_out(m).wait()


def bwd_kernel(subs, stages, width, tile,
               dy_in, x_all, mid_all, s_all, qkv_all, w2t_h, w1t_h, wot_h, wqt_h, wqt_p, ln_h,
               dy_all, dpre_all, gmid_all, dqkv_all, gin_all, db1_o, db2_o, dbo_o, dbq_o, dln_o,
               w2t, w1t, wot, wqt, dyb, slb, dpb, partb, peerb, rb, midb, xb, gmb, qkvb, gib, sb, db, pb, dsb, db1, db2, dbo, dbq, dln, ln,
               w_sem, in_sem, pre_sem, out_sem, dy_sem, gi_sem, part_send, part_recv, gi_send, dy_recv, dy_free):
    stage = lax.axis_index("pp")
    tp_me = lax.axis_index("tp")
    tp_peer = 1 - tp_me
    last_stage = stages - 1
    rows, d_model = xb.shape
    half = d_model // 2
    trio = 3 * half
    ff = slb.shape[1]
    scale = width ** -0.5
    log2_scale = scale * LOG2_E

    ln[...] = ln_h[...].astype(F32)
    mine_q = pl.ds(pl.multiple_of(tp_me * trio, LANES), trio)
    theirs_q = pl.ds(pl.multiple_of(tp_peer * trio, LANES), trio)
    loads = [pltpu.make_async_copy(src, dst, w_sem.at[i]) for i, (src, dst) in enumerate((
        (w2t_h, w2t), (w1t_h, w1t), (wot_h, wot), (wqt_h, wqt.at[mine_q, :]), (wqt_p, wqt.at[theirs_q, :])))]

    def fetch(m):
        return (pltpu.make_async_copy(s_all.at[m], slb, pre_sem.at[0]),
                pltpu.make_async_copy(mid_all.at[m], midb, pre_sem.at[1]),
                pltpu.make_async_copy(qkv_all.at[m], qkvb, pre_sem.at[2]),
                pltpu.make_async_copy(x_all.at[m], xb, pre_sem.at[3]))

    fetch(0)[0].start()
    for load in loads[:2]:
        load.start()
    for copy in fetch(0)[1:]:
        copy.start()
    for acc in (db1, db2, dbo, dbq, dln):
        acc[...] = jnp.zeros_like(acc)
    for acc in (pb, dsb):
        acc[:, LANES:rows, 0:LANES] = jnp.zeros((4, rows - LANES, LANES), BF16)
    neighbour_barrier(stage, tp_peer, stages)

    def outs(m):
        return (pltpu.make_async_copy(dpb, dpre_all.at[m], out_sem.at[0]),
                pltpu.make_async_copy(gmb, gmid_all.at[m], out_sem.at[1]),
                pltpu.make_async_copy(qkvb.at[:, pl.ds(pl.multiple_of(tp_me * trio, LANES), trio)], dqkv_all.at[m], out_sem.at[2]))

    def dy_load(m):
        return pltpu.make_async_copy(dy_in.at[m], dyb.at[ring_slot(m)], in_sem.at[parity(m)])

    def dy_out(m):
        return pltpu.make_async_copy(dyb.at[ring_slot(m)], dy_all.at[m], dy_sem.at[parity(m)])

    def gi_out(m):
        slot = parity(m)
        return pltpu.make_async_copy(gib.at[slot], gin_all.at[m], gi_sem.at[slot])

    def part_copy(m):
        slot = parity(m)
        return pltpu.make_async_remote_copy(src_ref=partb.at[slot], dst_ref=peerb.at[ring_slot(m)], send_sem=part_send.at[slot], recv_sem=part_recv.at[m],
                                            device_id={"tp": tp_peer}, device_id_type=MESH)

    def prev_copy(m):
        slot = parity(m)
        return pltpu.make_async_remote_copy(src_ref=gib.at[slot], dst_ref=dyb.at[ring_slot(m)], send_sem=gi_send.at[slot], recv_sem=dy_recv.at[m],
                                            device_id={"pp": jnp.maximum(stage - 1, 0)}, device_id_type=MESH)

    @pl.when(stage == last_stage)
    def _():
        dy_load(0).start()

    def norm_grad(x_rows, grad, gain, which):
        normed, inv_std = norm_stats(x_rows)
        dln[which] += fold_rows(grad * normed)
        dln[which + 1] += fold_rows(grad)
        scaled = grad * gain
        mean_scaled = jnp.mean(scaled, axis=-1, keepdims=True)
        mean_proj = jnp.mean(scaled * normed, axis=-1, keepdims=True)
        return inv_std * (scaled - mean_scaled - normed * mean_proj)

    def mlp_part(m):
        slot = parity(m)
        slope_f = fetch(m)[0]

        dy_slot = ring_slot(m)

        @pl.when(stage == last_stage)
        def _():
            dy_load(m).wait()

            @pl.when(m + 1 < subs)
            def _():
                dy_load(m + 1).start()

        @pl.when(stage < last_stage)
        def _():
            prev_copy(m).wait_recv()

        dy_out(m).start()

        @pl.when(m == 0)
        def _():
            loads[0].wait()
            for load in loads[2:]:
                load.start()

        @pl.when(m > 0)
        def _():
            outs(m - 1)[0].wait()

        slope_f.wait()
        for n in starts(ff, tile):
            grad = dot_nn(dyb[dy_slot], w2t[:, n:n + tile]).astype(BF16).astype(F32) * slb[:, n:n + tile]
            db1[:, n:n + tile] += fold_rows(grad)
            dpb[:, n:n + tile] = grad.astype(BF16)
        outs(m)[0].start()

        @pl.when(m + 1 < subs)
        def _():
            fetch(m + 1)[0].start()

        @pl.when(m == 0)
        def _():
            loads[1].wait()

        for n in starts(d_model, tile):
            partb[slot, :, n:n + tile] = dot_nn(dpb[...], w1t[:, n:n + tile]).astype(BF16)
        part_copy(m).start()

    def attend_grad():
        def window(base, spec):
            start, size, offset = spec
            return slice(base + start, base + start + size), offset

        def scores(group, base):
            for j, spec in enumerate(WINDOWS):
                q_lanes, offset = window(base, spec)
                k_lanes, _ = window(base + half, spec)
                v_lanes, _ = window(base + 2 * half, spec)
                d_lanes, _ = window(group * (4 * width), spec)
                sb[j] = dot_nt(qkvb[:, k_lanes], head_only(qkvb[:, q_lanes], offset, width))
                db[j] = dot_nt(qkvb[:, v_lanes], head_only(rb[:, d_lanes], offset, width))

        def softmax():
            for j in range(4):
                for q0 in starts(rows, LANES):
                    keys, lanes = q0 + LANES, slice(q0, q0 + LANES)
                    krow = lax.broadcasted_iota(jnp.int32, (keys, LANES), 0)
                    qcol = lax.broadcasted_iota(jnp.int32, (keys, LANES), 1) + q0
                    score = jnp.where(qcol >= krow, sb[j, 0:keys, lanes], NEG)
                    weight = jnp.exp2((score - jnp.max(score, axis=0, keepdims=True)) * log2_scale)
                    prob = weight * (1.0 / jnp.sum(weight, axis=0, keepdims=True))
                    pb[j, 0:keys, lanes] = prob.astype(BF16)
                    d_prob = db[j, 0:keys, lanes]
                    d_score = prob * (d_prob - jnp.sum(prob * d_prob, axis=0, keepdims=True))
                    dsb[j, 0:keys, lanes] = d_score.astype(BF16)

        def products(group, base):
            d_query, d_key, d_value = [], [], []
            for j, spec in enumerate(WINDOWS):
                q_lanes, _ = window(base, spec)
                k_lanes, _ = window(base + half, spec)
                d_lanes, _ = window(group * (4 * width), spec)
                d_value.append(dot_nn(pb[j], rb[:, d_lanes]))
                d_key.append(dot_nn(dsb[j], qkvb[:, q_lanes]) * scale)
                d_query.append(dot_tn(dsb[j], qkvb[:, k_lanes]) * scale)
            for c, parts in enumerate((d_query, d_key, d_value)):
                for i, piece in enumerate(join_heads(parts, width)):
                    piece = piece.astype(BF16)
                    first = base + c * half + i * LANES
                    qkvb[:, first:first + LANES] = piece
                    dbq[:, first:first + LANES] += fold_rows(piece.astype(F32))

        for group in range(d_model // (4 * width)):
            base = (group // 2) * trio + (group % 2) * (4 * width)
            scores(group, base)
            softmax()
            products(group, base)

    def attn_part(m):
        slot = parity(m)
        _, mid_f, qkv_f, x_f = fetch(m)
        _, gm_o, dq_o = outs(m)
        peer_slot = ring_slot(m)
        dy_slot = ring_slot(m)
        mid_f.wait()

        @pl.when(m > 0)
        def _():
            outs(m - 1)[1].wait()

        @pl.when(m == 0)
        def _():
            for load in loads[2:]:
                load.wait()

        part_copy(m).wait_recv()
        for r in starts(rows, ROW_CHUNK):
            rr = slice(r, r + ROW_CHUNK)
            grad = (partb[slot, rr, :].astype(F32) + peerb[peer_slot, rr, :].astype(F32)).astype(BF16).astype(F32)
            d_y = dyb[dy_slot, rr, :].astype(F32)
            db2[...] += fold_rows(d_y)
            total = d_y + norm_grad(midb[rr, :].astype(F32), grad, ln[2:3, :], 2)
            gmb[rr, :] = total.astype(BF16)
            dbo[...] += fold_rows(total)
        gm_o.start()
        dy_out(m).wait()

        @pl.when((stage < last_stage) & (m < subs - RING))
        def _():
            pl.semaphore_signal(dy_free, inc=1, device_id={"pp": jnp.minimum(stage + 1, last_stage)}, device_id_type=MESH)

        @pl.when(m + 1 < subs)
        def _():
            fetch(m + 1)[1].start()

        for n in starts(d_model, tile):
            rb[:, n:n + tile] = dot_nn(gmb[...], wot[:, n:n + tile]).astype(BF16)
        qkv_f.wait()
        attend_grad()
        dq_o.start()
        part_copy(m).wait_send()
        for n in starts(d_model, tile):
            rb[:, n:n + tile] = dot_nn(qkvb[...], wqt[:, n:n + tile]).astype(BF16)
        x_f.wait()

        @pl.when(m >= 2)
        def _():
            gi_out(m - 2).wait()

            @pl.when(stage > 0)
            def _():
                prev_copy(m - 2).wait_send()

        for r in starts(rows, ROW_CHUNK):
            rr = slice(r, r + ROW_CHUNK)
            total = gmb[rr, :].astype(F32) + norm_grad(xb[rr, :].astype(F32), rb[rr, :].astype(F32), ln[0:1, :], 0)
            gib[slot, rr, :] = total.astype(BF16)

        @pl.when(stage > 0)
        def _():
            @pl.when(m >= RING)
            def _():
                pl.semaphore_wait(dy_free, 1)

            prev_copy(m).start()

        gi_out(m).start()
        dq_o.wait()

        @pl.when(m + 1 < subs)
        def _():
            fetch(m + 1)[2].start()
            fetch(m + 1)[3].start()

    def step(m, carry):
        @pl.when(m < subs)
        def _():
            mlp_part(m)

        @pl.when(m > 0)
        def _():
            attn_part(m - 1)

        return carry

    lax.fori_loop(0, subs + 1, step, 0)
    for acc, out in ((db1, db1_o), (db2, db2_o), (dbo, dbo_o)):
        out[...] = jnp.sum(acc[...], axis=0, keepdims=True)
    dbq_o[...] = jnp.sum(dbq[:, mine_q], axis=0, keepdims=True)
    dln_o[...] = jnp.sum(dln[...], axis=1)
    for copy in outs(subs - 1)[:2]:
        copy.wait()
    for m in (subs - 2, subs - 1):
        gi_out(m).wait()

        @pl.when(stage > 0)
        def _():
            prev_copy(m).wait_send()


ANY = pl.BlockSpec(memory_space=pl.ANY)
VMEM = pl.BlockSpec(memory_space=pltpu.VMEM)
DMA = pltpu.SemaphoreType.DMA
VMEM_LIMIT = 67043328


def fwd_call(stages, width, tile, x_in, wqt_own, wo_own, w1, w2, bq, bo, b1, b2, ln):
    subs, rows, d_model = x_in.shape
    ff = w1.shape[1]
    half = d_model // 2
    trio = 3 * half

    def hbm(cols, dtype=BF16):
        return jax.ShapeDtypeStruct((subs, rows, cols), dtype)

    def buf(cols, dtype=BF16):
        return pltpu.VMEM((rows, cols), dtype)

    def two(cols):
        return pltpu.VMEM((2, rows, cols), BF16)

    weights = 2 * (4 * d_model * d_model + 2 * d_model * ff)
    return pl.pallas_call(
        functools.partial(fwd_kernel, subs, stages, width, tile),
        name="fwd_stage",
        out_shape=(hbm(d_model), hbm(3 * d_model), hbm(half), hbm(d_model), hbm(d_model), hbm(d_model), hbm(ff, F32), hbm(ff), hbm(d_model), hbm(d_model),
                   jax.ShapeDtypeStruct((trio, d_model), BF16), jax.ShapeDtypeStruct((d_model, d_model), BF16), jax.ShapeDtypeStruct((ff, d_model), BF16), jax.ShapeDtypeStruct((d_model, ff), BF16),
                   *[jax.ShapeDtypeStruct((RELAYED, rows, d_model), BF16)] * 2),
        in_specs=[ANY] * 5 + [VMEM] * 5,
        out_specs=[ANY] * 16,
        scratch_shapes=[
            pltpu.VMEM((d_model, 3 * d_model), BF16), pltpu.VMEM((d_model, d_model), BF16), pltpu.VMEM(w1.shape, BF16), pltpu.VMEM(w2.shape, BF16),
            pltpu.VMEM((RING, rows, d_model), BF16), buf(d_model), buf(3 * d_model), buf(d_model), two(d_model), buf(d_model), buf(ff, F32), buf(ff), two(d_model), pltpu.VMEM((RING, rows, d_model), BF16), two(d_model),
            pltpu.VMEM((2, 4, rows, rows), F32), pltpu.VMEM((2, 4, rows, rows), BF16), pltpu.VMEM((2, 1, trio), BF16), pltpu.VMEM((d_model, 256), BF16), pltpu.VMEM((1, ff + 6 * d_model), F32),
            DMA((3,)), DMA, DMA((trio // 256,)), DMA((trio // 256,)), DMA, DMA, DMA, DMA, DMA((3, RELAYED)), DMA((2, RELAYED)), DMA((2,)), DMA((7,)), DMA((2,)), DMA((2,)), DMA((2,)), DMA((subs,)), DMA((2,)), DMA((subs,)), pltpu.SemaphoreType.REGULAR,
        ],
        cost_estimate=pl.CostEstimate(flops=subs * rows * weights, bytes_accessed=weights + subs * rows * d_model * 30, transcendentals=subs * rows * (ff + rows * 16)),
        compiler_params=pltpu.CompilerParams(collective_id=0, has_side_effects=True, vmem_limit_bytes=VMEM_LIMIT),
    )(x_in, wqt_own, wo_own, w1, w2, bq, bo, b1, b2, ln)


def bwd_call(stages, width, tile, dy_in, x_all, mid_all, s_all, qkv_all, w2t, w1t, wot, wqt_own, wqt_peer, ln):
    subs, rows, d_model = dy_in.shape
    ff = s_all.shape[2]
    half = d_model // 2
    trio = 3 * half

    def hbm(cols, dtype=BF16):
        return jax.ShapeDtypeStruct((subs, rows, cols), dtype)

    def buf(cols, dtype=BF16):
        return pltpu.VMEM((rows, cols), dtype)

    def two(cols):
        return pltpu.VMEM((2, rows, cols), BF16)

    ring = pltpu.VMEM((RING, rows, d_model), BF16)

    def acc(*shape):
        return jax.ShapeDtypeStruct(shape, F32)

    weights = 2 * (4 * d_model * d_model + 2 * d_model * ff)
    return pl.pallas_call(
        functools.partial(bwd_kernel, subs, stages, width, tile),
        name="bwd_stage",
        out_shape=(hbm(d_model), hbm(ff), hbm(d_model), hbm(trio), hbm(d_model),
                   acc(1, ff), acc(1, d_model), acc(1, d_model), acc(1, trio), acc(4, d_model)),
        in_specs=[ANY] * 10 + [VMEM],
        out_specs=[ANY] * 5 + [VMEM] * 5,
        scratch_shapes=[
            pltpu.VMEM(w2t.shape, BF16), pltpu.VMEM(w1t.shape, BF16), pltpu.VMEM((d_model, d_model), BF16), pltpu.VMEM((3 * d_model, d_model), BF16),
            ring, buf(ff, F32), buf(ff), two(d_model), ring, buf(d_model), buf(d_model), buf(d_model), buf(d_model), buf(3 * d_model), two(d_model),
            pltpu.VMEM((4, rows, rows), F32), pltpu.VMEM((4, rows, rows), F32), pltpu.VMEM((4, rows, rows), BF16), pltpu.VMEM((4, rows, rows), BF16),
            pltpu.VMEM((8, ff), F32), pltpu.VMEM((8, d_model), F32), pltpu.VMEM((8, d_model), F32), pltpu.VMEM((8, 3 * d_model), F32), pltpu.VMEM((4, 8, d_model), F32), pltpu.VMEM((4, d_model), F32),
            DMA((5,)), DMA((2,)), DMA((4,)), DMA((3,)), DMA((2,)), DMA((2,)), DMA((2,)), DMA((subs,)), DMA((2,)), DMA((subs,)), pltpu.SemaphoreType.REGULAR,
        ],
        cost_estimate=pl.CostEstimate(flops=subs * rows * weights, bytes_accessed=weights + subs * rows * d_model * 30, transcendentals=subs * rows * (ff + rows * 16)),
        compiler_params=pltpu.CompilerParams(collective_id=1, has_side_effects=True, vmem_limit_bytes=VMEM_LIMIT),
    )(dy_in, x_all, mid_all, s_all, qkv_all, w2t, w1t, wot, wqt_own, wqt_peer, ln)


def grad_kernel(last_stage, extra_count, stage, left, right, *refs):
    extras, out, passed = refs[:extra_count], refs[extra_count], refs[extra_count + 1:]
    if len(extras) == len(passed):
        for src, dst in zip(extras, passed):
            dst[...] = src[...]
    else:
        y, mid, own, peer, b2 = extras

        @pl.when(stage[0] < last_stage)
        def _():
            passed[0][...] = y[...]

        @pl.when(stage[0] == last_stage)
        def _():
            both = own[...].astype(F32) + peer[...].astype(F32)
            passed[0][...] = (mid[...].astype(F32) + both + b2[...].astype(F32)).astype(BF16)

    @pl.when(pl.program_id(1) == 0)
    def _():
        out[...] = jnp.zeros_like(out)

    n_tile = 512
    for n in starts(out.shape[1], n_tile):
        out[:, n:n + n_tile] += dot_tn(left[...], right[:, n:n + n_tile])


def grad_call(stage, last_stage, left, right, m_block, n_block, k_block, extras=(), passed=0):
    tokens, m_size = left.shape
    n_size = right.shape[1]
    m_count = m_size // m_block
    grid = (m_count * (n_size // n_block), tokens // k_block)
    steps = grid[0] * grid[1]

    def spec(array, used=lambda s: 1):
        if array.ndim == 2:
            return pl.BlockSpec(array.shape, lambda i, k, s: (0, 0))
        block = (array.shape[0] // steps,) + array.shape[1:]
        return pl.BlockSpec(block, lambda i, k, s: ((i * grid[1] + k) * used(s), 0, 0))

    in_specs = [pl.BlockSpec((k_block, m_block), lambda i, k, s: (k, i % m_count)), pl.BlockSpec((k_block, n_block), lambda i, k, s: (k, i // m_count))]
    if len(extras) > passed:
        in_specs += [spec(extras[0], lambda s: 1 - s[0] // last_stage)] + [spec(array, lambda s: s[0] // last_stage) for array in extras[1:]]
    else:
        in_specs += [spec(array) for array in extras]
    moved = 2 * tokens * (m_size * (n_size // n_block) + n_size * m_count) + 4 * m_size * n_size
    return pl.pallas_call(
        functools.partial(grad_kernel, last_stage, len(extras)),
        name="weight_grad",
        grid_spec=pltpu.PrefetchScalarGridSpec(
            num_scalar_prefetch=1, grid=grid, in_specs=in_specs,
            out_specs=[pl.BlockSpec((m_block, n_block), lambda i, k, s: (i % m_count, i // m_count))] + [spec(array) for array in extras[:passed]]),
        out_shape=[jax.ShapeDtypeStruct((m_size, n_size), F32)] + [jax.ShapeDtypeStruct(array.shape, array.dtype) for array in extras[:passed]],
        cost_estimate=pl.CostEstimate(flops=2 * tokens * m_size * n_size, bytes_accessed=moved, transcendentals=0),
        compiler_params=pltpu.CompilerParams(dimension_semantics=("arbitrary", "arbitrary"), vmem_limit_bytes=VMEM_LIMIT),
    )(stage, left, right, *extras)


def solution(mesh):
    stages = mesh.shape["pp"]

    def stage_program(x_in, dy_out, w_qkv, b_qkv, w_out, b_out, ln_par, w_fc1, b_fc1, w_fc2, b_fc2):
        micro, batch, rows, d_model = x_in.shape
        heads, width = w_qkv.shape[3:]
        half = heads * width
        subs = micro * batch
        tile = half

        wqt_own = jnp.transpose(w_qkv[0], (0, 2, 3, 1)).reshape(3 * half, d_model)
        ln = ln_par[0]
        x_all, qkv_all, o_all, mid_all, h1_all, h2_all, s_all, a_all, y_all, part_all, wqt_peer, wot, w1t, w2t, _, _ = fwd_call(
            stages, width, tile, x_in.reshape(subs, rows, d_model), wqt_own, w_out[0].reshape(half, d_model), w_fc1[0], w_fc2[0], b_qkv.reshape(1, -1), b_out, b_fc1, b_fc2, ln)
        dy_all, dpre_all, gmid_all, dqkv_all, gin_all, db1, db2, dbo, dbq, dln = bwd_call(
            stages, width, tile, dy_out.reshape(subs, rows, d_model), x_all, mid_all, s_all, qkv_all, w2t, w1t, wot, wqt_own, wqt_peer, ln)

        def flat(stack):
            return stack.reshape(subs * rows, -1)

        last_stage = stages - 1
        stage = lax.axis_index("pp").reshape(1)
        held, _ = lax.optimization_barrier((part_all, gin_all))
        peer_part = lax.ppermute(held, ("tp", "pp"), [(last_stage, stages + last_stage), (stages + last_stage, last_stage)])
        g_w_out, dbo, dln, db1, db2 = grad_call(stage, last_stage, flat(o_all), flat(gmid_all), half, d_model, d_model, (dbo, dln, db1, db2), 4)
        g_w_fc1, g_in = grad_call(stage, last_stage, flat(h2_all), flat(dpre_all), d_model, 1024, d_model, (gin_all,), 1)
        g_w_fc2, h_out = grad_call(stage, last_stage, flat(a_all), flat(dy_all), 1024, d_model, d_model, (y_all, mid_all, part_all, peer_part, b_fc2), 1)
        g_w_qkv = lax.optimization_barrier(dot_tn(flat(dqkv_all), flat(h1_all)))
        g_w_out = g_w_out.reshape(heads, width, d_model)
        g_w_qkv = jnp.transpose(g_w_qkv.reshape(3, heads, width, d_model), (0, 3, 1, 2))
        g_b_qkv = dbq.reshape(3, heads, width)
        act = (1, micro, batch, rows, d_model)
        return (h_out.reshape(act), g_in.reshape(act), g_w_qkv[None], g_b_qkv[None], g_w_out[None], dbo,
                dln[None], g_w_fc1[None], db1, g_w_fc2[None], db2)

    act_spec = P(None, "dp", None, None)
    arg_specs = (act_spec, act_spec,
                 P("pp", None, None, "tp", None), P("pp", None, "tp", None), P("pp", "tp", None, None),
                 P("pp", None), P("pp", None, None), P("pp", None, "tp"), P("pp", "tp"),
                 P("pp", "tp", None), P("pp", None))
    stage_spec = P("pp", None, "dp", None, None)
    grad_axes = ("dp", "pp")
    result_specs = (stage_spec, stage_spec,
                    P(grad_axes, None, None, "tp", None), P(grad_axes, None, "tp", None), P(grad_axes, "tp", None, None),
                    P(grad_axes, None), P(grad_axes, None, None), P(grad_axes, None, "tp"), P(grad_axes, "tp"),
                    P(grad_axes, "tp", None), P(grad_axes, None))
    return jax.shard_map(stage_program, mesh=mesh, in_specs=arg_specs, out_specs=result_specs, check_vma=False)
```
